32 devices in a mesh: dom: 8 (over z, y), sub: 4 (over x, core).
Axes of the slice: x: 2, y: 2, z: 4, core: 2. Of those that a mesh axis runs over, the one named last changes fastest.
Arguments:
- source: float32 [32, 7, 16, 1024], P('dom', None, 'sub'), may hold values from -6 to 6
- zone_ids: int32 [32, 1024], P('dom'), may hold values from 0 to 15
- kappa_table: float32 [16, 7], replicated, may hold values from 0.05 to 1
- mu_table: float32 [16, 8], replicated, may hold values from 0.2 to 2
- owner_dev: int32 [8, 32], P('dom'), may hold values from 0 to 7, as said below
- owner_group: int32 [8, 32], P('dom'), may hold values from 0 to 31, as said below
Outputs:
- edge_field: float32 [32, 7, 16, 1024], P('dom', None, 'sub')
- potential: float32 [32, 16, 1024], P('dom', 'sub')
The draws below stay inside these ranges and needn't reach their ends.
Inputs may be any that keep to these rules, and one draw needn't show every extreme that they name: owner_dev[d, j] is the index along dom of the device that sums slot j of device d; one device sends at most 4 of its slots to one owner, and exactly 4 to some owner. At owner e, receive position d * 4 + c stands for the c-th slot, in slot order, that device d sends to e. owner_group[e, d * 4 + c] is a receive position held alike by all copies of one shared primitive; a primitive has at most four copies, all at one owner; positions that no slot reaches hold their own index.
All inputs are finite; a program needn't handle non-finite values.
Results may differ from the reference program's by a relative error of at most 0.0001.
Values sent between devices are 32-bit elements; how exact they have to be, the bound alone decides.
No kernel may reach another device: no remote copies, remote signals or barrier semaphores. Data moves between devices by JAX's collectives and lax.ppermute only.
A program may use at most 64 MiB of HBM per device.

```python
import math
import jax
import jax.numpy as jnp
from jax import lax

MACROS = 4
LAT = 32
ZONES = 16
SWEEPS = 2
CELLS = 1024
SLOTS = 32
CAP = 4
RECV = 32
MACRO_ALL = 32
DEPTH = 16
N_DOM = 8
N_SUB = 4


def layout(key):
    base_key = jax.random.fold_in(key, 4177)
    slot_key, peer_key, score_key = jax.random.split(base_key, 3)
    slot_orders = jax.vmap(lambda item_key: jax.random.permutation(item_key, SLOTS))(jax.random.split(slot_key, N_DOM))
    peer_orders = jax.vmap(lambda item_key: jax.random.permutation(item_key, N_DOM))(jax.random.split(peer_key, N_DOM))
    owners = jnp.take_along_axis(peer_orders, slot_orders % N_DOM, axis=1).astype(jnp.int32)
    earlier = jnp.arange(SLOTS)[None, :] < jnp.arange(SLOTS)[:, None]
    same_owner = owners[:, :, None] == owners[:, None, :]
    position = jnp.sum(same_owner & earlier[None], axis=2).astype(jnp.int32)
    receive = jnp.arange(N_DOM, dtype=jnp.int32)[:, None] * CAP + position
    flat_index = (owners * RECV + receive).reshape(-1)
    live = jnp.zeros((N_DOM * RECV,), jnp.int32).at[flat_index].set(1).reshape(N_DOM, RECV)
    random_part = jax.random.randint(score_key, (N_DOM, RECV), 0, 32768).astype(jnp.int32)
    index_row = jnp.arange(RECV, dtype=jnp.int32)[None, :]
    scores = jnp.where(live > 0, random_part * RECV + index_row, 1073741824 + index_row)
    order = jnp.argsort(scores, axis=1).astype(jnp.int32)
    ranks = jnp.argsort(order, axis=1).astype(jnp.int32)
    live_count = jnp.sum(live, axis=1, keepdims=True)
    quad_end = 4 * (live_count // 8)
    leader_rank = jnp.where(ranks < quad_end, ranks - ranks % 4, ranks - ranks % 2)
    leaders = jnp.take_along_axis(order, leader_rank, axis=1)
    groups = jnp.where(live > 0, leaders, index_row).astype(jnp.int32)
    return (owners, groups)


def draw_owner_dev(key, part):
    owners, groups = layout(key)
    return owners


def draw_owner_group(key, part):
    owners, groups = layout(key)
    return groups


def place_ends(values, stream_key, low, top_value):
    extent = values.shape
    index_at = [jax.random.randint(jax.random.fold_in(stream_key, axis), (), 0, extent[axis]) for axis in range(len(extent))]
    values = values.at[tuple(index_at)].set(low)
    longest = extent.index(max(extent))
    index_at[longest] = (index_at[longest] + 1) % extent[longest]
    return values.at[tuple(index_at)].set(top_value)


def shard_levels(own_key, shape, cuts, smallest, largest):
    level = 1.0
    for dim, blocks in cuts:
        heights = jax.random.uniform(jax.random.fold_in(jax.random.fold_in(own_key, 6), dim), (blocks,), jnp.float32, smallest / len(cuts), largest / len(cuts))
        level = level * jnp.repeat(jnp.exp(heights), shape[dim] // blocks).reshape((-1,) + (1,) * (len(shape) - 1 - dim))
    return level


def scatter_about(rng, extent, spread, reach, cuts=(), kind=jnp.bfloat16):
    loudness = shard_levels(rng, extent, cuts, -0.22, 0.18) if cuts else 1.0
    drawn = jax.random.normal(rng, extent, jnp.float32) * spread * loudness
    return jnp.minimum(jnp.maximum(drawn, -reach), reach).astype(kind)


def setup_inputs(seed: int = 0) -> dict:
    splits = jax.random.split(jax.random.key(seed), 7)
    source = scatter_about(splits[0], (MACRO_ALL, 7, DEPTH, CELLS), 1.0, 6.0, ((0, 8), (2, 4)), jnp.float32)
    zone_ids = place_ends(jax.random.randint(splits[1], (MACRO_ALL, CELLS), 0, ZONES), jax.random.fold_in(splits[1], 1), 0, ZONES - 1).astype(jnp.int32)
    kappa_table = jnp.clip(jnp.exp(jax.random.uniform(splits[2], (ZONES, 7), jnp.float32, math.log(0.05), math.log(1.0))), 0.05, 1.0)
    mu_table = jnp.clip(jnp.exp(jax.random.uniform(splits[3], (ZONES, 8), jnp.float32, math.log(0.2), math.log(2.0))), 0.2, 2.0)
    owner_dev = draw_owner_dev(jax.random.fold_in(splits[6], 71), 0)
    owner_group = draw_owner_group(jax.random.fold_in(splits[6], 71), 0)
    return {"source": source, "zone_ids": zone_ids, "kappa_table": kappa_table, "mu_table": mu_table, "owner_dev": owner_dev, "owner_group": owner_group}


EDGE_OFFSETS = ((0, 0, 1), (0, 1, 0), (1, 0, 0), (0, 1, 1), (1, 0, 1), (1, 1, 0), (1, 1, 1))
FACE_EDGES = ((0, 1, 3), (1, 0, 3), (0, 2, 4), (2, 0, 4), (1, 2, 5), (2, 1, 5), (3, 2, 6), (2, 3, 6))
SHARED_TYPES = (1, 2, 5)
EDGE_DAMPING = 0.6
NODE_DAMPING = 0.8


def shift_ahead(values, rise_y, rise_x):
    offset = rise_y * LAT + rise_x
    if offset == 0:
        return values
    padding = jnp.zeros(values.shape[:-1] + (offset,), values.dtype)
    shifted = jnp.concatenate([values[..., offset:], padding], axis=-1)
    if rise_x:
        column = jnp.arange(values.shape[-1]) % LAT
        shifted = jnp.where(column < LAT - rise_x, shifted, jnp.zeros_like(shifted))
    return shifted


def shift_behind(values, rise_y, rise_x):
    offset = rise_y * LAT + rise_x
    if offset == 0:
        return values
    padding = jnp.zeros(values.shape[:-1] + (offset,), values.dtype)
    shifted = jnp.concatenate([padding, values[..., :-offset]], axis=-1)
    if rise_x:
        column = jnp.arange(values.shape[-1]) % LAT
        shifted = jnp.where(column >= rise_x, shifted, jnp.zeros_like(shifted))
    return shifted


def apply_operator(padded, halo_width, extra_planes, first_plane, mass_coef, curl_coef):
    planes = padded.shape[2] - 2 * halo_width
    face_count = planes + extra_planes + 1
    first_face = halo_width - extra_planes - 1
    face_planes = first_plane - extra_planes - 1 + jnp.arange(face_count)
    face_valid = (face_planes >= 0)[None, :, None]
    result = [mass_coef[edge_type][:, None, :] * padded[:, edge_type, halo_width - extra_planes:halo_width + planes] for edge_type in range(7)]
    for face_index, (first_edge, second_edge, diagonal_edge) in enumerate(FACE_EDGES):
        rise_z, rise_y, rise_x = EDGE_OFFSETS[first_edge]
        far_values = shift_ahead(padded[:, second_edge, first_face + rise_z:first_face + rise_z + face_count], rise_y, rise_x)
        circulation = padded[:, first_edge, first_face:first_face + face_count] + far_values - padded[:, diagonal_edge, first_face:first_face + face_count]
        weighted = jnp.where(face_valid, curl_coef[face_index][:, None, :] * circulation, 0.0)
        result[first_edge] = result[first_edge] + weighted[:, 1:]
        result[diagonal_edge] = result[diagonal_edge] - weighted[:, 1:]
        result[second_edge] = result[second_edge] + shift_behind(weighted[:, 1 - rise_z:1 - rise_z + planes + extra_planes], rise_y, rise_x)
    return jnp.stack(result, axis=1)


def edge_diagonal(mass_coef, curl_coef, first_plane, planes):
    inside = ((first_plane + jnp.arange(planes)) >= 1)[None, :, None]
    flat_planes = jnp.zeros((1, planes, 1), mass_coef.dtype)
    diagonal = [mass_coef[edge_type][:, None, :] + flat_planes for edge_type in range(7)]
    for face_index, (first_edge, second_edge, diagonal_edge) in enumerate(FACE_EDGES):
        rise_z, rise_y, rise_x = EDGE_OFFSETS[first_edge]
        own_term = curl_coef[face_index][:, None, :]
        diagonal[first_edge] = diagonal[first_edge] + own_term
        diagonal[diagonal_edge] = diagonal[diagonal_edge] + own_term
        behind_term = shift_behind(curl_coef[face_index], rise_y, rise_x)[:, None, :] + flat_planes
        if rise_z:
            behind_term = jnp.where(inside, behind_term, 0.0)
        diagonal[second_edge] = diagonal[second_edge] + behind_term
    return jnp.stack(diagonal, axis=1)


def node_diagonal(mass_coef, first_plane, planes):
    inside = ((first_plane + jnp.arange(planes)) >= 1)[None, :, None]
    total = jnp.zeros((mass_coef.shape[1], planes, mass_coef.shape[2]), mass_coef.dtype)
    for edge_type in range(7):
        rise_z, rise_y, rise_x = EDGE_OFFSETS[edge_type]
        total = total + mass_coef[edge_type][:, None, :]
        behind_term = shift_behind(mass_coef[edge_type], rise_y, rise_x)[:, None, :] + jnp.zeros((1, planes, 1), mass_coef.dtype)
        if rise_z:
            behind_term = jnp.where(inside, behind_term, 0.0)
        total = total + behind_term
    return total


def node_residual(lowered, planes):
    total = jnp.zeros((lowered.shape[0], planes, lowered.shape[3]), lowered.dtype)
    for edge_type in range(7):
        rise_z, rise_y, rise_x = EDGE_OFFSETS[edge_type]
        total = total + shift_behind(lowered[:, edge_type, 1 - rise_z:1 - rise_z + planes], rise_y, rise_x) - lowered[:, edge_type, 1:]
    return total


def gradient(raised, planes):
    result = []
    for edge_type in range(7):
        rise_z, rise_y, rise_x = EDGE_OFFSETS[edge_type]
        result.append(shift_ahead(raised[:, rise_z:rise_z + planes], rise_y, rise_x) - raised[:, :planes])
    return jnp.stack(result, axis=1)


def edge_sides(values, layers):
    macro_count, type_count, plane_count, cell_count = values.shape
    lattice = values.reshape(macro_count, type_count, plane_count, LAT, LAT)
    chosen = jnp.stack([lattice[:, edge_type] for edge_type in SHARED_TYPES], axis=1)
    sides = jnp.stack([chosen[..., 0], chosen[..., LAT - 1]], axis=1)
    sides = jnp.transpose(sides, (0, 1, 3, 2, 4))
    sides = sides.reshape(macro_count, 2, layers, plane_count // layers, 3 * LAT)
    return jnp.transpose(sides, (2, 0, 1, 3, 4)).reshape(layers, -1, 3 * LAT)


def insert_edges(values, blocks, layers):
    macro_count, type_count, plane_count, cell_count = values.shape
    shaped = blocks.reshape(layers, macro_count, 2, plane_count // layers, 3, LAT)
    shaped = jnp.transpose(shaped, (1, 2, 4, 0, 3, 5)).reshape(macro_count, 2, 3, plane_count, LAT)
    lattice = values.reshape(macro_count, type_count, plane_count, LAT, LAT)
    for side_index, column in ((0, 0), (1, LAT - 1)):
        for slot_type, edge_type in enumerate(SHARED_TYPES):
            lattice = lattice.at[:, edge_type, :, :, column].set(shaped[:, side_index, slot_type])
    return lattice.reshape(values.shape)


def node_sides(values, layers):
    macro_count, plane_count, cell_count = values.shape
    lattice = values.reshape(macro_count, plane_count, LAT, LAT)
    sides = jnp.stack([lattice[..., 0], lattice[..., LAT - 1]], axis=1)
    sides = sides.reshape(macro_count, 2, layers, plane_count // layers, LAT)
    return jnp.transpose(sides, (2, 0, 1, 3, 4)).reshape(layers, -1, LAT)


def insert_nodes(values, blocks, layers):
    macro_count, plane_count, cell_count = values.shape
    shaped = blocks.reshape(layers, macro_count, 2, plane_count // layers, LAT)
    shaped = jnp.transpose(shaped, (1, 2, 0, 3, 4)).reshape(macro_count, 2, plane_count, LAT)
    lattice = values.reshape(macro_count, plane_count, LAT, LAT)
    for side_index, column in ((0, 0), (1, LAT - 1)):
        lattice = lattice.at[:, :, :, column].set(shaped[:, side_index])
    return lattice.reshape(values.shape)


def group_keys(owners, groups, capacity):
    device_count, slot_count = owners.shape
    earlier = jnp.arange(slot_count)[None, :] < jnp.arange(slot_count)[:, None]
    same_owner = owners[:, :, None] == owners[:, None, :]
    position = jnp.sum(same_owner & earlier[None], axis=2).astype(jnp.int32)
    receive = jnp.arange(device_count).astype(jnp.int32)[:, None] * capacity + position
    leaders = groups[owners, receive].astype(jnp.int32)
    return (owners * groups.shape[1] + leaders).astype(jnp.int32)


def assemble(blocks, keys):
    layers = blocks.shape[1]
    flattened = jnp.transpose(blocks, (1, 0, 2, 3)).reshape(layers, -1, blocks.shape[3])
    key_list = keys.reshape(-1)
    group_sums = jax.vmap(lambda layer_blocks: jax.ops.segment_sum(layer_blocks, key_list, N_DOM * RECV))(flattened)
    picked = group_sums[:, key_list]
    return jnp.transpose(picked.reshape(layers, N_DOM, -1, blocks.shape[3]), (1, 0, 2, 3))


def reference(source, zone_ids, kappa_table, mu_table, owner_dev, owner_group):
    fields = source.reshape(N_DOM, MACROS, 7, DEPTH, CELLS)
    zone_rows = zone_ids.reshape(N_DOM, MACROS, CELLS)
    keys = group_keys(owner_dev, owner_group, CAP)

    def lookup(zone_row):
        return jnp.moveaxis(kappa_table[zone_row], -1, 0), jnp.moveaxis(mu_table[zone_row], -1, 0)

    def operator_of(items):
        edge_values, zone_row = items
        mass_coef, curl_coef = lookup(zone_row)
        padded = jnp.pad(edge_values, ((0, 0), (0, 0), (1, 1), (0, 0)))
        return apply_operator(padded, 1, 0, 0, mass_coef, curl_coef)

    def diagonal_blocks(zone_row):
        mass_coef, curl_coef = lookup(zone_row)
        return edge_sides(edge_diagonal(mass_coef, curl_coef, 0, DEPTH), N_SUB), node_sides(node_diagonal(mass_coef, 0, DEPTH), N_SUB)

    edge_diag_blocks, node_diag_blocks = lax.map(diagonal_blocks, zone_rows)
    edge_diag_sum = assemble(edge_diag_blocks, keys)
    node_diag_sum = assemble(node_diag_blocks, keys)

    def edge_step(items):
        edge_values, residual_values, zone_row, residual_blocks, diag_blocks = items
        mass_coef, curl_coef = lookup(zone_row)
        full_residual = insert_edges(residual_values, residual_blocks, N_SUB)
        full_diagonal = insert_edges(edge_diagonal(mass_coef, curl_coef, 0, DEPTH), diag_blocks, N_SUB)
        return edge_values + EDGE_DAMPING * full_residual / full_diagonal

    def node_step(items):
        edge_values, source_values, zone_row = items
        residual_new = source_values - operator_of((edge_values, zone_row))
        lowered = jnp.pad(residual_new, ((0, 0), (0, 0), (1, 0), (0, 0)))
        return node_residual(lowered, DEPTH)

    def potential_step(items):
        node_values, zone_row, node_blocks, diag_blocks = items
        mass_coef, curl_coef = lookup(zone_row)
        full_nodes = insert_nodes(node_values, node_blocks, N_SUB)
        full_diagonal = insert_nodes(node_diagonal(mass_coef, 0, DEPTH), diag_blocks, N_SUB)
        return NODE_DAMPING * full_nodes / full_diagonal

    def raise_step(items):
        edge_values, correction_values = items
        raised = jnp.pad(correction_values, ((0, 0), (0, 1), (0, 0)))
        return edge_values + gradient(raised, DEPTH)

    edge_field = jnp.zeros_like(fields)
    potential = jnp.zeros((N_DOM, MACROS, DEPTH, CELLS), fields.dtype)
    for sweep_index in range(SWEEPS):
        if sweep_index == 0:
            residual = fields
        else:
            residual = fields - lax.map(operator_of, (edge_field, zone_rows))
        residual_sum = assemble(lax.map(lambda items: edge_sides(items, N_SUB), residual), keys)
        edge_field = lax.map(edge_step, (edge_field, residual, zone_rows, residual_sum, edge_diag_sum))
        node_values = lax.map(node_step, (edge_field, fields, zone_rows))
        node_sum = assemble(lax.map(lambda items: node_sides(items, N_SUB), node_values), keys)
        correction = lax.map(potential_step, (node_values, zone_rows, node_sum, node_diag_sum))
        edge_field = lax.map(raise_step, (edge_field, correction))
        potential = potential + correction
    return edge_field.reshape(MACRO_ALL, 7, DEPTH, CELLS), potential.reshape(MACRO_ALL, DEPTH, CELLS)
```

```python
import jax
import jax.numpy as jnp
from jax import lax
from jax.experimental import pallas as pl
from jax.experimental.pallas import tpu as pltpu
from jax.sharding import PartitionSpec as P

LAT = 32
SWEEPS = 2


EDGE_OFFSETS = ((0, 0, 1), (0, 1, 0), (1, 0, 0), (0, 1, 1), (1, 0, 1), (1, 1, 0), (1, 1, 1))
FACE_EDGES = (
    (0, 1, 3),
    (1, 0, 3),
    (0, 2, 4),
    (2, 0, 4),
    (1, 2, 5),
    (2, 1, 5),
    (3, 2, 6),
    (2, 3, 6),
)
SHARED_TYPES = (1, 2, 5)
EDGE_DAMPING = 0.6
NODE_DAMPING = 0.8


def with_halo(block, sides, width):
    for axis, dim in sides:
        count = lax.axis_size(axis)
        forward = [(i, i + 1) for i in range(count - 1)]
        backward = [(target, source) for source, target in forward]
        low = lax.ppermute(
            lax.slice_in_dim(block, block.shape[dim] - width, None, axis=dim), axis, forward
        )
        high = lax.ppermute(lax.slice_in_dim(block, 0, width, axis=dim), axis, backward)
        block = jnp.concatenate([low, block, high], axis=dim)
    return block


def from_behind(block, axis, distance):
    devices = range(lax.axis_size(axis))
    route = [(i - distance, i) for i in devices if i - distance in devices]
    return lax.ppermute(block, axis, route)


def shift_ahead(values, rise_y, rise_x):
    offset = rise_y * LAT + rise_x
    if offset == 0:
        return values
    padding = jnp.zeros(values.shape[:-1] + (offset,), values.dtype)
    shifted = jnp.concatenate([values[..., offset:], padding], axis=-1)
    if rise_x:
        column = jnp.arange(values.shape[-1]) % LAT
        shifted = jnp.where(column < LAT - rise_x, shifted, jnp.zeros_like(shifted))
    return shifted


def shift_behind(values, rise_y, rise_x):
    offset = rise_y * LAT + rise_x
    if offset == 0:
        return values
    padding = jnp.zeros(values.shape[:-1] + (offset,), values.dtype)
    shifted = jnp.concatenate([padding, values[..., :-offset]], axis=-1)
    if rise_x:
        column = jnp.arange(values.shape[-1]) % LAT
        shifted = jnp.where(column >= rise_x, shifted, jnp.zeros_like(shifted))
    return shifted


def apply_operator(padded, halo_width, extra_planes, first_plane, mass_coef, curl_coef):
    planes = padded.shape[2] - 2 * halo_width
    face_count = planes + extra_planes + 1
    first_face = halo_width - extra_planes - 1
    face_planes = first_plane - extra_planes - 1 + jnp.arange(face_count)
    face_valid = (face_planes >= 0)[None, :, None]
    result = [
        mass_coef[edge_type][:, None, :]
        * padded[:, edge_type, halo_width - extra_planes : halo_width + planes]
        for edge_type in range(7)
    ]
    for face_index, (first_edge, second_edge, diagonal_edge) in enumerate(FACE_EDGES):
        rise_z, rise_y, rise_x = EDGE_OFFSETS[first_edge]
        far_values = shift_ahead(
            padded[:, second_edge, first_face + rise_z : first_face + rise_z + face_count],
            rise_y,
            rise_x,
        )
        circulation = (
            padded[:, first_edge, first_face : first_face + face_count]
            + far_values
            - padded[:, diagonal_edge, first_face : first_face + face_count]
        )
        weighted = jnp.where(face_valid, curl_coef[face_index][:, None, :] * circulation, 0.0)
        result[first_edge] = result[first_edge] + weighted[:, 1:]
        result[diagonal_edge] = result[diagonal_edge] - weighted[:, 1:]
        result[second_edge] = result[second_edge] + shift_behind(
            weighted[:, 1 - rise_z : 1 - rise_z + planes + extra_planes], rise_y, rise_x
        )
    return jnp.stack(result, axis=1)


def edge_diagonal(mass_coef, curl_coef, first_plane, planes):
    inside = (first_plane + jnp.arange(planes) >= 1)[None, :, None]
    flat_planes = jnp.zeros((1, planes, 1), mass_coef.dtype)
    diagonal = [mass_coef[edge_type][:, None, :] + flat_planes for edge_type in range(7)]
    for face_index, (first_edge, second_edge, diagonal_edge) in enumerate(FACE_EDGES):
        rise_z, rise_y, rise_x = EDGE_OFFSETS[first_edge]
        own_term = curl_coef[face_index][:, None, :]
        diagonal[first_edge] = diagonal[first_edge] + own_term
        diagonal[diagonal_edge] = diagonal[diagonal_edge] + own_term
        behind_term = shift_behind(curl_coef[face_index], rise_y, rise_x)[:, None, :] + flat_planes
        if rise_z:
            behind_term = jnp.where(inside, behind_term, 0.0)
        diagonal[second_edge] = diagonal[second_edge] + behind_term
    return jnp.stack(diagonal, axis=1)


def node_diagonal(mass_coef, first_plane, planes):
    inside = (first_plane + jnp.arange(planes) >= 1)[None, :, None]
    total = jnp.zeros((mass_coef.shape[1], planes, mass_coef.shape[2]), mass_coef.dtype)
    for edge_type in range(7):
        rise_z, rise_y, rise_x = EDGE_OFFSETS[edge_type]
        total = total + mass_coef[edge_type][:, None, :]
        behind_term = shift_behind(mass_coef[edge_type], rise_y, rise_x)[:, None, :] + jnp.zeros(
            (1, planes, 1), mass_coef.dtype
        )
        if rise_z:
            behind_term = jnp.where(inside, behind_term, 0.0)
        total = total + behind_term
    return total


def node_residual(lowered, planes):
    total = jnp.zeros((lowered.shape[0], planes, lowered.shape[3]), lowered.dtype)
    for edge_type in range(7):
        rise_z, rise_y, rise_x = EDGE_OFFSETS[edge_type]
        total = (
            total
            + shift_behind(lowered[:, edge_type, 1 - rise_z : 1 - rise_z + planes], rise_y, rise_x)
            - lowered[:, edge_type, 1:]
        )
    return total


def gradient(raised, planes):
    result = []
    for edge_type in range(7):
        rise_z, rise_y, rise_x = EDGE_OFFSETS[edge_type]
        result.append(
            shift_ahead(raised[:, rise_z : rise_z + planes], rise_y, rise_x) - raised[:, :planes]
        )
    return jnp.stack(result, axis=1)


def edge_sides(values):
    macro_count, type_count, plane_count, cell_count = values.shape
    lattice = values.reshape(macro_count, type_count, plane_count, LAT, LAT)
    chosen = jnp.stack([lattice[:, edge_type] for edge_type in SHARED_TYPES], axis=1)
    sides = jnp.stack([chosen[..., 0], chosen[..., LAT - 1]], axis=1)
    return jnp.transpose(sides, (0, 1, 3, 2, 4)).reshape(-1, 3 * LAT)


def insert_edges(values, blocks):
    macro_count, type_count, plane_count, cell_count = values.shape
    shaped = blocks.reshape(macro_count, 2, plane_count, 3, LAT)
    shaped = jnp.transpose(shaped, (0, 1, 3, 2, 4))
    lattice = values.reshape(macro_count, type_count, plane_count, LAT, LAT)
    for side_index, column in ((0, 0), (1, LAT - 1)):
        for slot_type, edge_type in enumerate(SHARED_TYPES):
            lattice = lattice.at[:, edge_type, :, :, column].set(shaped[:, side_index, slot_type])
    return lattice.reshape(values.shape)


def node_sides(values):
    macro_count, plane_count, cell_count = values.shape
    lattice = values.reshape(macro_count, plane_count, LAT, LAT)
    sides = jnp.stack([lattice[..., 0], lattice[..., LAT - 1]], axis=1)
    return sides.reshape(-1, LAT)


def insert_nodes(values, blocks):
    macro_count, plane_count, cell_count = values.shape
    shaped = blocks.reshape(macro_count, 2, plane_count, LAT)
    lattice = values.reshape(macro_count, plane_count, LAT, LAT)
    for side_index, column in ((0, 0), (1, LAT - 1)):
        lattice = lattice.at[:, :, :, column].set(shaped[:, side_index])
    return lattice.reshape(values.shape)


def local(source, zone_ids, kappa_table, mu_table, owner_dev, owner_group):
    macro_count, type_count, planes, cell_count = source.shape
    first_plane = lax.axis_index("sub") * planes
    onehot = (jnp.arange(kappa_table.shape[0])[:, None] == zone_ids.reshape(1, -1)).astype(
        jnp.float32
    )
    mass_coef = jnp.dot(kappa_table.T, onehot, precision=lax.Precision.HIGHEST).reshape(
        type_count, macro_count, cell_count
    )
    curl_coef = jnp.dot(mu_table.T, onehot, precision=lax.Precision.HIGHEST).reshape(
        mu_table.shape[1], macro_count, cell_count
    )
    peer_count = lax.axis_size("dom")
    recv_rows = owner_group.shape[1]
    capacity = recv_rows // peer_count
    slot_count = owner_dev.shape[1]
    owner_of = owner_dev[0]
    groups = owner_group[0]
    earlier = jnp.arange(slot_count)[None, :] < jnp.arange(slot_count)[:, None]
    position = jnp.sum((owner_of[:, None] == owner_of[None, :]) & earlier, axis=1)
    slot_place = owner_of * capacity + position
    spread = (jnp.arange(recv_rows)[:, None] == slot_place[None, :]).astype(jnp.float32)
    same_group = (groups[:, None] == groups[None, :]).astype(jnp.float32)

    def owner_sum(received):
        summed = jnp.dot(
            same_group, received.reshape(recv_rows, -1), precision=lax.Precision.HIGHEST
        )
        return lax.all_to_all(
            summed.reshape(peer_count, capacity, -1), "dom", split_axis=0, concat_axis=0, tiled=True
        )

    def assemble(blocks):
        outgoing = jnp.dot(spread, blocks, precision=lax.Precision.HIGHEST).reshape(
            peer_count, capacity, blocks.shape[1]
        )
        returned = owner_sum(
            lax.all_to_all(outgoing, "dom", split_axis=0, concat_axis=0, tiled=True)
        )
        return jnp.take(returned.reshape(recv_rows, -1), slot_place, axis=0)

    rim_width = 2

    def rimmed(values):
        return with_halo(values, (("sub", 2),), rim_width)

    edge_diag = edge_diagonal(mass_coef, curl_coef, first_plane, planes)
    node_diag = node_diagonal(mass_coef, first_plane, planes)
    edge_width = 3 * LAT
    first_blocks = [edge_sides(edge_diag), node_sides(node_diag)]
    diag_sums = assemble(jnp.concatenate(first_blocks, axis=1))
    full_edge_diag = insert_edges(edge_diag, diag_sums[:, :edge_width])
    full_node_diag = insert_nodes(node_diag, diag_sums[:, edge_width : edge_width + LAT])
    source_below = from_behind(source[:, :, planes - 1 :], "sub", 1)
    edge_field = jnp.zeros_like(source)
    potential = jnp.zeros((macro_count, planes, cell_count), jnp.float32)
    for sweep_index in range(SWEEPS):
        if sweep_index == 0:
            residual = source
            residual_sum = assemble(edge_sides(residual))
        else:
            residual = source - apply_operator(
                rimmed(edge_field), rim_width, 0, first_plane, mass_coef, curl_coef
            )
            residual_sum = assemble(edge_sides(residual))
        full_residual = insert_edges(residual, residual_sum)
        edge_field = edge_field + EDGE_DAMPING * full_residual / full_edge_diag
        padded = rimmed(edge_field)
        lowered = jnp.concatenate([source_below, source], axis=2) - apply_operator(
            padded, 2, 1, first_plane, mass_coef, curl_coef
        )
        node_values = node_residual(lowered, planes)
        node_sum = assemble(node_sides(node_values))
        correction = NODE_DAMPING * insert_nodes(node_values, node_sum) / full_node_diag
        plane_above = from_behind(correction[:, :1], "sub", -1)
        edge_field = edge_field + gradient(
            jnp.concatenate([correction, plane_above], axis=1), planes
        )
        potential = potential + correction
    return (edge_field, potential)


LANES = 128
XS = (0, LAT - 1)


def lane_roll(v, s):
    s = s % v.shape[-1]
    return pltpu.roll(v, s, v.ndim - 1) if s else v


def row_roll(v, s):
    s = s % v.shape[0]
    return pltpu.roll(v, s, 0) if s else v


def iota(shape, dim):
    return lax.broadcasted_iota(jnp.int32, shape, dim)


class Plane:
    def __init__(self, shape):
        self.lane = iota(shape, 1)
        self.x = self.lane & (LAT - 1)
        self.cells = shape[1]
        self.side = (self.x == 0) | (self.x == LAT - 1)

    def ax(self, v):
        return jnp.where(self.x < LAT - 1, lane_roll(v, -1), 0.0)

    def ay(self, v):
        return jnp.where(self.lane < self.cells - LAT, lane_roll(v, -LAT), 0.0)

    def bx(self, v):
        return jnp.where(self.x > 0, lane_roll(v, 1), 0.0)

    def by(self, v):
        return jnp.where(self.lane >= LAT, lane_roll(v, LAT), 0.0)

    def bxy(self, v):
        return jnp.where((self.lane >= LAT) & (self.x > 0), lane_roll(v, LAT + 1), 0.0)

    def axy(self, v):
        return jnp.where(
            (self.lane < self.cells - LAT) & (self.x < LAT - 1), lane_roll(v, -LAT - 1), 0.0
        )


def zb(v):
    return row_roll(v, 1)


def za(v):
    return row_roll(v, -1)


def pack(feats, x_at):
    rows = feats[0].shape[0]
    low = iota((rows, LANES), 1) & 31
    out = jnp.zeros((rows, LANES), jnp.float32)
    for g, feat in enumerate(feats):
        for c in range(8):
            at = 8 * g + c
            column = feat[:, LANES * c : LANES * (c + 1)]
            out = jnp.where(low == at, lane_roll(column, at - x_at), out)
    return out


def unpack(packed_sides, g, base):
    rows = packed_sides[0].shape[0]
    low = iota((rows, LANES), 1) & 31
    columns = []
    for c in range(8):
        column = base[:, LANES * c : LANES * (c + 1)]
        for x_at, packed in zip(XS, packed_sides):
            column = jnp.where(low == x_at, lane_roll(packed, x_at - 8 * g - c), column)
        columns.append(column)
    return jnp.concatenate(columns, axis=1)


def packed_behind(v):
    lane = iota(v.shape, 1)
    first = jnp.where((lane & 7) == 0, 0.0, lane_roll(v, 33))
    return jnp.where(lane < 32, first, lane_roll(v, 32))


def packed_ahead(v):
    lane = iota(v.shape, 1)
    last = jnp.where((lane & 7) == 7, 0.0, lane_roll(v, -33))
    return jnp.where(lane >= 96, last, lane_roll(v, -32))


def group_of(shape):
    return (iota(shape, 1) >> 3) & 3


def group_sum(same, block):
    total = None
    rest = block
    for _ in range(3):
        part = rest.astype(jnp.bfloat16)
        rest = rest - part.astype(jnp.float32)
        piece = jnp.dot(same, part, preferred_element_type=jnp.float32)
        total = piece if total is None else total + piece
    return total


def node_back(r, valid):
    own = -(((r[0] + r[1]) + (r[2] + r[3])) + ((r[4] + r[5]) + r[6]))
    back = zb(r[2]) + valid.bx(r[0] + zb(r[4])) + valid.by(r[1] + zb(r[5]))
    return own + back + valid.bxy(r[3] + zb(r[6]))


def node_grad(c, plane):
    cx, cy, cxy = plane.ax(c), plane.ay(c), plane.axy(c)
    ends = (cx, cy, za(c), cxy, za(cx), za(cy), za(cxy))
    return [end - c for end in ends]


def curl_curl(e, mu, plane, valid):
    far = (
        plane.ax(e[1]),
        plane.ay(e[0]),
        plane.ax(e[2]),
        za(e[0]),
        plane.ay(e[2]),
        za(e[1]),
        plane.axy(e[2]),
        za(e[3]),
    )
    w = []
    for f, (first, second, diagonal) in enumerate(FACE_EDGES):
        w.append(jnp.where(valid, mu[f] * (e[first] + far[f] - e[diagonal]), 0.0))
    return [
        w[0] + w[2] + plane.by(w[1]) + zb(w[3]),
        w[1] + w[4] + plane.bx(w[0]) + zb(w[5]),
        w[3] + w[5] + w[7] + plane.bx(w[2]) + plane.by(w[4]) + plane.bxy(w[6]),
        w[6] + zb(w[7]) - w[0] - w[1],
        -w[2] - w[3],
        -w[4] - w[5],
        -w[6] - w[7],
    ]


def plane_flags(axis, planes, halo, cells):
    depth = planes * lax.axis_size(axis)
    at = lax.axis_index(axis) * planes - halo + iota((planes + 2 * halo, cells), 0)
    return at >= 1, (at >= 0) & (at < depth)


HALO = 2


def first_kernel(n_dom, n_sub, macros, planes, cells, slots, recv_rows):
    rows = planes + 2 * HALO
    sides = 2 * macros
    capacity = recv_rows // n_dom

    def body(zone_ref, table_ref, source_ref, owner_ref, group_ref, pay_ref, coef_ref, w_ref, nw_ref, sx_ref, hold_ref):
        k = lax.axis_index("sub")
        d = lax.axis_index("dom")
        plane = Plane((rows, cells))
        inside, _ = plane_flags("sub", planes, HALO, cells)
        owner = owner_ref[...]
        si, sj = iota((slots, slots), 0), iota((slots, slots), 1)
        owner_f = owner.astype(jnp.float32)
        column = jnp.sum(jnp.where(si == sj, owner_f, 0.0), axis=1, keepdims=True)
        lower = jnp.where((column == owner_f) & (si < sj), 1.0, 0.0)
        position = jnp.sum(lower, axis=0, keepdims=True)
        flat = owner_f * recv_rows + (d * capacity).astype(jnp.float32) + position
        keyed = group_ref[...].astype(jnp.float32) + (d * recv_rows).astype(jnp.float32)

        def spread_lanes(values, g):
            count = values.shape[1]
            place = iota((count, LANES), 0)
            place = 32 * (place >> 3) + (place & 7) + 8 * g
            hot = jnp.where(place == iota((count, LANES), 1), 1.0, 0.0)
            return jnp.dot(
                jnp.broadcast_to(values, (8, count)), hot, precision=lax.Precision.HIGHEST
            )

        index_rows = spread_lanes(flat, 0) + spread_lanes(keyed, 1)
        low = iota((rows, LANES), 1) & 31
        sx_ref[...] = jnp.zeros_like(sx_ref)

        def macro_step(m, carry):
            zone = jnp.broadcast_to(zone_ref[pl.ds(m, 1), :], (8, cells))
            mass8 = jnp.zeros((8, cells), jnp.float32)
            curl8 = jnp.zeros((8, cells), jnp.float32)
            for z in range(table_ref.shape[1]):
                hit = zone == z
                mass8 = jnp.where(hit, table_ref[0:8, z : z + 1], mass8)
                curl8 = jnp.where(hit, table_ref[8:16, z : z + 1], curl8)
            coef_ref[m, 0:8, :] = mass8
            coef_ref[m, 8:16, :] = curl8

            def coef(i):
                return jnp.broadcast_to(coef_ref[m, i : i + 1, :], (rows, cells))

            mass = [coef(t) for t in range(7)]
            mu = [coef(8 + f) for f in range(8)]
            flat_diag = [
                mass[0] + mu[0] + mu[2] + plane.by(mu[1]),
                mass[1] + mu[1] + mu[4] + plane.bx(mu[0]),
                mass[2] + mu[3] + mu[5] + mu[7] + plane.bx(mu[2]) + plane.by(mu[4]) + plane.bxy(mu[6]),
                mass[3] + mu[0] + mu[1] + mu[6],
                mass[4] + mu[2] + mu[3],
                mass[5] + mu[4] + mu[5],
                mass[6] + mu[6] + mu[7],
            ]
            rise = {0: mu[3], 1: mu[5], 3: mu[7]}
            for t in range(7):
                diag = flat_diag[t]
                if t in rise:
                    diag = diag + jnp.where(inside, rise[t], 0.0)
                w_ref[m, t] = EDGE_DAMPING / diag
            node_flat = plane.bx(mass[0]) + plane.by(mass[1]) + plane.bxy(mass[3])
            for t in range(7):
                node_flat = node_flat + mass[t]
            node_rise = mass[2] + plane.bx(mass[4]) + plane.by(mass[5]) + plane.bxy(mass[6])
            nw_ref[m] = NODE_DAMPING / (node_flat + jnp.where(inside, node_rise, 0.0))
            for t in range(7):
                sx_ref[t, HALO : HALO + planes, :] = source_ref[m, t]
            src = [sx_ref[t] for t in range(7)]
            left = []
            for t in range(7):
                value = src[t] - mass[t] * (w_ref[m, t] * src[t])
                if t in SHARED_TYPES:
                    value = jnp.where(plane.side, 0.0, value)
                left.append(value)
            node = node_back(left, plane)
            k0, k1 = k == 0, k == 1
            extra = [
                jnp.where(k0, mass[1], jnp.where(k1, flat_diag[1] + mu[5], flat_diag[1])),
                jnp.where(k0, mass[2], jnp.where(k1, flat_diag[2], node_flat + node_rise)),
                jnp.where(k0, mass[5], jnp.where(k1, flat_diag[5], node_flat)),
            ]
            for s, x_at in enumerate(XS):
                packed = pack([src[1], src[2], src[5], node], x_at)
                extras = jnp.where(k == 3, index_rows, pack(extra, x_at))
                row = jnp.where(low < 24, extras, row_roll(packed, -(HALO + planes)))
                hold_ref[m, s, 0:8, :] = packed
                hold_ref[m, s, 8:16, :] = row
            return carry

        lax.fori_loop(0, macros, macro_step, 0)
        for m in range(macros):
            for s in range(2):
                ms = 2 * m + s
                for p in range(planes):
                    pay_ref[0, p * sides + ms : p * sides + ms + 1, :] = hold_ref[m, s, HALO + p : HALO + p + 1, :]
                at = planes * sides + ms
                pay_ref[0, at : at + 1, :] = hold_ref[m, s, 8:9, :]
        block = pay_ref[0]
        for dest in range(1, n_dom * n_sub):
            pay_ref[dest] = block

    f32 = jnp.float32
    return pl.pallas_call(
        body,
        name="first",
        out_shape=(
            jax.ShapeDtypeStruct((n_dom * n_sub, (planes + 1) * sides, LANES), f32),
            jax.ShapeDtypeStruct((macros, 16, cells), f32),
            jax.ShapeDtypeStruct((macros, 7, rows, cells), f32),
            jax.ShapeDtypeStruct((macros, rows, cells), f32),
        ),
        scratch_shapes=[
            pltpu.VMEM((7, rows, cells), f32),
            pltpu.VMEM((macros, 2, 16, LANES), f32),
        ],
    )


class Boundary:
    def __init__(self, recv_ref, n_dom, n_sub, macros, planes):
        self.recv, self.n_dom, self.n_sub = recv_ref, n_dom, n_sub
        self.sides, self.planes = 2 * macros, planes
        self.rows = n_dom * self.sides
        self.group = group_of((self.rows, LANES))

    def rows_of(self, ref, k, at):
        n = self.sides
        return jnp.concatenate(
            [ref[d * self.n_sub + k, at * n : (at + 1) * n, :] for d in range(self.n_dom)], axis=0
        )

    def mass(self):
        return self.rows_of(self.recv, 0, self.planes)

    def fold(self, r, r_below):
        total = jnp.where(self.group == 0, packed_behind(r), 0.0) - r
        if r_below is not None:
            total = total + jnp.where(self.group == 1, r_below, 0.0)
            total = total + jnp.where(self.group == 2, packed_behind(r_below), 0.0)
        return lane_roll(total, 24) + lane_roll(total, 16) + lane_roll(total, 8)

    def layer_nodes(self, same, nodes):
        out = [None] * self.n_sub
        for start in range(0, self.n_sub, 4):
            count = min(4, self.n_sub - start)
            block = None
            for i in range(count):
                stacked = jnp.concatenate(nodes[start + i], axis=0)
                group = group_of(stacked.shape)
                moved = jnp.where(group == i, lane_roll(stacked, 8 * (i - 3)), 0.0)
                block = moved if block is None else block + moved
            summed = group_sum(same, block)
            for i in range(count):
                out[start + i] = lane_roll(summed, 8 * (3 - i))
        return out


def same_group(b, slots, recv_rows, capacity_rows):
    recv, n_sub, planes, sides = b.recv, b.n_sub, b.planes, b.sides
    index = b.rows_of(recv, 3, planes)
    lane = iota(index.shape, 1)
    side = iota(index.shape, 0) % sides
    flat = []
    for p in range(planes):
        slot = side * planes + p
        at = 32 * (slot >> 3) + (slot & 7)
        flat.append(jnp.sum(jnp.where(lane == at, index, 0.0), axis=1, keepdims=True))
    flat = jnp.concatenate(flat, axis=0).astype(jnp.int32)
    total = flat.shape[0]
    owner = flat // recv_rows
    receive = flat - owner * recv_rows
    table = jnp.zeros((total, LANES), jnp.float32)
    for e in range(b.n_dom):
        row = recv[e * n_sub + 3, planes * sides : planes * sides + 1, :]
        table = jnp.where(owner == e, jnp.broadcast_to(row, (total, LANES)), table)
    at = 32 * (receive >> 3) + (receive & 7) + 8
    key = jnp.sum(jnp.where(iota((total, LANES), 1) == at, table, 0.0), axis=1, keepdims=True)
    square = (total, total)
    key_row = jnp.sum(jnp.where(iota(square, 0) == iota(square, 1), key, 0.0), axis=0, keepdims=True)
    return jnp.where(key == key_row, 1.0, 0.0).astype(jnp.bfloat16)


def second_kernel(n_dom, n_sub, macros, planes, cells, slots, recv_rows):
    rows = planes + 2 * HALO
    sides = 2 * macros
    total = n_dom * slots
    depth = n_sub * planes

    def body(recv_ref, source_ref, low_ref, high_ref, coef_ref, w_ref, nw_ref, pay_ref, same_ref, base_ref, dw_ref, e2_ref, c1_ref, c2_ref, sh_ref, own_ref, turn_ref, sx_ref, hold_ref):
        k = lax.axis_index("sub")
        d = lax.axis_index("dom")
        b = Boundary(recv_ref, n_dom, n_sub, macros, planes)
        same_ref[...] = same_group(b, slots, recv_rows, None)
        same = same_ref[...]
        group = b.group
        extra_e = b.rows_of(recv_ref, 1, planes)
        extra_n = b.rows_of(recv_ref, 2, planes)
        inner = jnp.where(group == 3, lane_roll(extra_n, 16), extra_e)
        lowest = jnp.where(
            group == 0, extra_n, jnp.where(group == 3, lane_roll(extra_n, 8), extra_e)
        )
        damp = jnp.where(group_of((total, LANES)) == 3, NODE_DAMPING, EDGE_DAMPING)
        dw_ref[0] = damp / group_sum(same, jnp.concatenate([lowest] + [inner] * (planes - 1), axis=0))
        dw_ref[1] = damp / group_sum(same, jnp.concatenate([inner] * planes, axis=0))
        mass = b.mass()
        n = b.rows
        sh_ref[...] = jnp.zeros_like(sh_ref)
        nodes = [[None] * planes for _ in range(n_sub)]
        below = None
        for layer in range(n_sub):
            stacked = jnp.concatenate([b.rows_of(recv_ref, layer, p) for p in range(planes)], axis=0)
            e1 = group_sum(same, stacked) * dw_ref[min(layer, 1)]
            for p in range(planes):
                at = layer * planes + p
                src = stacked[p * n : (p + 1) * n]
                e1_p = e1[p * n : (p + 1) * n]
                sh_ref[HALO + at] = e1_p
                r = jnp.where(group < 3, src - mass * e1_p, 0.0)
                node = src + b.fold(r, below)
                if p == 0 and layer > 0:
                    node = node + b.rows_of(recv_ref, layer - 1, planes)
                nodes[layer][p] = node
                below = r
        summed = b.layer_nodes(same, nodes)
        above = None
        for layer in reversed(range(n_sub)):
            c1 = summed[layer] * dw_ref[min(layer, 1)]
            for p in reversed(range(planes)):
                at = layer * planes + p
                c = jnp.where(group == 3, c1[p * n : (p + 1) * n], 0.0)
                e1_p = sh_ref[HALO + at]
                sh_ref[HALO + at] = jnp.where(group == 3, c, e1_p)
                up = jnp.zeros_like(c) if above is None else above
                rise = lane_roll(packed_ahead(c) - c, -24)
                rise = jnp.where(group == 1, lane_roll(up - c, -16), rise)
                rise = jnp.where(group == 2, lane_roll(packed_ahead(up) - c, -8), rise)
                base_ref[at] = jnp.where(group < 3, e1_p + rise, 0.0)
                above = c
        for i in range(rows):
            own_ref[i] = sh_ref[k * planes + i, pl.ds(pl.multiple_of(d * sides, sides), sides), :]
        for ms in range(sides):
            turn_ref[ms] = own_ref[:, ms, :]
        plane = Plane((rows, cells))
        _, valid = plane_flags("sub", planes, HALO, cells)

        def macro_step(m, carry):
            def coef(i):
                return jnp.broadcast_to(coef_ref[m, i : i + 1, :], (rows, cells))

            own = [turn_ref[2 * m], turn_ref[2 * m + 1]]
            e1, r1 = [], []
            for t in range(7):
                sx_ref[t, 0:HALO, :] = low_ref[m, t]
                sx_ref[t, HALO : HALO + planes, :] = source_ref[m, t]
                sx_ref[t, HALO + planes : rows, :] = high_ref[m, t]
            for t in range(7):
                value = w_ref[m, t] * sx_ref[t]
                if t in SHARED_TYPES:
                    value = unpack(own, SHARED_TYPES.index(t), value)
                e1.append(value)
                r1.append(sx_ref[t] - coef(t) * value)
            c1 = jnp.where(valid, nw_ref[m] * node_back(r1, plane), 0.0)
            c1 = unpack(own, 3, c1)
            c1_ref[m] = c1
            grad = node_grad(c1, plane)
            curled = curl_curl(e1, [coef(8 + f) for f in range(8)], plane, valid)
            res, left = [], []
            for t in range(7):
                g = jnp.where(valid, grad[t], 0.0)
                res_t = jnp.where(valid, r1[t] - curled[t] - coef(t) * g, 0.0)
                e2 = e1[t] + g + w_ref[m, t] * res_t
                left_t = sx_ref[t] - coef(t) * e2
                if t in SHARED_TYPES:
                    e2 = jnp.where(plane.side, 0.0, e2)
                    left_t = jnp.where(plane.side, 0.0, left_t)
                    res.append(res_t)
                left.append(left_t)
                e2_ref[m, t] = e2[HALO : HALO + planes]
            node = node_back(left, plane)
            c2_ref[m] = jnp.where(valid, nw_ref[m] * node, 0.0)
            for s, x_at in enumerate(XS):
                hold_ref[m, s] = pack(res + [node], x_at)
            return carry

        lax.fori_loop(0, macros, macro_step, 0)
        for m in range(macros):
            for s in range(2):
                ms = 2 * m + s
                for p in range(planes):
                    pay_ref[0, p * sides + ms : p * sides + ms + 1, :] = hold_ref[m, s, HALO + p : HALO + p + 1, :]
        block = pay_ref[0]
        for dest in range(1, n_dom * n_sub):
            pay_ref[dest] = block

    f32 = jnp.float32
    n = n_dom * sides
    return pl.pallas_call(
        body,
        name="second",
        out_shape=(
            jax.ShapeDtypeStruct((n_dom * n_sub, planes * sides, LANES), f32),
            jax.ShapeDtypeStruct((total, total), jnp.bfloat16),
            jax.ShapeDtypeStruct((depth, n, LANES), f32),
            jax.ShapeDtypeStruct((2, total, LANES), f32),
            jax.ShapeDtypeStruct((macros, 7, planes, cells), f32),
            jax.ShapeDtypeStruct((macros, rows, cells), f32),
            jax.ShapeDtypeStruct((macros, rows, cells), f32),
        ),
        scratch_shapes=[
            pltpu.VMEM((depth + 2 * HALO, n, LANES), f32),
            pltpu.VMEM((rows, sides, LANES), f32),
            pltpu.VMEM((sides, rows, LANES), f32),
            pltpu.VMEM((7, rows, cells), f32),
            pltpu.VMEM((macros, 2, rows, LANES), f32),
        ],
    )


def third_kernel(n_dom, n_sub, macros, planes, cells, slots, recv_rows):
    rows = planes + 2 * HALO
    sides = 2 * macros
    depth = n_sub * planes

    def body(recv_ref, first_ref, same_ref, base_ref, dw_ref, e2_ref, c1_ref, c2_ref, edge_ref, pot_ref, sh_ref, own_ref, turn_ref):
        k = lax.axis_index("sub")
        d = lax.axis_index("dom")
        b = Boundary(first_ref, n_dom, n_sub, macros, planes)
        same = same_ref[...]
        group = b.group
        mass = b.mass()
        n = b.rows
        sh_ref[...] = jnp.zeros_like(sh_ref)
        nodes = [[None] * planes for _ in range(n_sub)]
        below = None
        for layer in range(n_sub):
            stacked = jnp.concatenate([b.rows_of(recv_ref, layer, p) for p in range(planes)], axis=0)
            step = group_sum(same, stacked) * dw_ref[min(layer, 1)]
            for p in range(planes):
                at = layer * planes + p
                e2_p = base_ref[at] + step[p * n : (p + 1) * n]
                sh_ref[HALO + at] = e2_p
                src = b.rows_of(first_ref, layer, p)
                r = jnp.where(group < 3, src - mass * e2_p, 0.0)
                nodes[layer][p] = stacked[p * n : (p + 1) * n] + b.fold(r, below)
                below = r
        summed = b.layer_nodes(same, nodes)
        for layer in range(n_sub):
            c2 = summed[layer] * dw_ref[min(layer, 1)]
            for p in range(planes):
                at = HALO + layer * planes + p
                sh_ref[at] = jnp.where(group == 3, c2[p * n : (p + 1) * n], sh_ref[at])
        for i in range(rows):
            own_ref[i] = sh_ref[k * planes + i, pl.ds(pl.multiple_of(d * sides, sides), sides), :]
        for ms in range(sides):
            turn_ref[ms] = own_ref[:, ms, :]
        plane = Plane((rows, cells))

        def macro_step(m, carry):
            own = [turn_ref[2 * m], turn_ref[2 * m + 1]]
            c2 = unpack(own, 3, c2_ref[m])
            pot_ref[m] = (c1_ref[m] + c2)[HALO : HALO + planes]
            grad = node_grad(c2, plane)
            for t in range(7):
                g = grad[t]
                if t in SHARED_TYPES:
                    zero = jnp.zeros((rows, cells), jnp.float32)
                    g = g + unpack(own, SHARED_TYPES.index(t), zero)
                edge_ref[m, t] = e2_ref[m, t] + g[HALO : HALO + planes]
            return carry

        lax.fori_loop(0, macros, macro_step, 0)

    f32 = jnp.float32
    n = n_dom * sides
    return pl.pallas_call(
        body,
        name="third",
        out_shape=(
            jax.ShapeDtypeStruct((macros, 7, planes, cells), f32),
            jax.ShapeDtypeStruct((macros, planes, cells), f32),
        ),
        scratch_shapes=[
            pltpu.VMEM((depth + 2 * HALO, n, LANES), f32),
            pltpu.VMEM((rows, sides, LANES), f32),
            pltpu.VMEM((sides, rows, LANES), f32),
        ],
    )


def local_small(source, zone_ids, kappa_table, mu_table, owner_dev, owner_group):
    macros, _, planes, cells = source.shape
    n_dom, n_sub = lax.axis_size("dom"), lax.axis_size("sub")
    sizes = (n_dom, n_sub, macros, planes, cells, owner_dev.shape[1], owner_group.shape[1])
    table = jnp.zeros((16, kappa_table.shape[0]), jnp.float32)
    table = table.at[0:7].set(kappa_table.T).at[8:16].set(mu_table.T)
    up = [(i, i + 1) for i in range(n_sub - 1)]
    down = [(i + 1, i) for i in range(n_sub - 1)]
    low = lax.ppermute(source[:, :, planes - HALO :], "sub", up)
    high = lax.ppermute(source[:, :, :HALO], "sub", down)
    pay, coef, w, nw = first_kernel(*sizes)(zone_ids, table, source, owner_dev, owner_group)
    everyone = ("dom", "sub")
    recv = lax.all_to_all(pay, everyone, 0, 0)
    pay, same, base, dw, e2, c1, c2 = second_kernel(*sizes)(recv, source, low, high, coef, w, nw)
    again = lax.all_to_all(pay, everyone, 0, 0)
    return third_kernel(*sizes)(again, recv, same, base, dw, e2, c1, c2)


def fits_small(mesh, source, owner_dev, owner_group):
    macros = source.shape[0] // mesh.shape["dom"]
    planes = source.shape[2] // mesh.shape["sub"]
    return (
        macros == 4
        and planes == 4
        and source.shape[3] == LAT * LAT
        and mesh.shape["sub"] == 4
        and owner_dev.shape[1] == 2 * macros * planes
        and owner_group.shape[1] == 32
        and mesh.shape["dom"] <= 8
    )


def solution(mesh):
    in_specs = (
        P("dom", None, "sub", None),
        P("dom", None),
        P(),
        P(),
        P("dom", None),
        P("dom", None),
    )
    out_specs = (P("dom", None, "sub", None), P("dom", "sub", None))

    def step(source, zone_ids, kappa_table, mu_table, owner_dev, owner_group):
        body = local_small if fits_small(mesh, source, owner_dev, owner_group) else local
        mapped = jax.shard_map(
            body, mesh=mesh, in_specs=in_specs, out_specs=out_specs, check_vma=False
        )
        return mapped(source, zone_ids, kappa_table, mu_table, owner_dev, owner_group)

    return step
```

```python
import jax
import jax.numpy as jnp
from jax import lax
from jax.experimental import pallas as pl
from jax.experimental.pallas import tpu as pltpu
from jax.sharding import PartitionSpec as P


LAT = 32
SWEEPS = 2


EDGE_OFFSETS = ((0, 0, 1), (0, 1, 0), (1, 0, 0), (0, 1, 1), (1, 0, 1), (1, 1, 0), (1, 1, 1))
FACE_EDGES = (
    (0, 1, 3),
    (1, 0, 3),
    (0, 2, 4),
    (2, 0, 4),
    (1, 2, 5),
    (2, 1, 5),
    (3, 2, 6),
    (2, 3, 6),
)
SHARED_TYPES = (1, 2, 5)
EDGE_DAMPING = 0.6
NODE_DAMPING = 0.8


def with_halo(block, sides, width):
    for axis, dim in sides:
        count = lax.axis_size(axis)
        forward = [(i, i + 1) for i in range(count - 1)]
        backward = [(target, source) for source, target in forward]
        low = lax.ppermute(
            lax.slice_in_dim(block, block.shape[dim] - width, None, axis=dim), axis, forward
        )
        high = lax.ppermute(lax.slice_in_dim(block, 0, width, axis=dim), axis, backward)
        block = jnp.concatenate([low, block, high], axis=dim)
    return block


def from_behind(block, axis, distance):
    devices = range(lax.axis_size(axis))
    route = [(i - distance, i) for i in devices if i - distance in devices]
    return lax.ppermute(block, axis, route)


def shift_ahead(values, rise_y, rise_x):
    offset = rise_y * LAT + rise_x
    if offset == 0:
        return values
    padding = jnp.zeros(values.shape[:-1] + (offset,), values.dtype)
    shifted = jnp.concatenate([values[..., offset:], padding], axis=-1)
    if rise_x:
        column = jnp.arange(values.shape[-1]) % LAT
        shifted = jnp.where(column < LAT - rise_x, shifted, jnp.zeros_like(shifted))
    return shifted


def shift_behind(values, rise_y, rise_x):
    offset = rise_y * LAT + rise_x
    if offset == 0:
        return values
    padding = jnp.zeros(values.shape[:-1] + (offset,), values.dtype)
    shifted = jnp.concatenate([padding, values[..., :-offset]], axis=-1)
    if rise_x:
        column = jnp.arange(values.shape[-1]) % LAT
        shifted = jnp.where(column >= rise_x, shifted, jnp.zeros_like(shifted))
    return shifted


def apply_operator(padded, halo_width, extra_planes, first_plane, mass_coef, curl_coef):
    planes = padded.shape[2] - 2 * halo_width
    face_count = planes + extra_planes + 1
    first_face = halo_width - extra_planes - 1
    face_planes = first_plane - extra_planes - 1 + jnp.arange(face_count)
    face_valid = (face_planes >= 0)[None, :, None]
    result = [
        mass_coef[edge_type][:, None, :]
        * padded[:, edge_type, halo_width - extra_planes : halo_width + planes]
        for edge_type in range(7)
    ]
    for face_index, (first_edge, second_edge, diagonal_edge) in enumerate(FACE_EDGES):
        rise_z, rise_y, rise_x = EDGE_OFFSETS[first_edge]
        far_values = shift_ahead(
            padded[:, second_edge, first_face + rise_z : first_face + rise_z + face_count],
            rise_y,
            rise_x,
        )
        circulation = (
            padded[:, first_edge, first_face : first_face + face_count]
            + far_values
            - padded[:, diagonal_edge, first_face : first_face + face_count]
        )
        weighted = jnp.where(face_valid, curl_coef[face_index][:, None, :] * circulation, 0.0)
        result[first_edge] = result[first_edge] + weighted[:, 1:]
        result[diagonal_edge] = result[diagonal_edge] - weighted[:, 1:]
        result[second_edge] = result[second_edge] + shift_behind(
            weighted[:, 1 - rise_z : 1 - rise_z + planes + extra_planes], rise_y, rise_x
        )
    return jnp.stack(result, axis=1)


def edge_diagonal(mass_coef, curl_coef, first_plane, planes):
    inside = (first_plane + jnp.arange(planes) >= 1)[None, :, None]
    flat_planes = jnp.zeros((1, planes, 1), mass_coef.dtype)
    diagonal = [mass_coef[edge_type][:, None, :] + flat_planes for edge_type in range(7)]
    for face_index, (first_edge, second_edge, diagonal_edge) in enumerate(FACE_EDGES):
        rise_z, rise_y, rise_x = EDGE_OFFSETS[first_edge]
        own_term = curl_coef[face_index][:, None, :]
        diagonal[first_edge] = diagonal[first_edge] + own_term
        diagonal[diagonal_edge] = diagonal[diagonal_edge] + own_term
        behind_term = shift_behind(curl_coef[face_index], rise_y, rise_x)[:, None, :] + flat_planes
        if rise_z:
            behind_term = jnp.where(inside, behind_term, 0.0)
        diagonal[second_edge] = diagonal[second_edge] + behind_term
    return jnp.stack(diagonal, axis=1)


def node_diagonal(mass_coef, first_plane, planes):
    inside = (first_plane + jnp.arange(planes) >= 1)[None, :, None]
    total = jnp.zeros((mass_coef.shape[1], planes, mass_coef.shape[2]), mass_coef.dtype)
    for edge_type in range(7):
        rise_z, rise_y, rise_x = EDGE_OFFSETS[edge_type]
        total = total + mass_coef[edge_type][:, None, :]
        behind_term = shift_behind(mass_coef[edge_type], rise_y, rise_x)[:, None, :] + jnp.zeros(
            (1, planes, 1), mass_coef.dtype
        )
        if rise_z:
            behind_term = jnp.where(inside, behind_term, 0.0)
        total = total + behind_term
    return total


def node_residual(lowered, planes):
    total = jnp.zeros((lowered.shape[0], planes, lowered.shape[3]), lowered.dtype)
    for edge_type in range(7):
        rise_z, rise_y, rise_x = EDGE_OFFSETS[edge_type]
        total = (
            total
            + shift_behind(lowered[:, edge_type, 1 - rise_z : 1 - rise_z + planes], rise_y, rise_x)
            - lowered[:, edge_type, 1:]
        )
    return total


def gradient(raised, planes):
    result = []
    for edge_type in range(7):
        rise_z, rise_y, rise_x = EDGE_OFFSETS[edge_type]
        result.append(
            shift_ahead(raised[:, rise_z : rise_z + planes], rise_y, rise_x) - raised[:, :planes]
        )
    return jnp.stack(result, axis=1)


def edge_sides(values):
    macro_count, type_count, plane_count, _ = values.shape
    lattice = values.reshape(macro_count, type_count, plane_count, LAT, LAT)
    chosen = jnp.stack([lattice[:, edge_type] for edge_type in SHARED_TYPES], axis=1)
    sides = jnp.stack([chosen[..., 0], chosen[..., LAT - 1]], axis=1)
    return jnp.transpose(sides, (0, 1, 3, 2, 4)).reshape(-1, 3 * LAT)


def insert_edges(values, blocks):
    macro_count, type_count, plane_count, _ = values.shape
    shaped = blocks.reshape(macro_count, 2, plane_count, 3, LAT)
    shaped = jnp.transpose(shaped, (0, 1, 3, 2, 4))
    lattice = values.reshape(macro_count, type_count, plane_count, LAT, LAT)
    for side_index, column in ((0, 0), (1, LAT - 1)):
        for slot_type, edge_type in enumerate(SHARED_TYPES):
            lattice = lattice.at[:, edge_type, :, :, column].set(shaped[:, side_index, slot_type])
    return lattice.reshape(values.shape)


def node_sides(values):
    macro_count, plane_count, _ = values.shape
    lattice = values.reshape(macro_count, plane_count, LAT, LAT)
    sides = jnp.stack([lattice[..., 0], lattice[..., LAT - 1]], axis=1)
    return sides.reshape(-1, LAT)


def insert_nodes(values, blocks):
    macro_count, plane_count, _ = values.shape
    shaped = blocks.reshape(macro_count, 2, plane_count, LAT)
    lattice = values.reshape(macro_count, plane_count, LAT, LAT)
    for side_index, column in ((0, 0), (1, LAT - 1)):
        lattice = lattice.at[:, :, :, column].set(shaped[:, side_index])
    return lattice.reshape(values.shape)


def local(source, zone_ids, kappa_table, mu_table, owner_dev, owner_group):
    macro_count, type_count, planes, cell_count = source.shape
    first_plane = lax.axis_index("sub") * planes
    onehot = (jnp.arange(kappa_table.shape[0])[:, None] == zone_ids.reshape(1, -1)).astype(
        jnp.float32
    )
    mass_coef = jnp.dot(kappa_table.T, onehot, precision=lax.Precision.HIGHEST).reshape(
        type_count, macro_count, cell_count
    )
    curl_coef = jnp.dot(mu_table.T, onehot, precision=lax.Precision.HIGHEST).reshape(
        mu_table.shape[1], macro_count, cell_count
    )
    peer_count = lax.axis_size("dom")
    recv_rows = owner_group.shape[1]
    capacity = recv_rows // peer_count
    slot_count = owner_dev.shape[1]
    owner_of = owner_dev[0]
    groups = owner_group[0]
    earlier = jnp.arange(slot_count)[None, :] < jnp.arange(slot_count)[:, None]
    position = jnp.sum((owner_of[:, None] == owner_of[None, :]) & earlier, axis=1)
    slot_place = owner_of * capacity + position
    spread = (jnp.arange(recv_rows)[:, None] == slot_place[None, :]).astype(jnp.float32)
    same_group = (groups[:, None] == groups[None, :]).astype(jnp.float32)

    def owner_sum(received):
        summed = jnp.dot(
            same_group, received.reshape(recv_rows, -1), precision=lax.Precision.HIGHEST
        )
        return lax.all_to_all(
            summed.reshape(peer_count, capacity, -1), "dom", split_axis=0, concat_axis=0, tiled=True
        )

    def assemble(blocks):
        outgoing = jnp.dot(spread, blocks, precision=lax.Precision.HIGHEST).reshape(
            peer_count, capacity, blocks.shape[1]
        )
        returned = owner_sum(
            lax.all_to_all(outgoing, "dom", split_axis=0, concat_axis=0, tiled=True)
        )
        return jnp.take(returned.reshape(recv_rows, -1), slot_place, axis=0)

    rim_width = 2

    def rimmed(values):
        return with_halo(values, (("sub", 2),), rim_width)

    edge_diag = edge_diagonal(mass_coef, curl_coef, first_plane, planes)
    node_diag = node_diagonal(mass_coef, first_plane, planes)
    edge_width = 3 * LAT
    first_blocks = [edge_sides(edge_diag), node_sides(node_diag)]
    diag_sums = assemble(jnp.concatenate(first_blocks, axis=1))
    full_edge_diag = insert_edges(edge_diag, diag_sums[:, :edge_width])
    full_node_diag = insert_nodes(node_diag, diag_sums[:, edge_width : edge_width + LAT])
    source_below = from_behind(source[:, :, planes - 1 :], "sub", 1)
    edge_field = jnp.zeros_like(source)
    potential = jnp.zeros((macro_count, planes, cell_count), jnp.float32)
    for sweep_index in range(SWEEPS):
        if sweep_index == 0:
            residual = source
            residual_sum = assemble(edge_sides(residual))
        else:
            residual = source - apply_operator(
                rimmed(edge_field), rim_width, 0, first_plane, mass_coef, curl_coef
            )
            residual_sum = assemble(edge_sides(residual))
        full_residual = insert_edges(residual, residual_sum)
        edge_field = edge_field + EDGE_DAMPING * full_residual / full_edge_diag
        padded = rimmed(edge_field)
        lowered = jnp.concatenate([source_below, source], axis=2) - apply_operator(
            padded, 2, 1, first_plane, mass_coef, curl_coef
        )
        node_values = node_residual(lowered, planes)
        node_sum = assemble(node_sides(node_values))
        correction = NODE_DAMPING * insert_nodes(node_values, node_sum) / full_node_diag
        plane_above = from_behind(correction[:, :1], "sub", -1)
        edge_field = edge_field + gradient(
            jnp.concatenate([correction, plane_above], axis=1), planes
        )
        potential = potential + correction
    return (edge_field, potential)


LANES = 128
HALO = 2
VMEM_BYTES = 24 * 1024 * 1024
LOOSE_TYPES = (0, 3, 4, 6)


def lane_roll(v, s):
    s = s % v.shape[-1]
    return pltpu.roll(v, s, v.ndim - 1) if s else v


def row_roll(v, s):
    s = s % v.shape[0]
    return pltpu.roll(v, s, 0) if s else v


def iota(shape, dim):
    return lax.broadcasted_iota(jnp.int32, shape, dim)


def zb(v):
    return row_roll(v, 1)


def za(v):
    return row_roll(v, -1)


class Plane:
    def __init__(self, shape):
        self.lane = iota(shape, 1)
        self.x = self.lane & (LAT - 1)
        self.cells = shape[1]
        self.side = (self.x == 0) | (self.x == LAT - 1)

    def ax(self, v):
        return jnp.where(self.x < LAT - 1, lane_roll(v, -1), 0.0)

    def ay(self, v):
        return jnp.where(self.lane < self.cells - LAT, lane_roll(v, -LAT), 0.0)

    def bx(self, v):
        return jnp.where(self.x > 0, lane_roll(v, 1), 0.0)

    def by(self, v):
        return jnp.where(self.lane >= LAT, lane_roll(v, LAT), 0.0)

    def bxy(self, v):
        return jnp.where((self.lane >= LAT) & (self.x > 0), lane_roll(v, LAT + 1), 0.0)

    def axy(self, v):
        inner = (self.lane < self.cells - LAT) & (self.x < LAT - 1)
        return jnp.where(inner, lane_roll(v, -LAT - 1), 0.0)


def yb(v):
    lane = iota(v.shape, 1)
    first = jnp.where(lane < 4, 0.0, lane_roll(v, 36))
    return jnp.where(lane < 32, first, lane_roll(v, 32))


def ya(v):
    lane = iota(v.shape, 1)
    last = jnp.where(lane >= 124, 0.0, lane_roll(v, -36))
    return jnp.where(lane >= 96, last, lane_roll(v, -32))


class Strip:
    def __init__(self, shape):
        half = shape[0] // 2
        self.col = iota(shape, 1) & 3
        self.upper = iota(shape, 0) >= half
        self.own = self.col == 0

    def ax(self, v):
        wrap = jnp.where(self.upper, lane_roll(v, 3), 0.0)
        step = jnp.where(self.upper & self.own, 0.0, lane_roll(v, -1))
        return jnp.where(self.col == 3, wrap, step)

    def bx(self, v):
        wrap = jnp.where(self.upper, lane_roll(v, -3), 0.0)
        step = jnp.where(self.upper & (self.col == 1), 0.0, lane_roll(v, 1))
        return jnp.where(self.own, wrap, step)

    def ay(self, v):
        return ya(v)

    def by(self, v):
        return yb(v)

    def bxy(self, v):
        return yb(self.bx(v))

    def axy(self, v):
        return ya(self.ax(v))


def to_strip(v):
    lane = iota((v.shape[0], LANES), 1)
    block = (lane & 31) >> 2
    low = jnp.zeros((v.shape[0], LANES), v.dtype)
    high = low
    for c in range(8):
        column = v[:, LANES * c : LANES * (c + 1)]
        low = jnp.where(block == c, lane_roll(column, 4 * c), low)
        high = jnp.where(block == c, lane_roll(column, 4 * c - 28), high)
    high = jnp.where((lane & 3) == 0, lane_roll(high, -3), lane_roll(high, 1))
    return jnp.concatenate([low, high], axis=0)


def plus(*terms):
    total = None
    for term in terms:
        if term is not None:
            total = term if total is None else total + term
    return total


def on(f, v):
    return None if v is None else f(v)


def minus(v):
    return on(lambda a: -a, v)


def times(c, v):
    return on(lambda a: c * a, v)


def table_lookup(zone, table_ref, width):
    out = [jnp.zeros(zone.shape, jnp.float32)] * width
    for z in range(table_ref.shape[1]):
        hit = zone == z
        out = [jnp.where(hit, table_ref[i, z], v) for i, v in enumerate(out)]
    return out


def diagonals(mass, mu, sh):
    flat = [
        mass[0] + mu[0] + mu[2] + sh.by(mu[1]),
        mass[1] + mu[1] + mu[4] + sh.bx(mu[0]),
        mass[2] + mu[3] + mu[5] + mu[7] + sh.bx(mu[2]) + sh.by(mu[4]) + sh.bxy(mu[6]),
        mass[3] + mu[0] + mu[1] + mu[6],
        mass[4] + mu[2] + mu[3],
        mass[5] + mu[4] + mu[5],
        mass[6] + mu[6] + mu[7],
    ]
    rise = {0: mu[3], 1: mu[5], 3: mu[7]}
    node_flat = sh.bx(mass[0]) + sh.by(mass[1]) + sh.bxy(mass[3])
    for t in range(7):
        node_flat = node_flat + mass[t]
    node_rise = mass[2] + sh.bx(mass[4]) + sh.by(mass[5]) + sh.bxy(mass[6])
    return flat, rise, node_flat, node_rise


def grad_at(c, c_up, sh, types=range(7)):
    moves = (sh.ax, sh.ay, lambda v: v, sh.axy, sh.ax, sh.ay, sh.axy)
    out = [None] * 7
    for t in types:
        out[t] = plus(on(moves[t], c_up if EDGE_OFFSETS[t][0] else c), minus(c))
    return out


def back_at(r, r_below, sh):
    return plus(
        minus(plus(*r)),
        r_below[2],
        on(sh.bx, plus(r[0], r_below[4])),
        on(sh.by, plus(r[1], r_below[5])),
        on(sh.bxy, plus(r[3], r_below[6])),
    )


NONE7 = [None] * 7


def first_kernel(n_dom, n_sub, macros, planes, cells):
    sides = 2 * macros
    blocks = 2 * planes

    def body(kappa_ref, mu_ref, zone_ref, source_ref, pay_ref, coef_ref, hold_ref):
        k = lax.axis_index("sub")
        shape = (sides, LANES)
        sh = Strip(shape)
        row = iota(shape, 0)
        group = iota(shape, 1) & 3
        zone = to_strip(zone_ref[...])
        mass = table_lookup(zone, kappa_ref, 7)
        mu = table_lookup(zone, mu_ref, 8)
        flat, rise, node_flat, node_rise = diagonals(mass, mu, sh)
        w = [EDGE_DAMPING / (flat[t] + rise[t] if t in rise else flat[t]) for t in range(7)]
        w_low = [EDGE_DAMPING / flat[t] if t in rise else w[t] for t in range(7)]
        lowest = k == 0
        w_zero = [jnp.where(lowest, w_low[t], w[t]) for t in range(7)]
        nw = NODE_DAMPING / (node_flat + node_rise)
        nw_zero = jnp.where(lowest, NODE_DAMPING / node_flat, nw)
        for i, v in enumerate(mass + mu + w + w_zero + [nw, nw_zero]):
            coef_ref[i] = v
        has_below = jnp.where(lowest, 0.0, 1.0)
        has_above = jnp.where(k == n_sub - 1, 0.0, 1.0)

        def loose(t, v):
            return jnp.where(sh.own, 0.0, v) if t in SHARED_TYPES else v

        def flagged(p, v):
            flag = has_below if p < 0 else has_above if p >= planes else None
            return v if flag is None or v is None else v * flag

        src = {p: [to_strip(source_ref[:, t, p, :]) for t in range(7)] for p in range(planes)}
        e1, r1 = {}, {}
        for p in range(planes):
            wp = w_zero if p == 0 else w
            e1[p] = [loose(t, wp[t] * src[p][t]) for t in range(7)]
            r1[p] = [loose(t, src[p][t] - mass[t] * e1[p][t]) for t in range(7)]
        n1, c1 = {}, {}
        for p in range(planes + 1):
            n1[p] = back_at(r1.get(p, NONE7), r1.get(p - 1, NONE7), sh)
            c1[p] = jnp.where(sh.own, 0.0, (nw_zero if p == 0 else nw) * n1[p])
            c1[p] = flagged(p, c1[p])
        faces = {}
        for p in range(-1, planes):
            e, e_up = e1.get(p, NONE7), e1.get(p + 1, NONE7)
            far = (
                on(sh.ax, e[1]),
                on(sh.ay, e[0]),
                on(sh.ax, e[2]),
                e_up[0],
                on(sh.ay, e[2]),
                e_up[1],
                on(sh.axy, e[2]),
                e_up[3],
            )
            faces[p] = [
                flagged(p, times(mu[f], plus(e[a], far[f], minus(e[g]))))
                for f, (a, _, g) in enumerate(FACE_EDGES)
            ]
        res, r2 = {}, {}
        none8 = [None] * 8
        for p in range(-1, planes + 1):
            f, f_below = faces.get(p, none8), faces.get(p - 1, none8)
            curled = [
                plus(f[0], f[2], on(sh.by, f[1]), f_below[3]),
                plus(f[1], f[4], on(sh.bx, f[0]), f_below[5]),
                plus(f[3], f[5], f[7], on(sh.bx, f[2]), on(sh.by, f[4]), on(sh.bxy, f[6])),
                plus(f[6], f_below[7], minus(f[0]), minus(f[1])),
                minus(plus(f[2], f[3])),
                minus(plus(f[4], f[5])),
                minus(plus(f[6], f[7])),
            ]
            grad = grad_at(c1.get(p), c1.get(p + 1), sh)
            wp = w_zero if p == 0 else w
            res[p], r2[p] = [], []
            for t in range(7):
                g = grad[t]
                value = plus(
                    r1.get(p, NONE7)[t], minus(curled[t]), minus(times(mass[t], g))
                )
                res[p].append(value)
                e2 = plus(e1.get(p, NONE7)[t], g, times(wp[t], value))
                s = src[p][t] if p in src else None
                left = flagged(p, plus(s, minus(times(mass[t], e2))))
                r2[p].append(on(lambda v: loose(t, v), left))
        n2 = {p: back_at(r2.get(p, NONE7), r2.get(p - 1, NONE7), sh) for p in range(-1, planes + 2)}

        def merge(g0, g1, g2, g3):
            out = jnp.where(group == 1, lane_roll(g1, 1), g0)
            out = jnp.where(group == 2, lane_roll(g2, 2), out)
            return jnp.where(group == 3, lane_roll(g3, 3), out)

        high = jnp.where(row < macros, row_roll(n2[planes + 1], macros), n1[planes])
        spare = [flagged(-1, res[-1][2]), high, n2[-1], n2[planes]]
        for p in range(planes):
            hold_ref[p * sides : (p + 1) * sides, :] = merge(src[p][1], src[p][2], src[p][5], n1[p])
            at = planes + p
            hold_ref[at * sides : (at + 1) * sides, :] = merge(res[p][1], res[p][2], spare[p], n2[p])
        block = hold_ref[...]
        for dest in range(n_dom * n_sub):
            pay_ref[dest] = block

    f32 = jnp.float32
    smem = pl.BlockSpec(memory_space=pltpu.SMEM)
    vmem = pl.BlockSpec(memory_space=pltpu.VMEM)
    return pl.pallas_call(
        body,
        compiler_params=pltpu.CompilerParams(vmem_limit_bytes=VMEM_BYTES),
        name="first",
        in_specs=[smem, smem, vmem, vmem],
        out_shape=(
            pltpu.VMEM((n_dom * n_sub, blocks * sides, LANES), f32),
            pltpu.VMEM((31, sides, LANES), f32),
        ),
        scratch_shapes=[pltpu.VMEM((blocks * sides, LANES), f32)],
    )


def label_kernel(n_dom, n_sub, macros, planes, cells, slots, recv_rows):
    sides = 2 * macros
    capacity = recv_rows // n_dom

    def body(zone_ref, owner_ref, group_ref, pay_ref):
        d = lax.axis_index("dom")
        shape = (sides, LANES)
        row = iota(shape, 0)
        group = iota(shape, 1) & 3
        owner = owner_ref[...].astype(jnp.float32)
        si, sj = iota((slots, slots), 0), iota((slots, slots), 1)
        column = jnp.sum(jnp.where(si == sj, owner, 0.0), axis=1, keepdims=True)
        lower = jnp.where((column == owner) & (si < sj), 1.0, 0.0)
        position = jnp.sum(lower, axis=0, keepdims=True)
        flat_index = owner * recv_rows + (d * capacity).astype(jnp.float32) + position
        keyed = group_ref[...].astype(jnp.float32) + (d * recv_rows).astype(jnp.float32)

        def spread_lanes(values):
            count = values.shape[1]
            place = iota((count, LANES), 0)
            place = 32 * (place >> 3) + 4 * (place & 7) + 3
            hot = jnp.where(place == iota((count, LANES), 1), 1.0, 0.0)
            rows = jnp.broadcast_to(values, (sides, count))
            return jnp.dot(rows, hot, precision=lax.Precision.HIGHEST)

        index = jnp.where(row < macros, spread_lanes(flat_index), spread_lanes(keyed))
        zone = to_strip(zone_ref[...]).astype(jnp.float32)
        block = jnp.where(group == 2, lane_roll(zone, -1), lane_roll(zone, 1))
        block = jnp.where(group == 3, index, block)
        pay_ref[...] = block

    return pl.pallas_call(
        body,
        compiler_params=pltpu.CompilerParams(vmem_limit_bytes=VMEM_BYTES),
        name="label",
        out_shape=pltpu.VMEM((sides, LANES), jnp.float32),
    )


def inner_kernel(n_dom, n_sub, macros, planes, cells):
    rows = planes + 2 * HALO

    def body(kappa_ref, mu_ref, zone_ref, source_ref, low_ref, high_ref, edge_ref, pot_ref, coef_ref, sx_ref, w_ref):
        k = lax.axis_index("sub")
        sh = Plane((rows, cells))
        at = k * planes - HALO + iota((rows, cells), 0)
        inside, valid = at >= 1, (at >= 0) & (at < n_sub * planes)
        zones = zone_ref[...]
        for i, v in enumerate(table_lookup(zones, kappa_ref, 7) + table_lookup(zones, mu_ref, 8)):
            coef_ref[i] = v

        def macro_step(m, carry):
            def coef(i):
                return jnp.broadcast_to(coef_ref[i, pl.ds(m, 1), :], (rows, cells))

            mass = [coef(t) for t in range(7)]
            mu = [coef(7 + f) for f in range(8)]
            flat, rise, node_flat, node_rise = diagonals(mass, mu, sh)
            for t in range(7):
                diag = flat[t]
                if t in rise:
                    diag = diag + jnp.where(inside, rise[t], 0.0)
                w_ref[t] = EDGE_DAMPING / diag
            w_ref[7] = NODE_DAMPING / (node_flat + jnp.where(inside, node_rise, 0.0))
            node_open = valid & jnp.logical_not(sh.side)

            def loose(t, v):
                return jnp.where(sh.side, 0.0, v) if t in SHARED_TYPES else v

            def node_back(r):
                own = -(((r[0] + r[1]) + (r[2] + r[3])) + ((r[4] + r[5]) + r[6]))
                back = zb(r[2]) + sh.bx(r[0] + zb(r[4])) + sh.by(r[1] + zb(r[5]))
                return jnp.where(node_open, w_ref[7] * (own + back + sh.bxy(r[3] + zb(r[6]))), 0.0)

            def node_grad(c):
                cx, cy, cxy = sh.ax(c), sh.ay(c), sh.axy(c)
                ends = (cx, cy, za(c), cxy, za(cx), za(cy), za(cxy))
                return [jnp.where(valid, end - c, 0.0) for end in ends]

            e, r1 = [], []
            for t in range(7):
                sx_ref[t, 0:HALO, :] = low_ref[m, t]
                sx_ref[t, HALO : HALO + planes, :] = source_ref[m, t]
                sx_ref[t, HALO + planes : rows, :] = high_ref[m, t]
            for t in range(7):
                e.append(loose(t, w_ref[t] * sx_ref[t]))
                r1.append(loose(t, sx_ref[t] - mass[t] * e[t]))
            c1 = node_back(r1)
            grad = node_grad(c1)
            far = (
                sh.ax(e[1]),
                sh.ay(e[0]),
                sh.ax(e[2]),
                za(e[0]),
                sh.ay(e[2]),
                za(e[1]),
                sh.axy(e[2]),
                za(e[3]),
            )
            f = [
                jnp.where(valid, mu[i] * (e[a] + far[i] - e[g]), 0.0)
                for i, (a, _, g) in enumerate(FACE_EDGES)
            ]
            curled = [
                f[0] + f[2] + sh.by(f[1]) + zb(f[3]),
                f[1] + f[4] + sh.bx(f[0]) + zb(f[5]),
                f[3] + f[5] + f[7] + sh.bx(f[2]) + sh.by(f[4]) + sh.bxy(f[6]),
                f[6] + zb(f[7]) - f[0] - f[1],
                -f[2] - f[3],
                -f[4] - f[5],
                -f[6] - f[7],
            ]
            e2, left = [], []
            for t in range(7):
                res = r1[t] - curled[t] - mass[t] * grad[t]
                value = jnp.where(valid, loose(t, e[t] + grad[t] + w_ref[t] * res), 0.0)
                e2.append(value)
                left.append(loose(t, sx_ref[t] - mass[t] * value))
            c2 = node_back(left)
            grad = node_grad(c2)
            for t in range(7):
                edge_ref[m, t] = (e2[t] + grad[t])[HALO : HALO + planes]
            pot_ref[m] = (c1 + c2)[HALO : HALO + planes]
            return carry

        lax.fori_loop(0, macros, macro_step, 0)

    f32 = jnp.float32
    smem = pl.BlockSpec(memory_space=pltpu.SMEM)
    vmem = pl.BlockSpec(memory_space=pltpu.VMEM)
    return pl.pallas_call(
        body,
        compiler_params=pltpu.CompilerParams(vmem_limit_bytes=VMEM_BYTES),
        name="inner",
        in_specs=[smem, smem, vmem, vmem, vmem, vmem],
        out_shape=(
            pltpu.VMEM((macros, 7, planes, cells), f32),
            pltpu.VMEM((macros, planes, cells), f32),
        ),
        scratch_shapes=[
            pltpu.VMEM((15, macros, cells), f32),
            pltpu.VMEM((7, rows, cells), f32),
            pltpu.VMEM((8, rows, cells), f32),
        ],
    )


def group_sum(same, block):
    parts = []
    rest = block
    for _ in range(3):
        parts.append(rest.astype(jnp.bfloat16))
        rest = rest - parts[-1].astype(jnp.float32)
    wide = jnp.concatenate([same] * 3, axis=1)
    return jnp.dot(wide, jnp.concatenate(parts, axis=0), preferred_element_type=jnp.float32)


def prepare_kernel(n_dom, n_sub, macros, planes, cells, slots, recv_rows):
    sides = 2 * macros
    n = n_dom * sides
    total = n * planes

    def body(kappa_ref, mu_ref, *refs):
        same_ref, weight_ref, field_ref, recv_ref = refs[n_dom + 1 :]
        d = lax.axis_index("dom")
        for i in range(n_dom):
            recv_ref[d ^ i] = refs[i][...]
        shape = (n, LANES)
        group = iota(shape, 1) & 3
        index = jnp.concatenate([recv_ref[e] for e in range(n_dom)], axis=0)
        lane = iota(shape, 1)
        row = iota(shape, 0) % sides
        firsts = []
        for e in range(n_dom):
            one = recv_ref[e, 0:1, :]
            firsts.append(jnp.broadcast_to(one, (sides, LANES)))
        firsts = jnp.concatenate(firsts, axis=0)
        flat = []
        for p in range(planes):
            slot = (2 * (row % macros) + row // macros) * planes + p
            here = lane == 32 * (slot >> 3) + 4 * (slot & 7) + 3
            flat.append(jnp.sum(jnp.where(here, firsts, 0.0), axis=1, keepdims=True))
        flat = jnp.concatenate(flat, axis=0).astype(jnp.int32)
        owner = flat // recv_rows
        receive = flat - owner * recv_rows
        table = jnp.zeros((total, LANES), jnp.float32)
        for e in range(n_dom):
            one = recv_ref[e, macros : macros + 1, :]
            table = jnp.where(owner == e, jnp.broadcast_to(one, (total, LANES)), table)
        here = iota((total, LANES), 1) == 32 * (receive >> 3) + 4 * (receive & 7) + 3
        key = jnp.sum(jnp.where(here, table, 0.0), axis=1, keepdims=True)
        square = (total, total)
        diagonal = iota(square, 0) == iota(square, 1)
        key_row = jnp.sum(jnp.where(diagonal, key, 0.0), axis=0, keepdims=True)
        same = jnp.where(key == key_row, 1.0, 0.0).astype(jnp.bfloat16)

        zone = index.astype(jnp.int32)
        mass = table_lookup(zone, kappa_ref, 7)
        mu = table_lookup(zone, mu_ref, 8)
        upper = (iota(shape, 0) % sides) >= macros

        def near(v):
            return jnp.where(upper, lane_roll(v, -1), 0.0)

        def place(*fields):
            out = jnp.zeros(shape, jnp.float32)
            for g, field in enumerate(fields):
                if field is not None:
                    out = jnp.where(group == g, lane_roll(field, g - 1), out)
            return out

        near_mu = [near(v) for v in mu]
        near_mass = [near(v) for v in mass]
        edge_mass = place(mass[1], mass[2], mass[5])
        e1_low = mass[1] + mu[1] + mu[4] + near_mu[0]
        e2_diag = mass[2] + mu[3] + mu[5] + mu[7] + near_mu[2] + yb(mu[4]) + yb(near_mu[6])
        e5_diag = mass[5] + mu[4] + mu[5]
        node_low = near_mass[0] + yb(mass[1]) + yb(near_mass[3])
        for t in range(7):
            node_low = node_low + mass[t]
        node_diag = node_low + mass[2] + near_mass[4] + yb(mass[5]) + yb(near_mass[6])
        self_coef = place(mu[1] + near_mu[0], mu[3] + mu[7] + near_mu[2] + yb(near_mu[6]))
        cross_coef = place(mu[4], mu[5])

        def loose_terms(low):
            diag = {
                0: mass[0] + mu[0] + mu[2] + yb(mu[1]),
                3: mass[3] + mu[0] + mu[1] + mu[6],
                4: mass[4] + mu[2] + mu[3],
                6: mass[6] + mu[6] + mu[7],
            }
            if not low:
                diag[0] = diag[0] + mu[3]
                diag[3] = diag[3] + mu[7]
            al = {t: mass[t] * (EDGE_DAMPING / diag[t]) for t in LOOSE_TYPES}
            be = {t: mass[t] * (1.0 - al[t]) for t in LOOSE_TYPES}
            al_n = {t: near(al[t]) for t in LOOSE_TYPES}
            be_n = {t: near(be[t]) for t in LOOSE_TYPES}
            p0 = al[3] * mu[1] + al_n[0] * near_mu[0]
            r0 = -al[0] * yb(mu[1]) - yb(al_n[3] * near_mu[0])
            p1 = al[4] * mu[3] + al[6] * mu[7] + al_n[0] * near_mu[2] + yb(al_n[3] * near_mu[6])
            r1 = -al[0] * mu[3] - al[3] * mu[7] - al_n[4] * near_mu[2] - yb(al_n[6] * near_mu[6])
            p3 = -(be[0] + be[3] + be[4] + be[6]) - be_n[0] - yb(be_n[3])
            if not low:
                p3 = p3 - be_n[4] - yb(be_n[6])
            return place(p0, p1, None, p3), place(r0, r1)

        terms = (loose_terms(True), loose_terms(False))
        low_diag = place(e1_low, e2_diag, e5_diag, node_low)
        high_diag = place(e1_low + mu[5], e2_diag, e5_diag, node_diag)

        blocks = [
            jnp.concatenate([low_diag] + [high_diag] * (planes - 1), axis=0),
            jnp.concatenate([high_diag] * planes, axis=0),
        ]
        same_ref[...] = same
        summed = group_sum(same, jnp.concatenate(blocks, axis=1))
        damp = jnp.where((iota((total, LANES), 1) & 3) == 3, NODE_DAMPING, EDGE_DAMPING)
        for i in range(2):
            weight_ref[i] = damp / summed[:, LANES * i : LANES * (i + 1)]
        out = (edge_mass, self_coef, cross_coef) + terms[0] + terms[1]
        for i, v in enumerate(out):
            field_ref[i] = v

    f32 = jnp.float32
    smem = pl.BlockSpec(memory_space=pltpu.SMEM)
    vmem = pl.BlockSpec(memory_space=pltpu.VMEM)
    return pl.pallas_call(
        body,
        compiler_params=pltpu.CompilerParams(vmem_limit_bytes=VMEM_BYTES),
        name="prepare",
        in_specs=[smem, smem] + [vmem] * (n_dom + 1),
        out_shape=(
            pltpu.VMEM((total, total), jnp.bfloat16),
            pltpu.VMEM((2, total, LANES), f32),
            pltpu.VMEM((7, n, LANES), f32),
        ),
        scratch_shapes=[pltpu.VMEM((n_dom, sides, LANES), f32)],
    )


def solve_kernel(n_dom, n_sub, macros, planes, cells):
    sides = 2 * macros
    n = n_dom * sides
    depth = n_sub * planes

    def body(recv_ref, coef_ref, edge_in, pot_in, same_ref, weight_ref, field_ref, edge_ref, pot_ref, one_ref, two_ref, turn_ref):
        k = lax.axis_index("sub")
        d = lax.axis_index("dom")
        shape = (n, LANES)
        group = iota(shape, 1) & 3
        edges = group < 3
        upper = (iota(shape, 0) % sides) >= macros

        def rows_of(layer, at):
            parts = [
                recv_ref[e * n_sub + layer, at * sides : (at + 1) * sides, :] for e in range(n_dom)
            ]
            return jnp.concatenate(parts, axis=0)

        same = same_ref[...]
        blocks = [
            jnp.concatenate([rows_of(layer, p) for p in range(planes)], axis=0)
            for layer in range(n_sub)
        ]
        summed = group_sum(same, jnp.concatenate(blocks, axis=1))

        def lanes(v, i):
            return v[:, LANES * i : LANES * (i + 1)]

        weight = [weight_ref[0], weight_ref[1]]
        edge_mass, self_coef, cross_coef = (field_ref[i] for i in range(3))
        terms = ((field_ref[3], field_ref[4]), (field_ref[5], field_ref[6]))

        def fold(v):
            return lane_roll(v, 3) + lane_roll(v, 2) + lane_roll(v, 1)

        def fold_edges(r, r_below):
            out = jnp.where(group == 0, yb(r), 0.0) - r
            if r_below is not None:
                out = out + jnp.where(group == 1, r_below, 0.0)
                out = out + jnp.where(group == 2, yb(r_below), 0.0)
            return out

        def node_sums(nodes):
            block = None
            for layer in range(n_sub):
                stacked = jnp.concatenate(nodes[layer], axis=0)
                moved = lane_roll(stacked, layer - 3)
                moved = jnp.where((iota(moved.shape, 1) & 3) == layer, moved, 0.0)
                block = moved if block is None else block + moved
            out = group_sum(same, block)
            return [lane_roll(out, 3 - layer) for layer in range(n_sub)]

        def of(v, p):
            return v[p * n : (p + 1) * n]

        e1, r1 = {}, {}
        nodes = [[None] * planes for _ in range(n_sub)]
        for layer in range(n_sub):
            value = lanes(summed, layer) * weight[min(layer, 1)]
            for p in range(planes):
                at = layer * planes + p
                src = of(blocks[layer], p)
                e1[at] = jnp.where(edges, of(value, p), 0.0)
                r1[at] = jnp.where(edges, src - edge_mass * e1[at], 0.0)
                node = src + fold(fold_edges(r1[at], r1.get(at - 1)))
                if p == 0 and layer > 0:
                    shifted = lane_roll(rows_of(layer - 1, planes + 1), 1)
                    node = node + jnp.where(upper, shifted, 0.0)
                nodes[layer][p] = node
        node_sum = node_sums(nodes)
        c1 = {}
        for at in range(depth):
            layer, p = at // planes, at % planes
            value = of(node_sum[layer], p) * of(weight[min(layer, 1)], p)
            c1[at] = jnp.where(group == 3, value, 0.0)
            one_ref[HALO + at] = e1[at] + c1[at]

        cross = {}
        base = {}
        for at in range(depth):
            e = e1[at]
            first = lane_roll(ya(e), -1) - lane_roll(e, -2)
            second = -lane_roll(e, -1)
            if at + 1 in e1:
                second = second + lane_roll(e1[at + 1], 1)
            cross[at] = jnp.where(
                group < 2, cross_coef * (e + jnp.where(group == 0, first, second)), 0.0
            )
        second_blocks = []
        for layer in range(n_sub):
            stacked = []
            for p in range(planes):
                at = layer * planes + p
                v = cross[at]
                own0 = v if at == 0 else v + lane_roll(cross[at - 1], -1)
                own1 = v + lane_roll(yb(v), 1)
                own2 = -(lane_roll(v, 2) + lane_roll(v, 1))
                coupled = jnp.where(group == 0, own0, jnp.where(group == 1, own1, own2))
                c = c1[at]
                ahead = ya(c)
                rise0 = lane_roll(ahead - c, -3)
                if at + 1 in c1:
                    up = c1[at + 1]
                    rise1 = lane_roll(up - c, -2)
                    rise2 = lane_roll(ya(up) - c, -1)
                else:
                    rise1, rise2 = lane_roll(-c, -2), lane_roll(-c, -1)
                rise = jnp.where(group == 0, rise0, jnp.where(group == 1, rise1, rise2))
                rise = jnp.where(edges, rise, 0.0)
                base[at] = e1[at] + rise
                given = jnp.where(group < 2, rows_of(layer, planes + p), 0.0)
                if p == planes - 1 and layer + 1 < n_sub:
                    extra = lane_roll(rows_of(layer + 1, planes), -1)
                    given = given + jnp.where(group == 1, extra, 0.0)
                res = r1[at] + given - self_coef * e1[at] - coupled - edge_mass * rise
                stacked.append(jnp.where(edges, res, 0.0))
            second_blocks.append(jnp.concatenate(stacked, axis=0))
        summed = group_sum(same, jnp.concatenate(second_blocks, axis=1))
        e2, r2 = {}, {}
        for layer in range(n_sub):
            value = lanes(summed, layer) * weight[min(layer, 1)]
            for p in range(planes):
                at = layer * planes + p
                e2[at] = jnp.where(edges, base[at] + of(value, p), 0.0)
                src = of(blocks[layer], p)
                r2[at] = jnp.where(edges, src - edge_mass * e2[at], 0.0)
                by_p, by_r = terms[min(at, 1)]
                e = e1[at]
                behind = yb(e)
                if at > 0:
                    behind = jnp.where(group == 1, e1[at - 1], behind)
                    reach = jnp.where(group < 2, by_r * behind, 0.0)
                else:
                    reach = jnp.where(group == 0, by_r * behind, 0.0)
                inner = fold_edges(r2[at], r2.get(at - 1)) + jnp.where(group < 2, by_p * e, 0.0)
                node = rows_of(layer, planes + p) + fold(inner + reach) + by_p * c1[at]
                if p == 0 and layer > 0:
                    node = node + lane_roll(rows_of(layer - 1, 2 * planes - 1), 1)
                if p == 1 and layer > 0:
                    shifted = row_roll(lane_roll(rows_of(layer - 1, planes + 1), 1), macros)
                    node = node + jnp.where(upper, shifted, 0.0)
                if p == planes - 1 and layer + 1 < n_sub:
                    node = node + lane_roll(rows_of(layer + 1, planes + 2), 1)
                nodes[layer][p] = node
        node_sum = node_sums(nodes)
        for at in range(depth):
            layer, p = at // planes, at % planes
            value = of(node_sum[layer], p) * of(weight[min(layer, 1)], p)
            two_ref[HALO + at] = jnp.where(group == 3, value, e2[at])
        for ref in (one_ref, two_ref):
            for i in range(HALO):
                ref[i] = jnp.zeros(shape, jnp.float32)
                ref[HALO + depth + i] = jnp.zeros(shape, jnp.float32)

        strip = (sides, LANES)
        sh = Strip(strip)
        has_below = jnp.where(k == 0, 0.0, 1.0)
        has_above = jnp.where(k == n_sub - 1, 0.0, 1.0)

        def flagged(p, v):
            flag = has_below if p < 0 else has_above if p >= planes else None
            return v if flag is None or v is None else v * flag

        mine = pl.ds(pl.multiple_of(d * sides, sides), sides)

        def taken(ref, p, g):
            value = ref[k * planes + p + HALO, mine, :]
            return jnp.where(sh.own, lane_roll(value, -g), 0.0)

        my_mass = [coef_ref[t] for t in range(7)]
        my_mu = [coef_ref[7 + f] for f in range(8)]
        loose_r = {}
        step_e = {}
        c_one = {p: taken(one_ref, p, 3) for p in range(-1, planes + 2)}
        faces = {}
        for p in range(-1, planes + 1):
            ea, eb = taken(one_ref, p, 0), taken(one_ref, p, 1)
            faces[p] = (
                my_mu[0] * sh.ax(ea),
                my_mu[1] * ea,
                my_mu[2] * sh.ax(eb),
                my_mu[3] * eb,
                my_mu[6] * sh.axy(eb),
                my_mu[7] * eb,
            )
        for p in range(-1, planes + 1):
            f0, f1, f2, f3, f6, f7 = faces[p]
            types = LOOSE_TYPES if p >= 0 else (4, 6)
            grad = grad_at(c_one[p], c_one[p + 1], sh, types)
            curled = {4: -f2 - f3, 6: -f6 - f7}
            if p >= 0:
                below = faces[p - 1]
                curled[0] = f0 + f2 + yb(f1) + below[3]
                curled[3] = f6 + below[5] - f0 - f1
            step_e[p], loose_r[p] = [None] * 7, [None] * 7
            for t in types:
                weight_t = coef_ref[22 + t] if p == 0 else coef_ref[15 + t]
                value = grad[t] - weight_t * (curled[t] + my_mass[t] * grad[t])
                value = flagged(p, value)
                step_e[p][t] = value
                loose_r[p][t] = -my_mass[t] * value
        c_two = {}
        for p in range(planes + 1):
            node = back_at(loose_r[p], loose_r[p - 1], sh)
            node = (coef_ref[30] if p == 0 else coef_ref[29]) * node
            node = jnp.where(sh.own, taken(two_ref, p, 3), node)
            c_two[p] = flagged(p, node)

        def plain(v):
            return jnp.where(sh.upper, jnp.where(sh.col == 3, lane_roll(v, 3), lane_roll(v, -1)), v)

        for p in range(planes):
            grad = grad_at(c_two[p], c_two[p + 1], sh)
            for t in range(7):
                if t in SHARED_TYPES:
                    start = taken(two_ref, p, SHARED_TYPES.index(t))
                else:
                    start = step_e[p][t]
                turn_ref[t, :, p, :] = plain(start + grad[t])
            turn_ref[7, :, p, :] = plain(c_one[p] + c_two[p])

        x = iota((planes, LANES), 1) & (LAT - 1)

        def overlaid(v, low, high):
            columns = []
            for c in range(8):
                add = jnp.where(x >= LAT - 4, lane_roll(high, 28 - 4 * c), 0.0)
                add = jnp.where(x < 4, lane_roll(low, -4 * c), add)
                columns.append(v[:, LANES * c : LANES * (c + 1)] + add)
            return jnp.concatenate(columns, axis=1)

        def macro_step(m, carry):
            for t in range(7):
                low, high = turn_ref[t, m], turn_ref[t, macros + m]
                edge_ref[m, t] = overlaid(edge_in[m, t], low, high)
            pot_ref[m] = overlaid(pot_in[m], turn_ref[7, m], turn_ref[7, macros + m])
            return carry

        lax.fori_loop(0, macros, macro_step, 0)

    f32 = jnp.float32
    return pl.pallas_call(
        body,
        compiler_params=pltpu.CompilerParams(vmem_limit_bytes=VMEM_BYTES),
        name="solve",
        out_shape=(
            jax.ShapeDtypeStruct((macros, 7, planes, cells), f32),
            jax.ShapeDtypeStruct((macros, planes, cells), f32),
        ),
        scratch_shapes=[
            pltpu.VMEM((depth + 2 * HALO, n, LANES), f32),
            pltpu.VMEM((depth + 2 * HALO, n, LANES), f32),
            pltpu.VMEM((8, sides, planes, LANES), f32),
        ],
    )


def near_core(*values):
    return [pltpu.with_memory_space_constraint(v, pltpu.VMEM) for v in values]


def local_small(source, zone_ids, kappa_table, mu_table, owner_dev, owner_group):
    macros, _, planes, cells = source.shape
    n_dom, n_sub = lax.axis_size("dom"), lax.axis_size("sub")
    sizes = (n_dom, n_sub, macros, planes, cells)
    lists = (owner_dev.shape[1], owner_group.shape[1])
    up = [(i, i + 1) for i in range(n_sub - 1)]
    down = [(i + 1, i) for i in range(n_sub - 1)]
    tables = (kappa_table.T, mu_table.T)
    far = [pltpu.with_memory_space_constraint(v, pltpu.HBM) for v in (*tables, zone_ids, source)]
    pay, coef = first_kernel(*sizes)(*far)
    recv = lax.all_to_all(pay, ("dom", "sub"), 0, 0)
    labels = label_kernel(*sizes, *lists)(zone_ids, owner_dev, owner_group)
    labels = [labels]
    for i in range(1, n_dom):
        route = [(e, e ^ i) for e in range(n_dom)]
        labels.append(lax.ppermute(labels[0], "dom", route))
    low = lax.ppermute(source[:, :, planes - HALO :], "sub", up)
    high = lax.ppermute(source[:, :, :HALO], "sub", down)
    edge, pot = inner_kernel(*sizes)(*tables, zone_ids, source, *near_core(low, high))
    fields = prepare_kernel(*sizes, *lists)(*tables, *near_core(*labels, pot))
    return solve_kernel(*sizes)(*near_core(recv, coef, edge, pot, *fields))


def fits_small(mesh, source, owner_dev, owner_group):
    macros = source.shape[0] // mesh.shape["dom"]
    planes = source.shape[2] // mesh.shape["sub"]
    return (
        macros == 4
        and planes == 4
        and source.shape[3] == LAT * LAT
        and mesh.shape["sub"] == 4
        and owner_dev.shape[1] == 2 * macros * planes
        and owner_group.shape[1] == 32
        and mesh.shape["dom"] in (1, 2, 4, 8)
    )


def solution(mesh):
    in_specs = (
        P("dom", None, "sub", None),
        P("dom", None),
        P(),
        P(),
        P("dom", None),
        P("dom", None),
    )
    out_specs = (P("dom", None, "sub", None), P("dom", "sub", None))

    def step(source, zone_ids, kappa_table, mu_table, owner_dev, owner_group):
        body = local_small if fits_small(mesh, source, owner_dev, owner_group) else local
        mapped = jax.shard_map(
            body, mesh=mesh, in_specs=in_specs, out_specs=out_specs, check_vma=False
        )
        return mapped(source, zone_ids, kappa_table, mu_table, owner_dev, owner_group)

    return step
```

```python
import jax
import jax.numpy as jnp
from jax import lax
from jax.experimental import pallas as pl
from jax.experimental.pallas import tpu as pltpu
from jax.sharding import PartitionSpec as P


LAT = 32
SWEEPS = 2


EDGE_OFFSETS = ((0, 0, 1), (0, 1, 0), (1, 0, 0), (0, 1, 1), (1, 0, 1), (1, 1, 0), (1, 1, 1))
FACE_EDGES = (
    (0, 1, 3),
    (1, 0, 3),
    (0, 2, 4),
    (2, 0, 4),
    (1, 2, 5),
    (2, 1, 5),
    (3, 2, 6),
    (2, 3, 6),
)
SHARED_TYPES = (1, 2, 5)
EDGE_DAMPING = 0.6
NODE_DAMPING = 0.8


def with_halo(block, sides, width):
    for axis, dim in sides:
        count = lax.axis_size(axis)
        forward = [(i, i + 1) for i in range(count - 1)]
        backward = [(target, source) for source, target in forward]
        low = lax.ppermute(
            lax.slice_in_dim(block, block.shape[dim] - width, None, axis=dim), axis, forward
        )
        high = lax.ppermute(lax.slice_in_dim(block, 0, width, axis=dim), axis, backward)
        block = jnp.concatenate([low, block, high], axis=dim)
    return block


def from_behind(block, axis, distance):
    devices = range(lax.axis_size(axis))
    route = [(i - distance, i) for i in devices if i - distance in devices]
    return lax.ppermute(block, axis, route)


def shift_ahead(values, rise_y, rise_x):
    offset = rise_y * LAT + rise_x
    if offset == 0:
        return values
    padding = jnp.zeros(values.shape[:-1] + (offset,), values.dtype)
    shifted = jnp.concatenate([values[..., offset:], padding], axis=-1)
    if rise_x:
        column = jnp.arange(values.shape[-1]) % LAT
        shifted = jnp.where(column < LAT - rise_x, shifted, jnp.zeros_like(shifted))
    return shifted


def shift_behind(values, rise_y, rise_x):
    offset = rise_y * LAT + rise_x
    if offset == 0:
        return values
    padding = jnp.zeros(values.shape[:-1] + (offset,), values.dtype)
    shifted = jnp.concatenate([padding, values[..., :-offset]], axis=-1)
    if rise_x:
        column = jnp.arange(values.shape[-1]) % LAT
        shifted = jnp.where(column >= rise_x, shifted, jnp.zeros_like(shifted))
    return shifted


def apply_operator(padded, halo_width, extra_planes, first_plane, mass_coef, curl_coef):
    planes = padded.shape[2] - 2 * halo_width
    face_count = planes + extra_planes + 1
    first_face = halo_width - extra_planes - 1
    face_planes = first_plane - extra_planes - 1 + jnp.arange(face_count)
    face_valid = (face_planes >= 0)[None, :, None]
    result = [
        mass_coef[edge_type][:, None, :]
        * padded[:, edge_type, halo_width - extra_planes : halo_width + planes]
        for edge_type in range(7)
    ]
    for face_index, (first_edge, second_edge, diagonal_edge) in enumerate(FACE_EDGES):
        rise_z, rise_y, rise_x = EDGE_OFFSETS[first_edge]
        far_values = shift_ahead(
            padded[:, second_edge, first_face + rise_z : first_face + rise_z + face_count],
            rise_y,
            rise_x,
        )
        circulation = (
            padded[:, first_edge, first_face : first_face + face_count]
            + far_values
            - padded[:, diagonal_edge, first_face : first_face + face_count]
        )
        weighted = jnp.where(face_valid, curl_coef[face_index][:, None, :] * circulation, 0.0)
        result[first_edge] = result[first_edge] + weighted[:, 1:]
        result[diagonal_edge] = result[diagonal_edge] - weighted[:, 1:]
        result[second_edge] = result[second_edge] + shift_behind(
            weighted[:, 1 - rise_z : 1 - rise_z + planes + extra_planes], rise_y, rise_x
        )
    return jnp.stack(result, axis=1)


def edge_diagonal(mass_coef, curl_coef, first_plane, planes):
    inside = (first_plane + jnp.arange(planes) >= 1)[None, :, None]
    flat_planes = jnp.zeros((1, planes, 1), mass_coef.dtype)
    diagonal = [mass_coef[edge_type][:, None, :] + flat_planes for edge_type in range(7)]
    for face_index, (first_edge, second_edge, diagonal_edge) in enumerate(FACE_EDGES):
        rise_z, rise_y, rise_x = EDGE_OFFSETS[first_edge]
        own_term = curl_coef[face_index][:, None, :]
        diagonal[first_edge] = diagonal[first_edge] + own_term
        diagonal[diagonal_edge] = diagonal[diagonal_edge] + own_term
        behind_term = shift_behind(curl_coef[face_index], rise_y, rise_x)[:, None, :] + flat_planes
        if rise_z:
            behind_term = jnp.where(inside, behind_term, 0.0)
        diagonal[second_edge] = diagonal[second_edge] + behind_term
    return jnp.stack(diagonal, axis=1)


def node_diagonal(mass_coef, first_plane, planes):
    inside = (first_plane + jnp.arange(planes) >= 1)[None, :, None]
    total = jnp.zeros((mass_coef.shape[1], planes, mass_coef.shape[2]), mass_coef.dtype)
    for edge_type in range(7):
        rise_z, rise_y, rise_x = EDGE_OFFSETS[edge_type]
        total = total + mass_coef[edge_type][:, None, :]
        behind_term = shift_behind(mass_coef[edge_type], rise_y, rise_x)[:, None, :] + jnp.zeros(
            (1, planes, 1), mass_coef.dtype
        )
        if rise_z:
            behind_term = jnp.where(inside, behind_term, 0.0)
        total = total + behind_term
    return total


def node_residual(lowered, planes):
    total = jnp.zeros((lowered.shape[0], planes, lowered.shape[3]), lowered.dtype)
    for edge_type in range(7):
        rise_z, rise_y, rise_x = EDGE_OFFSETS[edge_type]
        total = (
            total
            + shift_behind(lowered[:, edge_type, 1 - rise_z : 1 - rise_z + planes], rise_y, rise_x)
            - lowered[:, edge_type, 1:]
        )
    return total


def gradient(raised, planes):
    result = []
    for edge_type in range(7):
        rise_z, rise_y, rise_x = EDGE_OFFSETS[edge_type]
        result.append(
            shift_ahead(raised[:, rise_z : rise_z + planes], rise_y, rise_x) - raised[:, :planes]
        )
    return jnp.stack(result, axis=1)


def edge_sides(values):
    macro_count, type_count, plane_count, _ = values.shape
    lattice = values.reshape(macro_count, type_count, plane_count, LAT, LAT)
    chosen = jnp.stack([lattice[:, edge_type] for edge_type in SHARED_TYPES], axis=1)
    sides = jnp.stack([chosen[..., 0], chosen[..., LAT - 1]], axis=1)
    return jnp.transpose(sides, (0, 1, 3, 2, 4)).reshape(-1, 3 * LAT)


def insert_edges(values, blocks):
    macro_count, type_count, plane_count, _ = values.shape
    shaped = blocks.reshape(macro_count, 2, plane_count, 3, LAT)
    shaped = jnp.transpose(shaped, (0, 1, 3, 2, 4))
    lattice = values.reshape(macro_count, type_count, plane_count, LAT, LAT)
    for side_index, column in ((0, 0), (1, LAT - 1)):
        for slot_type, edge_type in enumerate(SHARED_TYPES):
            lattice = lattice.at[:, edge_type, :, :, column].set(shaped[:, side_index, slot_type])
    return lattice.reshape(values.shape)


def node_sides(values):
    macro_count, plane_count, _ = values.shape
    lattice = values.reshape(macro_count, plane_count, LAT, LAT)
    sides = jnp.stack([lattice[..., 0], lattice[..., LAT - 1]], axis=1)
    return sides.reshape(-1, LAT)


def insert_nodes(values, blocks):
    macro_count, plane_count, _ = values.shape
    shaped = blocks.reshape(macro_count, 2, plane_count, LAT)
    lattice = values.reshape(macro_count, plane_count, LAT, LAT)
    for side_index, column in ((0, 0), (1, LAT - 1)):
        lattice = lattice.at[:, :, :, column].set(shaped[:, side_index])
    return lattice.reshape(values.shape)


def local(source, zone_ids, kappa_table, mu_table, owner_dev, owner_group):
    macro_count, type_count, planes, cell_count = source.shape
    first_plane = lax.axis_index("sub") * planes
    onehot = (jnp.arange(kappa_table.shape[0])[:, None] == zone_ids.reshape(1, -1)).astype(
        jnp.float32
    )
    mass_coef = jnp.dot(kappa_table.T, onehot, precision=lax.Precision.HIGHEST).reshape(
        type_count, macro_count, cell_count
    )
    curl_coef = jnp.dot(mu_table.T, onehot, precision=lax.Precision.HIGHEST).reshape(
        mu_table.shape[1], macro_count, cell_count
    )
    peer_count = lax.axis_size("dom")
    recv_rows = owner_group.shape[1]
    capacity = recv_rows // peer_count
    slot_count = owner_dev.shape[1]
    owner_of = owner_dev[0]
    groups = owner_group[0]
    earlier = jnp.arange(slot_count)[None, :] < jnp.arange(slot_count)[:, None]
    position = jnp.sum((owner_of[:, None] == owner_of[None, :]) & earlier, axis=1)
    slot_place = owner_of * capacity + position
    spread = (jnp.arange(recv_rows)[:, None] == slot_place[None, :]).astype(jnp.float32)
    same_group = (groups[:, None] == groups[None, :]).astype(jnp.float32)

    def owner_sum(received):
        summed = jnp.dot(
            same_group, received.reshape(recv_rows, -1), precision=lax.Precision.HIGHEST
        )
        return lax.all_to_all(
            summed.reshape(peer_count, capacity, -1), "dom", split_axis=0, concat_axis=0, tiled=True
        )

    def assemble(blocks):
        outgoing = jnp.dot(spread, blocks, precision=lax.Precision.HIGHEST).reshape(
            peer_count, capacity, blocks.shape[1]
        )
        returned = owner_sum(
            lax.all_to_all(outgoing, "dom", split_axis=0, concat_axis=0, tiled=True)
        )
        return jnp.take(returned.reshape(recv_rows, -1), slot_place, axis=0)

    rim_width = 2

    def rimmed(values):
        return with_halo(values, (("sub", 2),), rim_width)

    edge_diag = edge_diagonal(mass_coef, curl_coef, first_plane, planes)
    node_diag = node_diagonal(mass_coef, first_plane, planes)
    edge_width = 3 * LAT
    first_blocks = [edge_sides(edge_diag), node_sides(node_diag)]
    diag_sums = assemble(jnp.concatenate(first_blocks, axis=1))
    full_edge_diag = insert_edges(edge_diag, diag_sums[:, :edge_width])
    full_node_diag = insert_nodes(node_diag, diag_sums[:, edge_width : edge_width + LAT])
    source_below = from_behind(source[:, :, planes - 1 :], "sub", 1)
    edge_field = jnp.zeros_like(source)
    potential = jnp.zeros((macro_count, planes, cell_count), jnp.float32)
    for sweep_index in range(SWEEPS):
        if sweep_index == 0:
            residual = source
            residual_sum = assemble(edge_sides(residual))
        else:
            residual = source - apply_operator(
                rimmed(edge_field), rim_width, 0, first_plane, mass_coef, curl_coef
            )
            residual_sum = assemble(edge_sides(residual))
        full_residual = insert_edges(residual, residual_sum)
        edge_field = edge_field + EDGE_DAMPING * full_residual / full_edge_diag
        padded = rimmed(edge_field)
        lowered = jnp.concatenate([source_below, source], axis=2) - apply_operator(
            padded, 2, 1, first_plane, mass_coef, curl_coef
        )
        node_values = node_residual(lowered, planes)
        node_sum = assemble(node_sides(node_values))
        correction = NODE_DAMPING * insert_nodes(node_values, node_sum) / full_node_diag
        plane_above = from_behind(correction[:, :1], "sub", -1)
        edge_field = edge_field + gradient(
            jnp.concatenate([correction, plane_above], axis=1), planes
        )
        potential = potential + correction
    return (edge_field, potential)


LANES = 128
HALO = 2
VMEM_BYTES = 24 * 1024 * 1024
LOOSE_TYPES = (0, 3, 4, 6)


def lane_roll(v, s):
    s = s % v.shape[-1]
    return pltpu.roll(v, s, v.ndim - 1) if s else v


def row_roll(v, s):
    s = s % v.shape[0]
    return pltpu.roll(v, s, 0) if s else v


def iota(shape, dim):
    return lax.broadcasted_iota(jnp.int32, shape, dim)


def zb(v):
    return row_roll(v, 1)


def za(v):
    return row_roll(v, -1)


class Plane:
    def __init__(self, shape):
        self.lane = iota(shape, 1)
        self.x = self.lane & (LAT - 1)
        self.cells = shape[1]
        self.side = (self.x == 0) | (self.x == LAT - 1)

    def ax(self, v):
        return jnp.where(self.x < LAT - 1, lane_roll(v, -1), 0.0)

    def ay(self, v):
        return jnp.where(self.lane < self.cells - LAT, lane_roll(v, -LAT), 0.0)

    def bx(self, v):
        return jnp.where(self.x > 0, lane_roll(v, 1), 0.0)

    def by(self, v):
        return jnp.where(self.lane >= LAT, lane_roll(v, LAT), 0.0)

    def bxy(self, v):
        return jnp.where((self.lane >= LAT) & (self.x > 0), lane_roll(v, LAT + 1), 0.0)

    def axy(self, v):
        inner = (self.lane < self.cells - LAT) & (self.x < LAT - 1)
        return jnp.where(inner, lane_roll(v, -LAT - 1), 0.0)


def yb(v):
    lane = iota(v.shape, 1)
    first = jnp.where(lane < 4, 0.0, lane_roll(v, 36))
    return jnp.where(lane < 32, first, lane_roll(v, 32))


def ya(v):
    lane = iota(v.shape, 1)
    last = jnp.where(lane >= 124, 0.0, lane_roll(v, -36))
    return jnp.where(lane >= 96, last, lane_roll(v, -32))


class Strip:
    def __init__(self, shape):
        half = shape[0] // 2
        self.col = iota(shape, 1) & 3
        self.upper = iota(shape, 0) >= half
        self.own = self.col == 0

    def ax(self, v):
        wrap = jnp.where(self.upper, lane_roll(v, 3), 0.0)
        step = jnp.where(self.upper & self.own, 0.0, lane_roll(v, -1))
        return jnp.where(self.col == 3, wrap, step)

    def bx(self, v):
        wrap = jnp.where(self.upper, lane_roll(v, -3), 0.0)
        step = jnp.where(self.upper & (self.col == 1), 0.0, lane_roll(v, 1))
        return jnp.where(self.own, wrap, step)

    def ay(self, v):
        return ya(v)

    def by(self, v):
        return yb(v)

    def bxy(self, v):
        return yb(self.bx(v))

    def axy(self, v):
        return ya(self.ax(v))


def to_strip(v):
    lane = iota((v.shape[0], LANES), 1)
    block = (lane & 31) >> 2
    low = jnp.zeros((v.shape[0], LANES), v.dtype)
    high = low
    for c in range(8):
        column = v[:, LANES * c : LANES * (c + 1)]
        low = jnp.where(block == c, lane_roll(column, 4 * c), low)
        high = jnp.where(block == c, lane_roll(column, 4 * c - 28), high)
    high = jnp.where((lane & 3) == 0, lane_roll(high, -3), lane_roll(high, 1))
    return jnp.concatenate([low, high], axis=0)


def plus(*terms):
    total = None
    for term in terms:
        if term is not None:
            total = term if total is None else total + term
    return total


def on(f, v):
    return None if v is None else f(v)


def minus(v):
    return on(lambda a: -a, v)


def times(c, v):
    return on(lambda a: c * a, v)


def table_lookup(zone, table_ref, width):
    out = [jnp.zeros(zone.shape, jnp.float32)] * width
    for z in range(table_ref.shape[1]):
        hit = zone == z
        out = [jnp.where(hit, table_ref[i, z], v) for i, v in enumerate(out)]
    return out


def diagonals(mass, mu, sh):
    flat = [
        mass[0] + mu[0] + mu[2] + sh.by(mu[1]),
        mass[1] + mu[1] + mu[4] + sh.bx(mu[0]),
        mass[2] + mu[3] + mu[5] + mu[7] + sh.bx(mu[2]) + sh.by(mu[4]) + sh.bxy(mu[6]),
        mass[3] + mu[0] + mu[1] + mu[6],
        mass[4] + mu[2] + mu[3],
        mass[5] + mu[4] + mu[5],
        mass[6] + mu[6] + mu[7],
    ]
    rise = {0: mu[3], 1: mu[5], 3: mu[7]}
    node_flat = sh.bx(mass[0]) + sh.by(mass[1]) + sh.bxy(mass[3])
    for t in range(7):
        node_flat = node_flat + mass[t]
    node_rise = mass[2] + sh.bx(mass[4]) + sh.by(mass[5]) + sh.bxy(mass[6])
    return flat, rise, node_flat, node_rise


def grad_at(c, c_up, sh, types=range(7)):
    moves = (sh.ax, sh.ay, lambda v: v, sh.axy, sh.ax, sh.ay, sh.axy)
    out = [None] * 7
    for t in types:
        out[t] = plus(on(moves[t], c_up if EDGE_OFFSETS[t][0] else c), minus(c))
    return out


def back_at(r, r_below, sh):
    return plus(
        minus(plus(*r)),
        r_below[2],
        on(sh.bx, plus(r[0], r_below[4])),
        on(sh.by, plus(r[1], r_below[5])),
        on(sh.bxy, plus(r[3], r_below[6])),
    )


NONE7 = [None] * 7


def first_kernel(n_dom, n_sub, macros, planes, cells):
    sides = 2 * macros
    blocks = 2 * planes

    def body(kappa_ref, mu_ref, zone_ref, source_ref, pay_ref, coef_ref, hold_ref, sems):
        k = lax.axis_index("sub")
        shape = (sides, LANES)
        sh = Strip(shape)
        row = iota(shape, 0)
        group = iota(shape, 1) & 3
        zone = to_strip(zone_ref[...])
        mass = table_lookup(zone, kappa_ref, 7)
        mu = table_lookup(zone, mu_ref, 8)
        flat, rise, node_flat, node_rise = diagonals(mass, mu, sh)
        w = [EDGE_DAMPING / (flat[t] + rise[t] if t in rise else flat[t]) for t in range(7)]
        w_low = [EDGE_DAMPING / flat[t] if t in rise else w[t] for t in range(7)]
        lowest = k == 0
        w_zero = [jnp.where(lowest, w_low[t], w[t]) for t in range(7)]
        nw = NODE_DAMPING / (node_flat + node_rise)
        nw_zero = jnp.where(lowest, NODE_DAMPING / node_flat, nw)
        for i, v in enumerate(mass + mu + w + w_zero + [nw, nw_zero]):
            coef_ref[i] = v
        has_below = jnp.where(lowest, 0.0, 1.0)
        has_above = jnp.where(k == n_sub - 1, 0.0, 1.0)

        def loose(t, v):
            return jnp.where(sh.own, 0.0, v) if t in SHARED_TYPES else v

        def flagged(p, v):
            flag = has_below if p < 0 else has_above if p >= planes else None
            return v if flag is None or v is None else v * flag

        src = {p: [to_strip(source_ref[:, t, p, :]) for t in range(7)] for p in range(planes)}
        e1, r1 = {}, {}
        for p in range(planes):
            wp = w_zero if p == 0 else w
            e1[p] = [loose(t, wp[t] * src[p][t]) for t in range(7)]
            r1[p] = [loose(t, src[p][t] - mass[t] * e1[p][t]) for t in range(7)]
        n1, c1 = {}, {}
        for p in range(planes + 1):
            n1[p] = back_at(r1.get(p, NONE7), r1.get(p - 1, NONE7), sh)
            c1[p] = jnp.where(sh.own, 0.0, (nw_zero if p == 0 else nw) * n1[p])
            c1[p] = flagged(p, c1[p])
        faces = {}
        for p in range(-1, planes):
            e, e_up = e1.get(p, NONE7), e1.get(p + 1, NONE7)
            far = (
                on(sh.ax, e[1]),
                on(sh.ay, e[0]),
                on(sh.ax, e[2]),
                e_up[0],
                on(sh.ay, e[2]),
                e_up[1],
                on(sh.axy, e[2]),
                e_up[3],
            )
            faces[p] = [
                flagged(p, times(mu[f], plus(e[a], far[f], minus(e[g]))))
                for f, (a, _, g) in enumerate(FACE_EDGES)
            ]
        res, r2 = {}, {}
        none8 = [None] * 8
        for p in range(-1, planes + 1):
            f, f_below = faces.get(p, none8), faces.get(p - 1, none8)
            curled = [
                plus(f[0], f[2], on(sh.by, f[1]), f_below[3]),
                plus(f[1], f[4], on(sh.bx, f[0]), f_below[5]),
                plus(f[3], f[5], f[7], on(sh.bx, f[2]), on(sh.by, f[4]), on(sh.bxy, f[6])),
                plus(f[6], f_below[7], minus(f[0]), minus(f[1])),
                minus(plus(f[2], f[3])),
                minus(plus(f[4], f[5])),
                minus(plus(f[6], f[7])),
            ]
            grad = grad_at(c1.get(p), c1.get(p + 1), sh)
            wp = w_zero if p == 0 else w
            res[p], r2[p] = [], []
            for t in range(7):
                g = grad[t]
                value = plus(
                    r1.get(p, NONE7)[t], minus(curled[t]), minus(times(mass[t], g))
                )
                res[p].append(value)
                e2 = plus(e1.get(p, NONE7)[t], g, times(wp[t], value))
                s = src[p][t] if p in src else None
                left = flagged(p, plus(s, minus(times(mass[t], e2))))
                r2[p].append(on(lambda v: loose(t, v), left))
        n2 = {p: back_at(r2.get(p, NONE7), r2.get(p - 1, NONE7), sh) for p in range(-1, planes + 2)}

        def merge(g0, g1, g2, g3):
            out = jnp.where(group == 1, lane_roll(g1, 1), g0)
            out = jnp.where(group == 2, lane_roll(g2, 2), out)
            return jnp.where(group == 3, lane_roll(g3, 3), out)

        high = jnp.where(row < macros, row_roll(n2[planes + 1], macros), n1[planes])
        spare = [flagged(-1, res[-1][2]), high, n2[-1], n2[planes]]
        for p in range(planes):
            hold_ref[p * sides : (p + 1) * sides, :] = merge(src[p][1], src[p][2], src[p][5], n1[p])
            at = planes + p
            hold_ref[at * sides : (at + 1) * sides, :] = merge(res[p][1], res[p][2], spare[p], n2[p])
        copies = [
            pltpu.make_async_copy(hold_ref, pay_ref.at[dest], sems.at[dest])
            for dest in range(n_dom * n_sub)
        ]
        for copy in copies:
            copy.start()
        for copy in copies:
            copy.wait()

    f32 = jnp.float32
    smem = pl.BlockSpec(memory_space=pltpu.SMEM)
    vmem = pl.BlockSpec(memory_space=pltpu.VMEM)
    return pl.pallas_call(
        body,
        compiler_params=pltpu.CompilerParams(vmem_limit_bytes=VMEM_BYTES),
        name="first",
        in_specs=[smem, smem, vmem, vmem],
        out_shape=(
            jax.ShapeDtypeStruct((n_dom * n_sub, blocks * sides, LANES), f32),
            pltpu.VMEM((31, sides, LANES), f32),
        ),
        out_specs=(pl.BlockSpec(memory_space=pltpu.HBM), vmem),
        scratch_shapes=[
            pltpu.VMEM((blocks * sides, LANES), f32),
            pltpu.SemaphoreType.DMA((n_dom * n_sub,)),
        ],
    )


def label_kernel(n_dom, n_sub, macros, planes, cells, slots, recv_rows):
    sides = 2 * macros
    capacity = recv_rows // n_dom

    def body(zone_ref, owner_ref, group_ref, pay_ref):
        d = lax.axis_index("dom")
        shape = (sides, LANES)
        row = iota(shape, 0)
        group = iota(shape, 1) & 3
        owner = owner_ref[...].astype(jnp.float32)
        si, sj = iota((slots, slots), 0), iota((slots, slots), 1)
        column = jnp.sum(jnp.where(si == sj, owner, 0.0), axis=1, keepdims=True)
        lower = jnp.where((column == owner) & (si < sj), 1.0, 0.0)
        position = jnp.sum(lower, axis=0, keepdims=True)
        flat_index = owner * recv_rows + (d * capacity).astype(jnp.float32) + position
        keyed = group_ref[...].astype(jnp.float32) + (d * recv_rows).astype(jnp.float32)

        def spread_lanes(values):
            count = values.shape[1]
            place = iota((count, LANES), 0)
            place = 32 * (place >> 3) + 4 * (place & 7) + 3
            hot = jnp.where(place == iota((count, LANES), 1), 1.0, 0.0)
            rows = jnp.broadcast_to(values, (sides, count))
            return jnp.dot(rows, hot, precision=lax.Precision.HIGHEST)

        index = jnp.where(row < macros, spread_lanes(flat_index), spread_lanes(keyed))
        zone = to_strip(zone_ref[...]).astype(jnp.float32)
        block = jnp.where(group == 2, lane_roll(zone, -1), lane_roll(zone, 1))
        block = jnp.where(group == 3, index, block)
        pay_ref[...] = block

    return pl.pallas_call(
        body,
        compiler_params=pltpu.CompilerParams(vmem_limit_bytes=VMEM_BYTES),
        name="label",
        out_shape=pltpu.VMEM((sides, LANES), jnp.float32),
    )


def inner_kernel(n_dom, n_sub, macros, planes, cells):
    rows = planes + 2 * HALO

    def body(kappa_ref, mu_ref, zone_ref, source_ref, low_ref, high_ref, edge_ref, pot_ref, coef_ref, sx_ref, w_ref):
        k = lax.axis_index("sub")
        sh = Plane((rows, cells))
        at = k * planes - HALO + iota((rows, cells), 0)
        inside, valid = at >= 1, (at >= 0) & (at < n_sub * planes)
        zones = zone_ref[...]
        for i, v in enumerate(table_lookup(zones, kappa_ref, 7) + table_lookup(zones, mu_ref, 8)):
            coef_ref[i] = v

        def macro_step(m, carry):
            def coef(i):
                return jnp.broadcast_to(coef_ref[i, pl.ds(m, 1), :], (rows, cells))

            mass = [coef(t) for t in range(7)]
            mu = [coef(7 + f) for f in range(8)]
            flat, rise, node_flat, node_rise = diagonals(mass, mu, sh)
            for t in range(7):
                diag = flat[t]
                if t in rise:
                    diag = diag + jnp.where(inside, rise[t], 0.0)
                w_ref[t] = EDGE_DAMPING / diag
            w_ref[7] = NODE_DAMPING / (node_flat + jnp.where(inside, node_rise, 0.0))
            node_open = valid & jnp.logical_not(sh.side)

            def loose(t, v):
                return jnp.where(sh.side, 0.0, v) if t in SHARED_TYPES else v

            def node_back(r):
                own = -(((r[0] + r[1]) + (r[2] + r[3])) + ((r[4] + r[5]) + r[6]))
                back = zb(r[2]) + sh.bx(r[0] + zb(r[4])) + sh.by(r[1] + zb(r[5]))
                return jnp.where(node_open, w_ref[7] * (own + back + sh.bxy(r[3] + zb(r[6]))), 0.0)

            def node_grad(c):
                cx, cy, cxy = sh.ax(c), sh.ay(c), sh.axy(c)
                ends = (cx, cy, za(c), cxy, za(cx), za(cy), za(cxy))
                return [jnp.where(valid, end - c, 0.0) for end in ends]

            e, r1 = [], []
            for t in range(7):
                sx_ref[t, 0:HALO, :] = low_ref[m, t]
                sx_ref[t, HALO : HALO + planes, :] = source_ref[m, t]
                sx_ref[t, HALO + planes : rows, :] = high_ref[m, t]
            for t in range(7):
                e.append(loose(t, w_ref[t] * sx_ref[t]))
                r1.append(loose(t, sx_ref[t] - mass[t] * e[t]))
            c1 = node_back(r1)
            grad = node_grad(c1)
            far = (
                sh.ax(e[1]),
                sh.ay(e[0]),
                sh.ax(e[2]),
                za(e[0]),
                sh.ay(e[2]),
                za(e[1]),
                sh.axy(e[2]),
                za(e[3]),
            )
            f = [
                jnp.where(valid, mu[i] * (e[a] + far[i] - e[g]), 0.0)
                for i, (a, _, g) in enumerate(FACE_EDGES)
            ]
            curled = [
                f[0] + f[2] + sh.by(f[1]) + zb(f[3]),
                f[1] + f[4] + sh.bx(f[0]) + zb(f[5]),
                f[3] + f[5] + f[7] + sh.bx(f[2]) + sh.by(f[4]) + sh.bxy(f[6]),
                f[6] + zb(f[7]) - f[0] - f[1],
                -f[2] - f[3],
                -f[4] - f[5],
                -f[6] - f[7],
            ]
            e2, left = [], []
            for t in range(7):
                res = r1[t] - curled[t] - mass[t] * grad[t]
                value = jnp.where(valid, loose(t, e[t] + grad[t] + w_ref[t] * res), 0.0)
                e2.append(value)
                left.append(loose(t, sx_ref[t] - mass[t] * value))
            c2 = node_back(left)
            grad = node_grad(c2)
            for t in range(7):
                edge_ref[m, t] = (e2[t] + grad[t])[HALO : HALO + planes]
            pot_ref[m] = (c1 + c2)[HALO : HALO + planes]
            return carry

        lax.fori_loop(0, macros, macro_step, 0)

    f32 = jnp.float32
    smem = pl.BlockSpec(memory_space=pltpu.SMEM)
    vmem = pl.BlockSpec(memory_space=pltpu.VMEM)
    return pl.pallas_call(
        body,
        compiler_params=pltpu.CompilerParams(vmem_limit_bytes=VMEM_BYTES),
        name="inner",
        in_specs=[smem, smem, vmem, vmem, vmem, vmem],
        out_shape=(
            pltpu.VMEM((macros, 7, planes, cells), f32),
            pltpu.VMEM((macros, planes, cells), f32),
        ),
        scratch_shapes=[
            pltpu.VMEM((15, macros, cells), f32),
            pltpu.VMEM((7, rows, cells), f32),
            pltpu.VMEM((8, rows, cells), f32),
        ],
    )


def group_sum(same, block):
    parts = []
    rest = block
    for _ in range(3):
        parts.append(rest.astype(jnp.bfloat16))
        rest = rest - parts[-1].astype(jnp.float32)
    wide = jnp.concatenate([same] * 3, axis=1)
    return jnp.dot(wide, jnp.concatenate(parts, axis=0), preferred_element_type=jnp.float32)


def prepare_kernel(n_dom, n_sub, macros, planes, cells, slots, recv_rows):
    sides = 2 * macros
    n = n_dom * sides
    total = n * planes

    def body(kappa_ref, mu_ref, *refs):
        same_ref, weight_ref, field_ref, recv_ref = refs[n_dom + 1 :]
        d = lax.axis_index("dom")
        for i in range(n_dom):
            recv_ref[d ^ i] = refs[i][...]
        shape = (n, LANES)
        group = iota(shape, 1) & 3
        index = jnp.concatenate([recv_ref[e] for e in range(n_dom)], axis=0)
        lane = iota(shape, 1)
        row = iota(shape, 0) % sides
        firsts = []
        for e in range(n_dom):
            one = recv_ref[e, 0:1, :]
            firsts.append(jnp.broadcast_to(one, (sides, LANES)))
        firsts = jnp.concatenate(firsts, axis=0)
        flat = []
        for p in range(planes):
            slot = (2 * (row % macros) + row // macros) * planes + p
            here = lane == 32 * (slot >> 3) + 4 * (slot & 7) + 3
            flat.append(jnp.sum(jnp.where(here, firsts, 0.0), axis=1, keepdims=True))
        flat = jnp.concatenate(flat, axis=0).astype(jnp.int32)
        owner = flat // recv_rows
        receive = flat - owner * recv_rows
        table = jnp.zeros((total, LANES), jnp.float32)
        for e in range(n_dom):
            one = recv_ref[e, macros : macros + 1, :]
            table = jnp.where(owner == e, jnp.broadcast_to(one, (total, LANES)), table)
        here = iota((total, LANES), 1) == 32 * (receive >> 3) + 4 * (receive & 7) + 3
        key = jnp.sum(jnp.where(here, table, 0.0), axis=1, keepdims=True)
        square = (total, total)
        diagonal = iota(square, 0) == iota(square, 1)
        key_row = jnp.sum(jnp.where(diagonal, key, 0.0), axis=0, keepdims=True)
        same = jnp.where(key == key_row, 1.0, 0.0).astype(jnp.bfloat16)

        zone = index.astype(jnp.int32)
        mass = table_lookup(zone, kappa_ref, 7)
        mu = table_lookup(zone, mu_ref, 8)
        upper = (iota(shape, 0) % sides) >= macros

        def near(v):
            return jnp.where(upper, lane_roll(v, -1), 0.0)

        def everywhere(v):
            out = jnp.where(group == 0, lane_roll(v, -1), v)
            out = jnp.where(group == 2, lane_roll(v, 1), out)
            return jnp.where(group == 3, lane_roll(v, 2), out)

        near_mu = [near(v) for v in mu]
        near_mass = [near(v) for v in mass]
        e1_low = mass[1] + mu[1] + mu[4] + near_mu[0]
        e2_diag = mass[2] + mu[3] + mu[5] + mu[7] + near_mu[2] + yb(mu[4]) + yb(near_mu[6])
        e5_diag = mass[5] + mu[4] + mu[5]
        node_low = near_mass[0] + yb(mass[1]) + yb(near_mass[3])
        for t in range(7):
            node_low = node_low + mass[t]
        node_diag = node_low + mass[2] + near_mass[4] + yb(mass[5]) + yb(near_mass[6])

        def loose_terms(low):
            diag = {
                0: mass[0] + mu[0] + mu[2] + yb(mu[1]),
                3: mass[3] + mu[0] + mu[1] + mu[6],
                4: mass[4] + mu[2] + mu[3],
                6: mass[6] + mu[6] + mu[7],
            }
            if not low:
                diag[0] = diag[0] + mu[3]
                diag[3] = diag[3] + mu[7]
            al = {t: mass[t] * (EDGE_DAMPING / diag[t]) for t in LOOSE_TYPES}
            be = {t: mass[t] * (1.0 - al[t]) for t in LOOSE_TYPES}
            al_n = {t: near(al[t]) for t in LOOSE_TYPES}
            be_n = {t: near(be[t]) for t in LOOSE_TYPES}
            p0 = al[3] * mu[1] + al_n[0] * near_mu[0]
            r0 = -al[0] * yb(mu[1]) - yb(al_n[3] * near_mu[0])
            p1 = al[4] * mu[3] + al[6] * mu[7] + al_n[0] * near_mu[2] + yb(al_n[3] * near_mu[6])
            r1 = -al[0] * mu[3] - al[3] * mu[7] - al_n[4] * near_mu[2] - yb(al_n[6] * near_mu[6])
            p3 = -(be[0] + be[3] + be[4] + be[6]) - be_n[0] - yb(be_n[3])
            if not low:
                p3 = p3 - be_n[4] - yb(be_n[6])
            return p0, r0, p1, p3, r1

        low_terms, high_terms = loose_terms(True), loose_terms(False)

        def lowest(low, high):
            return jnp.where(group == 0, everywhere(low), everywhere(high))

        blocks = []
        for low, high in (
            (e1_low, e1_low + mu[5]),
            (e2_diag, e2_diag),
            (e5_diag, e5_diag),
            (node_low, node_diag),
        ):
            high_all = everywhere(high)
            low_all = high_all if low is high else jnp.where(group == 0, everywhere(low), high_all)
            blocks.append(jnp.concatenate([low_all] + [high_all] * (planes - 1), axis=0))
        same_ref[...] = same
        summed = group_sum(same, jnp.concatenate(blocks, axis=1))
        for i in range(4):
            damp = EDGE_DAMPING if i < 3 else NODE_DAMPING
            weight_ref[i] = damp / summed[:, LANES * i : LANES * (i + 1)]
        out = [
            mass[1],
            mass[2],
            mass[5],
            mu[1] + near_mu[0],
            mu[3] + mu[7] + near_mu[2] + yb(near_mu[6]),
            mu[4],
            mu[5],
        ]
        out += list(high_terms)
        for i, v in enumerate(out):
            field_ref[i] = everywhere(v)
        for i in range(4):
            field_ref[12 + i] = lowest(low_terms[i], high_terms[i])

    f32 = jnp.float32
    smem = pl.BlockSpec(memory_space=pltpu.SMEM)
    vmem = pl.BlockSpec(memory_space=pltpu.VMEM)
    return pl.pallas_call(
        body,
        compiler_params=pltpu.CompilerParams(vmem_limit_bytes=VMEM_BYTES),
        name="prepare",
        in_specs=[smem, smem] + [vmem] * (n_dom + 1),
        out_shape=(
            pltpu.VMEM((total, total), jnp.bfloat16),
            pltpu.VMEM((4, total, LANES), f32),
            pltpu.VMEM((16, n, LANES), f32),
        ),
        scratch_shapes=[pltpu.VMEM((n_dom, sides, LANES), f32)],
    )


def solve_kernel(n_dom, n_sub, macros, planes, cells):
    sides = 2 * macros
    n = n_dom * sides

    def body(recv_ref, coef_ref, edge_in, pot_in, same_ref, weight_ref, field_ref, edge_ref, pot_ref, one_ref, two_ref, turn_ref):
        k = lax.axis_index("sub")
        d = lax.axis_index("dom")
        shape = (n, LANES)
        group = iota(shape, 1) & 3
        upper = (iota(shape, 0) % sides) >= macros

        def rows_of(layer, at):
            parts = [
                recv_ref[e * n_sub + layer, at * sides : (at + 1) * sides, :] for e in range(n_dom)
            ]
            return jnp.concatenate(parts, axis=0)

        same = same_ref[...]
        edge_mass = [field_ref[i] for i in range(3)]

        def of(v, p):
            return v[p * n : (p + 1) * n]

        def weight(i, p):
            return weight_ref[i, p * n : (p + 1) * n, :]

        def by_layer(at):
            r = [rows_of(layer, at) for layer in range(4)]
            even = (group & 1) == 0
            halves = []
            for i in (0, 2):
                halves.append(jnp.where(even, r[i], lane_roll(r[i + 1], 1)))
                halves.append(jnp.where(even, lane_roll(r[i], -1), r[i + 1]))
            low = group < 2
            out = [jnp.where(low, halves[i], lane_roll(halves[i + 2], 2)) for i in (0, 1)]
            return out + [jnp.where(low, lane_roll(halves[i], -2), halves[i + 2]) for i in (0, 1)]

        def from_below(v):
            return jnp.where(group > 0, lane_roll(v, 1), 0.0)

        def from_above(v):
            return jnp.where(group < 3, lane_roll(v, -1), 0.0)

        def below(f, p):
            return f[p - 1] if p > 0 else from_below(f[planes - 1])

        def above(f, p):
            return f[p + 1] if p < planes - 1 else from_above(f[0])

        def summed(fields):
            block = jnp.concatenate([jnp.concatenate(f, axis=0) for f in fields], axis=1)
            out = group_sum(same, block)
            return [out[:, LANES * i : LANES * (i + 1)] for i in range(len(fields))]

        span = range(planes)

        def edge_terms(r):
            by0 = [yb(r[0][p]) for p in span]
            by2 = [yb(r[2][p]) for p in span]
            out = []
            for p in span:
                value = by0[p] - r[0][p] - r[1][p] - r[2][p]
                out.append(value + below(r[1], p) + below(by2, p))
            return out

        given = [by_layer(p) for p in span]
        more = [by_layer(planes + p) for p in span]
        src = [[given[p][i] for p in span] for i in range(3)]
        sums = summed(src)
        e1 = [[of(sums[i], p) * weight(i, p) for p in span] for i in range(3)]
        r1 = [[src[i][p] - edge_mass[i] * e1[i][p] for p in span] for i in range(3)]
        nodes = [given[p][3] + v for p, v in enumerate(edge_terms(r1))]
        nodes[0] = nodes[0] + jnp.where(upper, from_below(more[1][2]), 0.0)
        (sums,) = summed([nodes])
        c1 = [of(sums, p) * weight(3, p) for p in span]
        for p in span:
            one_ref[0, p], one_ref[1, p], one_ref[2, p] = e1[0][p], e1[1][p], c1[p]

        w4 = [field_ref[5] * (e1[0][p] + ya(e1[1][p]) - e1[2][p]) for p in span]
        w5 = [field_ref[6] * (e1[1][p] + above(e1[0], p) - e1[2][p]) for p in span]
        ahead = [ya(c1[p]) for p in span]
        base, res = [[], [], []], [[], [], []]
        for p in span:
            curled = (
                field_ref[3] * e1[0][p] + w4[p] + below(w5, p),
                field_ref[4] * e1[1][p] + w5[p] + yb(w4[p]),
                -w4[p] - w5[p],
            )
            grad = (ahead[p] - c1[p], above(c1, p) - c1[p], above(ahead, p) - c1[p])
            for i in range(3):
                value = r1[i][p] - curled[i] - edge_mass[i] * grad[i]
                if i < 2:
                    value = value + more[p][i]
                if i == 1 and p == planes - 1:
                    value = value + from_above(more[0][2])
                res[i].append(value)
                base[i].append(e1[i][p] + grad[i])
        sums = summed(res)
        e2 = [[base[i][p] + of(sums[i], p) * weight(i, p) for p in span] for i in range(3)]
        r2 = [[src[i][p] - edge_mass[i] * e2[i][p] for p in span] for i in range(3)]
        nodes = []
        for p, value in enumerate(edge_terms(r2)):
            p0, r0, p1, p3 = (field_ref[(12 if p == 0 else 7) + i] for i in range(4))
            value = value + more[p][3] + p0 * e1[0][p] + r0 * yb(e1[0][p]) + p1 * e1[1][p]
            value = value + field_ref[11] * below(e1[1], p) + p3 * c1[p]
            if p == 0:
                value = value + from_below(more[planes - 1][2])
            if p == 1:
                moved = row_roll(more[1][2], macros)
                value = value + jnp.where(upper, from_below(moved), 0.0)
            if p == planes - 1:
                value = value + from_above(more[2][2])
            nodes.append(value)
        (sums,) = summed([nodes])
        for p in span:
            for i in range(3):
                two_ref[i, p] = e2[i][p]
            two_ref[3, p] = of(sums, p) * weight(3, p)

        strip = (sides, LANES)
        sh = Strip(strip)
        has_below = jnp.where(k == 0, 0.0, 1.0)
        has_above = jnp.where(k == n_sub - 1, 0.0, 1.0)

        def flagged(p, v):
            flag = has_below if p < 0 else has_above if p >= planes else None
            return v if flag is None or v is None else v * flag

        mine = pl.ds(pl.multiple_of(d * sides, sides), sides)
        turned = {}

        def taken(ref, p, i):
            step, plane = p // planes, p % planes
            key = (ref is two_ref, i, plane)
            if key not in turned:
                turned[key] = pltpu.roll(ref[i, plane, mine, :], (LANES - k) & (LANES - 1), 1)
            value = jnp.where(sh.own, lane_roll(turned[key], -step), 0.0)
            return value * (has_below if step < 0 else has_above) if step else value

        my_mass = [coef_ref[t] for t in range(7)]
        my_mu = [coef_ref[7 + f] for f in range(8)]
        loose_r = {}
        step_e = {}
        c_one = {p: taken(one_ref, p, 2) for p in range(-1, planes + 2)}
        faces = {}
        for p in range(-1, planes + 1):
            ea, eb = taken(one_ref, p, 0), taken(one_ref, p, 1)
            faces[p] = (
                my_mu[0] * sh.ax(ea),
                my_mu[1] * ea,
                my_mu[2] * sh.ax(eb),
                my_mu[3] * eb,
                my_mu[6] * sh.axy(eb),
                my_mu[7] * eb,
            )
        for p in range(-1, planes + 1):
            f0, f1, f2, f3, f6, f7 = faces[p]
            types = LOOSE_TYPES if p >= 0 else (4, 6)
            grad = grad_at(c_one[p], c_one[p + 1], sh, types)
            curled = {4: -f2 - f3, 6: -f6 - f7}
            if p >= 0:
                below = faces[p - 1]
                curled[0] = f0 + f2 + yb(f1) + below[3]
                curled[3] = f6 + below[5] - f0 - f1
            step_e[p], loose_r[p] = [None] * 7, [None] * 7
            for t in types:
                weight_t = coef_ref[22 + t] if p == 0 else coef_ref[15 + t]
                value = grad[t] - weight_t * (curled[t] + my_mass[t] * grad[t])
                value = flagged(p, value)
                step_e[p][t] = value
                loose_r[p][t] = -my_mass[t] * value
        c_two = {}
        for p in range(planes + 1):
            node = back_at(loose_r[p], loose_r[p - 1], sh)
            node = (coef_ref[30] if p == 0 else coef_ref[29]) * node
            node = jnp.where(sh.own, taken(two_ref, p, 3), node)
            c_two[p] = flagged(p, node)

        def plain(v):
            return jnp.where(sh.upper, jnp.where(sh.col == 3, lane_roll(v, 3), lane_roll(v, -1)), v)

        for p in range(planes):
            grad = grad_at(c_two[p], c_two[p + 1], sh)
            for t in range(7):
                if t in SHARED_TYPES:
                    start = taken(two_ref, p, SHARED_TYPES.index(t))
                else:
                    start = step_e[p][t]
                turn_ref[t, :, p, :] = plain(start + grad[t])
            turn_ref[7, :, p, :] = plain(c_one[p] + c_two[p])

        x = iota((planes, LANES), 1) & (LAT - 1)

        def overlaid(v, low, high):
            columns = []
            for c in range(8):
                add = jnp.where(x >= LAT - 4, lane_roll(high, 28 - 4 * c), 0.0)
                add = jnp.where(x < 4, lane_roll(low, -4 * c), add)
                columns.append(v[:, LANES * c : LANES * (c + 1)] + add)
            return jnp.concatenate(columns, axis=1)

        def macro_step(m, carry):
            for t in range(7):
                low, high = turn_ref[t, m], turn_ref[t, macros + m]
                edge_ref[m, t] = overlaid(edge_in[m, t], low, high)
            pot_ref[m] = overlaid(pot_in[m], turn_ref[7, m], turn_ref[7, macros + m])
            return carry

        lax.fori_loop(0, macros, macro_step, 0)

    f32 = jnp.float32
    return pl.pallas_call(
        body,
        compiler_params=pltpu.CompilerParams(vmem_limit_bytes=VMEM_BYTES),
        name="solve",
        out_shape=(
            jax.ShapeDtypeStruct((macros, 7, planes, cells), f32),
            jax.ShapeDtypeStruct((macros, planes, cells), f32),
        ),
        scratch_shapes=[
            pltpu.VMEM((3, planes, n, LANES), f32),
            pltpu.VMEM((4, planes, n, LANES), f32),
            pltpu.VMEM((8, sides, planes, LANES), f32),
        ],
    )


def near_core(*values):
    return [pltpu.with_memory_space_constraint(v, pltpu.VMEM) for v in values]


def local_small(source, zone_ids, kappa_table, mu_table, owner_dev, owner_group):
    macros, _, planes, cells = source.shape
    n_dom, n_sub = lax.axis_size("dom"), lax.axis_size("sub")
    sizes = (n_dom, n_sub, macros, planes, cells)
    lists = (owner_dev.shape[1], owner_group.shape[1])
    up = [(i, i + 1) for i in range(n_sub - 1)]
    down = [(i + 1, i) for i in range(n_sub - 1)]
    tables = (kappa_table.T, mu_table.T)
    far = [pltpu.with_memory_space_constraint(v, pltpu.HBM) for v in (*tables, zone_ids, source)]
    pay, coef = first_kernel(*sizes)(*far)
    recv = lax.all_to_all(pay, ("dom", "sub"), 0, 0)
    labels = label_kernel(*sizes, *lists)(zone_ids, owner_dev, owner_group)
    labels = [labels]
    for i in range(1, n_dom):
        route = [(e, e ^ i) for e in range(n_dom)]
        labels.append(lax.ppermute(labels[0], "dom", route))
    low = lax.ppermute(source[:, :, planes - HALO :], "sub", up)
    high = lax.ppermute(source[:, :, :HALO], "sub", down)
    edge, pot = inner_kernel(*sizes)(*tables, zone_ids, source, *near_core(low, high))
    fields = prepare_kernel(*sizes, *lists)(*tables, *near_core(*labels, pot))
    return solve_kernel(*sizes)(*near_core(recv, coef, edge, pot, *fields))


def fits_small(mesh, source, owner_dev, owner_group):
    macros = source.shape[0] // mesh.shape["dom"]
    planes = source.shape[2] // mesh.shape["sub"]
    return (
        macros == 4
        and planes == 4
        and source.shape[3] == LAT * LAT
        and mesh.shape["sub"] == 4
        and owner_dev.shape[1] == 2 * macros * planes
        and owner_group.shape[1] == 32
        and mesh.shape["dom"] in (1, 2, 4, 8)
    )


def solution(mesh):
    in_specs = (
        P("dom", None, "sub", None),
        P("dom", None),
        P(),
        P(),
        P("dom", None),
        P("dom", None),
    )
    out_specs = (P("dom", None, "sub", None), P("dom", "sub", None))

    def step(source, zone_ids, kappa_table, mu_table, owner_dev, owner_group):
        body = local_small if fits_small(mesh, source, owner_dev, owner_group) else local
        mapped = jax.shard_map(
            body, mesh=mesh, in_specs=in_specs, out_specs=out_specs, check_vma=False
        )
        return mapped(source, zone_ids, kappa_table, mu_table, owner_dev, owner_group)

    return step
```

```python
import jax
import jax.numpy as jnp
from jax import lax
from jax.experimental import pallas as pl
from jax.experimental.pallas import tpu as pltpu
from jax.sharding import PartitionSpec as P


LAT = 32
SWEEPS = 2


EDGE_OFFSETS = ((0, 0, 1), (0, 1, 0), (1, 0, 0), (0, 1, 1), (1, 0, 1), (1, 1, 0), (1, 1, 1))
FACE_EDGES = (
    (0, 1, 3),
    (1, 0, 3),
    (0, 2, 4),
    (2, 0, 4),
    (1, 2, 5),
    (2, 1, 5),
    (3, 2, 6),
    (2, 3, 6),
)
SHARED_TYPES = (1, 2, 5)
EDGE_DAMPING = 0.6
NODE_DAMPING = 0.8


def with_halo(block, sides, width):
    for axis, dim in sides:
        count = lax.axis_size(axis)
        forward = [(i, i + 1) for i in range(count - 1)]
        backward = [(target, source) for source, target in forward]
        low = lax.ppermute(
            lax.slice_in_dim(block, block.shape[dim] - width, None, axis=dim), axis, forward
        )
        high = lax.ppermute(lax.slice_in_dim(block, 0, width, axis=dim), axis, backward)
        block = jnp.concatenate([low, block, high], axis=dim)
    return block


def from_behind(block, axis, distance):
    devices = range(lax.axis_size(axis))
    route = [(i - distance, i) for i in devices if i - distance in devices]
    return lax.ppermute(block, axis, route)


def shift_ahead(values, rise_y, rise_x):
    offset = rise_y * LAT + rise_x
    if offset == 0:
        return values
    padding = jnp.zeros(values.shape[:-1] + (offset,), values.dtype)
    shifted = jnp.concatenate([values[..., offset:], padding], axis=-1)
    if rise_x:
        column = jnp.arange(values.shape[-1]) % LAT
        shifted = jnp.where(column < LAT - rise_x, shifted, jnp.zeros_like(shifted))
    return shifted


def shift_behind(values, rise_y, rise_x):
    offset = rise_y * LAT + rise_x
    if offset == 0:
        return values
    padding = jnp.zeros(values.shape[:-1] + (offset,), values.dtype)
    shifted = jnp.concatenate([padding, values[..., :-offset]], axis=-1)
    if rise_x:
        column = jnp.arange(values.shape[-1]) % LAT
        shifted = jnp.where(column >= rise_x, shifted, jnp.zeros_like(shifted))
    return shifted


def apply_operator(padded, halo_width, extra_planes, first_plane, mass_coef, curl_coef):
    planes = padded.shape[2] - 2 * halo_width
    face_count = planes + extra_planes + 1
    first_face = halo_width - extra_planes - 1
    face_planes = first_plane - extra_planes - 1 + jnp.arange(face_count)
    face_valid = (face_planes >= 0)[None, :, None]
    result = [
        mass_coef[edge_type][:, None, :]
        * padded[:, edge_type, halo_width - extra_planes : halo_width + planes]
        for edge_type in range(7)
    ]
    for face_index, (first_edge, second_edge, diagonal_edge) in enumerate(FACE_EDGES):
        rise_z, rise_y, rise_x = EDGE_OFFSETS[first_edge]
        far_values = shift_ahead(
            padded[:, second_edge, first_face + rise_z : first_face + rise_z + face_count],
            rise_y,
            rise_x,
        )
        circulation = (
            padded[:, first_edge, first_face : first_face + face_count]
            + far_values
            - padded[:, diagonal_edge, first_face : first_face + face_count]
        )
        weighted = jnp.where(face_valid, curl_coef[face_index][:, None, :] * circulation, 0.0)
        result[first_edge] = result[first_edge] + weighted[:, 1:]
        result[diagonal_edge] = result[diagonal_edge] - weighted[:, 1:]
        result[second_edge] = result[second_edge] + shift_behind(
            weighted[:, 1 - rise_z : 1 - rise_z + planes + extra_planes], rise_y, rise_x
        )
    return jnp.stack(result, axis=1)


def edge_diagonal(mass_coef, curl_coef, first_plane, planes):
    inside = (first_plane + jnp.arange(planes) >= 1)[None, :, None]
    flat_planes = jnp.zeros((1, planes, 1), mass_coef.dtype)
    diagonal = [mass_coef[edge_type][:, None, :] + flat_planes for edge_type in range(7)]
    for face_index, (first_edge, second_edge, diagonal_edge) in enumerate(FACE_EDGES):
        rise_z, rise_y, rise_x = EDGE_OFFSETS[first_edge]
        own_term = curl_coef[face_index][:, None, :]
        diagonal[first_edge] = diagonal[first_edge] + own_term
        diagonal[diagonal_edge] = diagonal[diagonal_edge] + own_term
        behind_term = shift_behind(curl_coef[face_index], rise_y, rise_x)[:, None, :] + flat_planes
        if rise_z:
            behind_term = jnp.where(inside, behind_term, 0.0)
        diagonal[second_edge] = diagonal[second_edge] + behind_term
    return jnp.stack(diagonal, axis=1)


def node_diagonal(mass_coef, first_plane, planes):
    inside = (first_plane + jnp.arange(planes) >= 1)[None, :, None]
    total = jnp.zeros((mass_coef.shape[1], planes, mass_coef.shape[2]), mass_coef.dtype)
    for edge_type in range(7):
        rise_z, rise_y, rise_x = EDGE_OFFSETS[edge_type]
        total = total + mass_coef[edge_type][:, None, :]
        behind_term = shift_behind(mass_coef[edge_type], rise_y, rise_x)[:, None, :] + jnp.zeros(
            (1, planes, 1), mass_coef.dtype
        )
        if rise_z:
            behind_term = jnp.where(inside, behind_term, 0.0)
        total = total + behind_term
    return total


def node_residual(lowered, planes):
    total = jnp.zeros((lowered.shape[0], planes, lowered.shape[3]), lowered.dtype)
    for edge_type in range(7):
        rise_z, rise_y, rise_x = EDGE_OFFSETS[edge_type]
        total = (
            total
            + shift_behind(lowered[:, edge_type, 1 - rise_z : 1 - rise_z + planes], rise_y, rise_x)
            - lowered[:, edge_type, 1:]
        )
    return total


def gradient(raised, planes):
    result = []
    for edge_type in range(7):
        rise_z, rise_y, rise_x = EDGE_OFFSETS[edge_type]
        result.append(
            shift_ahead(raised[:, rise_z : rise_z + planes], rise_y, rise_x) - raised[:, :planes]
        )
    return jnp.stack(result, axis=1)


def edge_sides(values):
    macro_count, type_count, plane_count, _ = values.shape
    lattice = values.reshape(macro_count, type_count, plane_count, LAT, LAT)
    chosen = jnp.stack([lattice[:, edge_type] for edge_type in SHARED_TYPES], axis=1)
    sides = jnp.stack([chosen[..., 0], chosen[..., LAT - 1]], axis=1)
    return jnp.transpose(sides, (0, 1, 3, 2, 4)).reshape(-1, 3 * LAT)


def insert_edges(values, blocks):
    macro_count, type_count, plane_count, _ = values.shape
    shaped = blocks.reshape(macro_count, 2, plane_count, 3, LAT)
    shaped = jnp.transpose(shaped, (0, 1, 3, 2, 4))
    lattice = values.reshape(macro_count, type_count, plane_count, LAT, LAT)
    for side_index, column in ((0, 0), (1, LAT - 1)):
        for slot_type, edge_type in enumerate(SHARED_TYPES):
            lattice = lattice.at[:, edge_type, :, :, column].set(shaped[:, side_index, slot_type])
    return lattice.reshape(values.shape)


def node_sides(values):
    macro_count, plane_count, _ = values.shape
    lattice = values.reshape(macro_count, plane_count, LAT, LAT)
    sides = jnp.stack([lattice[..., 0], lattice[..., LAT - 1]], axis=1)
    return sides.reshape(-1, LAT)


def insert_nodes(values, blocks):
    macro_count, plane_count, _ = values.shape
    shaped = blocks.reshape(macro_count, 2, plane_count, LAT)
    lattice = values.reshape(macro_count, plane_count, LAT, LAT)
    for side_index, column in ((0, 0), (1, LAT - 1)):
        lattice = lattice.at[:, :, :, column].set(shaped[:, side_index])
    return lattice.reshape(values.shape)


def local(source, zone_ids, kappa_table, mu_table, owner_dev, owner_group):
    macro_count, type_count, planes, cell_count = source.shape
    first_plane = lax.axis_index("sub") * planes
    onehot = (jnp.arange(kappa_table.shape[0])[:, None] == zone_ids.reshape(1, -1)).astype(
        jnp.float32
    )
    mass_coef = jnp.dot(kappa_table.T, onehot, precision=lax.Precision.HIGHEST).reshape(
        type_count, macro_count, cell_count
    )
    curl_coef = jnp.dot(mu_table.T, onehot, precision=lax.Precision.HIGHEST).reshape(
        mu_table.shape[1], macro_count, cell_count
    )
    peer_count = lax.axis_size("dom")
    recv_rows = owner_group.shape[1]
    capacity = recv_rows // peer_count
    slot_count = owner_dev.shape[1]
    owner_of = owner_dev[0]
    groups = owner_group[0]
    earlier = jnp.arange(slot_count)[None, :] < jnp.arange(slot_count)[:, None]
    position = jnp.sum((owner_of[:, None] == owner_of[None, :]) & earlier, axis=1)
    slot_place = owner_of * capacity + position
    spread = (jnp.arange(recv_rows)[:, None] == slot_place[None, :]).astype(jnp.float32)
    same_group = (groups[:, None] == groups[None, :]).astype(jnp.float32)

    def owner_sum(received):
        summed = jnp.dot(
            same_group, received.reshape(recv_rows, -1), precision=lax.Precision.HIGHEST
        )
        return lax.all_to_all(
            summed.reshape(peer_count, capacity, -1), "dom", split_axis=0, concat_axis=0, tiled=True
        )

    def assemble(blocks):
        outgoing = jnp.dot(spread, blocks, precision=lax.Precision.HIGHEST).reshape(
            peer_count, capacity, blocks.shape[1]
        )
        returned = owner_sum(
            lax.all_to_all(outgoing, "dom", split_axis=0, concat_axis=0, tiled=True)
        )
        return jnp.take(returned.reshape(recv_rows, -1), slot_place, axis=0)

    rim_width = 2

    def rimmed(values):
        return with_halo(values, (("sub", 2),), rim_width)

    edge_diag = edge_diagonal(mass_coef, curl_coef, first_plane, planes)
    node_diag = node_diagonal(mass_coef, first_plane, planes)
    edge_width = 3 * LAT
    first_blocks = [edge_sides(edge_diag), node_sides(node_diag)]
    diag_sums = assemble(jnp.concatenate(first_blocks, axis=1))
    full_edge_diag = insert_edges(edge_diag, diag_sums[:, :edge_width])
    full_node_diag = insert_nodes(node_diag, diag_sums[:, edge_width : edge_width + LAT])
    source_below = from_behind(source[:, :, planes - 1 :], "sub", 1)
    edge_field = jnp.zeros_like(source)
    potential = jnp.zeros((macro_count, planes, cell_count), jnp.float32)
    for sweep_index in range(SWEEPS):
        if sweep_index == 0:
            residual = source
            residual_sum = assemble(edge_sides(residual))
        else:
            residual = source - apply_operator(
                rimmed(edge_field), rim_width, 0, first_plane, mass_coef, curl_coef
            )
            residual_sum = assemble(edge_sides(residual))
        full_residual = insert_edges(residual, residual_sum)
        edge_field = edge_field + EDGE_DAMPING * full_residual / full_edge_diag
        padded = rimmed(edge_field)
        lowered = jnp.concatenate([source_below, source], axis=2) - apply_operator(
            padded, 2, 1, first_plane, mass_coef, curl_coef
        )
        node_values = node_residual(lowered, planes)
        node_sum = assemble(node_sides(node_values))
        correction = NODE_DAMPING * insert_nodes(node_values, node_sum) / full_node_diag
        plane_above = from_behind(correction[:, :1], "sub", -1)
        edge_field = edge_field + gradient(
            jnp.concatenate([correction, plane_above], axis=1), planes
        )
        potential = potential + correction
    return (edge_field, potential)


LANES = 128
HALO = 2
VMEM_BYTES = 24 * 1024 * 1024
LOOSE_TYPES = (0, 3, 4, 6)


def lane_roll(v, s):
    s = s % v.shape[-1]
    return pltpu.roll(v, s, v.ndim - 1) if s else v


def row_roll(v, s):
    s = s % v.shape[0]
    return pltpu.roll(v, s, 0) if s else v


def iota(shape, dim):
    return lax.broadcasted_iota(jnp.int32, shape, dim)


def zb(v):
    return row_roll(v, 1)


def za(v):
    return row_roll(v, -1)


class Plane:
    def __init__(self, shape):
        self.lane = iota(shape, 1)
        self.x = self.lane & (LAT - 1)
        self.cells = shape[1]
        self.side = (self.x == 0) | (self.x == LAT - 1)

    def ax(self, v):
        return jnp.where(self.x < LAT - 1, lane_roll(v, -1), 0.0)

    def ay(self, v):
        return jnp.where(self.lane < self.cells - LAT, lane_roll(v, -LAT), 0.0)

    def bx(self, v):
        return jnp.where(self.x > 0, lane_roll(v, 1), 0.0)

    def by(self, v):
        return jnp.where(self.lane >= LAT, lane_roll(v, LAT), 0.0)

    def bxy(self, v):
        return jnp.where((self.lane >= LAT) & (self.x > 0), lane_roll(v, LAT + 1), 0.0)

    def axy(self, v):
        inner = (self.lane < self.cells - LAT) & (self.x < LAT - 1)
        return jnp.where(inner, lane_roll(v, -LAT - 1), 0.0)


def yb(v):
    lane = iota(v.shape, 1)
    first = jnp.where(lane < 4, 0.0, lane_roll(v, 36))
    return jnp.where(lane < 32, first, lane_roll(v, 32))


def ya(v):
    lane = iota(v.shape, 1)
    last = jnp.where(lane >= 124, 0.0, lane_roll(v, -36))
    return jnp.where(lane >= 96, last, lane_roll(v, -32))


class Strip:
    def __init__(self, shape):
        half = shape[0] // 2
        self.col = iota(shape, 1) & 3
        self.upper = iota(shape, 0) >= half
        self.own = self.col == 0

    def ax(self, v):
        wrap = jnp.where(self.upper, lane_roll(v, 3), 0.0)
        step = jnp.where(self.upper & self.own, 0.0, lane_roll(v, -1))
        return jnp.where(self.col == 3, wrap, step)

    def bx(self, v):
        wrap = jnp.where(self.upper, lane_roll(v, -3), 0.0)
        step = jnp.where(self.upper & (self.col == 1), 0.0, lane_roll(v, 1))
        return jnp.where(self.own, wrap, step)

    def ay(self, v):
        return ya(v)

    def by(self, v):
        return yb(v)

    def bxy(self, v):
        return yb(self.bx(v))

    def axy(self, v):
        return ya(self.ax(v))


def to_strip(v):
    lane = iota((v.shape[0], LANES), 1)
    block = (lane & 31) >> 2
    low = jnp.zeros((v.shape[0], LANES), v.dtype)
    high = low
    for c in range(8):
        column = v[:, LANES * c : LANES * (c + 1)]
        low = jnp.where(block == c, lane_roll(column, 4 * c), low)
        high = jnp.where(block == c, lane_roll(column, 4 * c - 28), high)
    high = jnp.where((lane & 3) == 0, lane_roll(high, -3), lane_roll(high, 1))
    return jnp.concatenate([low, high], axis=0)


def plus(*terms):
    total = None
    for term in terms:
        if term is not None:
            total = term if total is None else total + term
    return total


def on(f, v):
    return None if v is None else f(v)


def minus(v):
    return on(lambda a: -a, v)


def times(c, v):
    return on(lambda a: c * a, v)


def table_lookup(zone, table_ref, width):
    out = [jnp.zeros(zone.shape, jnp.float32)] * width
    for z in range(table_ref.shape[1]):
        hit = zone == z
        out = [jnp.where(hit, table_ref[i, z], v) for i, v in enumerate(out)]
    return out


def diagonals(mass, mu, sh):
    flat = [
        mass[0] + mu[0] + mu[2] + sh.by(mu[1]),
        mass[1] + mu[1] + mu[4] + sh.bx(mu[0]),
        mass[2] + mu[3] + mu[5] + mu[7] + sh.bx(mu[2]) + sh.by(mu[4]) + sh.bxy(mu[6]),
        mass[3] + mu[0] + mu[1] + mu[6],
        mass[4] + mu[2] + mu[3],
        mass[5] + mu[4] + mu[5],
        mass[6] + mu[6] + mu[7],
    ]
    rise = {0: mu[3], 1: mu[5], 3: mu[7]}
    node_flat = sh.bx(mass[0]) + sh.by(mass[1]) + sh.bxy(mass[3])
    for t in range(7):
        node_flat = node_flat + mass[t]
    node_rise = mass[2] + sh.bx(mass[4]) + sh.by(mass[5]) + sh.bxy(mass[6])
    return flat, rise, node_flat, node_rise


def grad_at(c, c_up, sh, types=range(7)):
    moves = (sh.ax, sh.ay, lambda v: v, sh.axy, sh.ax, sh.ay, sh.axy)
    out = [None] * 7
    for t in types:
        out[t] = plus(on(moves[t], c_up if EDGE_OFFSETS[t][0] else c), minus(c))
    return out


def back_at(r, r_below, sh):
    return plus(
        minus(plus(*r)),
        r_below[2],
        on(sh.bx, plus(r[0], r_below[4])),
        on(sh.by, plus(r[1], r_below[5])),
        on(sh.bxy, plus(r[3], r_below[6])),
    )


NONE7 = [None] * 7


def first_kernel(n_dom, n_sub, macros, planes, cells):
    sides = 2 * macros
    blocks = 2 * planes
    half = planes * sides

    def body(kappa_ref, mu_ref, zone_ref, source_ref, pay_ref, coef_ref, hold_ref, sems):
        k = lax.axis_index("sub")
        shape = (sides, LANES)
        sh = Strip(shape)
        row = iota(shape, 0)
        group = iota(shape, 1) & 3
        zone = to_strip(zone_ref[...])
        mass = table_lookup(zone, kappa_ref, 7)
        mu = table_lookup(zone, mu_ref, 8)
        flat, rise, node_flat, node_rise = diagonals(mass, mu, sh)
        w = [EDGE_DAMPING / (flat[t] + rise[t] if t in rise else flat[t]) for t in range(7)]
        w_low = [EDGE_DAMPING / flat[t] if t in rise else w[t] for t in range(7)]
        lowest = k == 0
        w_zero = [jnp.where(lowest, w_low[t], w[t]) for t in range(7)]
        nw = NODE_DAMPING / (node_flat + node_rise)
        nw_zero = jnp.where(lowest, NODE_DAMPING / node_flat, nw)
        for i, v in enumerate(mass + mu + w + w_zero + [nw, nw_zero]):
            coef_ref[i] = v
        has_below = jnp.where(lowest, 0.0, 1.0)
        has_above = jnp.where(k == n_sub - 1, 0.0, 1.0)

        def loose(t, v):
            return jnp.where(sh.own, 0.0, v) if t in SHARED_TYPES else v

        def flagged(p, v):
            flag = has_below if p < 0 else has_above if p >= planes else None
            return v if flag is None or v is None else v * flag

        src = {p: [to_strip(source_ref[:, t, p, :]) for t in range(7)] for p in range(planes)}
        e1, r1 = {}, {}
        for p in range(planes):
            wp = w_zero if p == 0 else w
            e1[p] = [loose(t, wp[t] * src[p][t]) for t in range(7)]
            r1[p] = [loose(t, src[p][t] - mass[t] * e1[p][t]) for t in range(7)]
        n1, c1 = {}, {}
        for p in range(planes + 1):
            n1[p] = back_at(r1.get(p, NONE7), r1.get(p - 1, NONE7), sh)
            c1[p] = jnp.where(sh.own, 0.0, (nw_zero if p == 0 else nw) * n1[p])
            c1[p] = flagged(p, c1[p])
        faces = {}
        for p in range(-1, planes):
            e, e_up = e1.get(p, NONE7), e1.get(p + 1, NONE7)
            far = (
                on(sh.ax, e[1]),
                on(sh.ay, e[0]),
                on(sh.ax, e[2]),
                e_up[0],
                on(sh.ay, e[2]),
                e_up[1],
                on(sh.axy, e[2]),
                e_up[3],
            )
            faces[p] = [
                flagged(p, times(mu[f], plus(e[a], far[f], minus(e[g]))))
                for f, (a, _, g) in enumerate(FACE_EDGES)
            ]
        res, r2 = {}, {}
        none8 = [None] * 8
        for p in range(-1, planes + 1):
            f, f_below = faces.get(p, none8), faces.get(p - 1, none8)
            curled = [
                plus(f[0], f[2], on(sh.by, f[1]), f_below[3]),
                plus(f[1], f[4], on(sh.bx, f[0]), f_below[5]),
                plus(f[3], f[5], f[7], on(sh.bx, f[2]), on(sh.by, f[4]), on(sh.bxy, f[6])),
                plus(f[6], f_below[7], minus(f[0]), minus(f[1])),
                minus(plus(f[2], f[3])),
                minus(plus(f[4], f[5])),
                minus(plus(f[6], f[7])),
            ]
            grad = grad_at(c1.get(p), c1.get(p + 1), sh)
            wp = w_zero if p == 0 else w
            res[p], r2[p] = [], []
            for t in range(7):
                g = grad[t]
                value = plus(
                    r1.get(p, NONE7)[t], minus(curled[t]), minus(times(mass[t], g))
                )
                res[p].append(value)
                e2 = plus(e1.get(p, NONE7)[t], g, times(wp[t], value))
                s = src[p][t] if p in src else None
                left = flagged(p, plus(s, minus(times(mass[t], e2))))
                r2[p].append(on(lambda v: loose(t, v), left))
        n2 = {p: back_at(r2.get(p, NONE7), r2.get(p - 1, NONE7), sh) for p in range(-1, planes + 2)}

        def merge(g0, g1, g2, g3):
            out = jnp.where(group == 1, lane_roll(g1, 1), g0)
            out = jnp.where(group == 2, lane_roll(g2, 2), out)
            return jnp.where(group == 3, lane_roll(g3, 3), out)

        high = jnp.where(row < macros, row_roll(n2[planes + 1], macros), n1[planes])
        spare = [flagged(-1, res[-1][2]), high, n2[-1], n2[planes]]
        for p in range(planes):
            hold_ref[p * sides : (p + 1) * sides, :] = merge(src[p][1], src[p][2], src[p][5], n1[p])
            at = planes + p
            hold_ref[at * sides : (at + 1) * sides, :] = merge(res[p][1], res[p][2], spare[p], n2[p])
        copies = [
            pltpu.make_async_copy(
                hold_ref.at[pl.ds(dest % 2 * half, half)], pay_ref.at[dest], sems.at[dest]
            )
            for dest in range(n_dom * n_sub)
        ]
        for copy in copies:
            copy.start()
        for copy in copies:
            copy.wait()

    f32 = jnp.float32
    smem = pl.BlockSpec(memory_space=pltpu.SMEM)
    vmem = pl.BlockSpec(memory_space=pltpu.VMEM)
    return pl.pallas_call(
        body,
        compiler_params=pltpu.CompilerParams(vmem_limit_bytes=VMEM_BYTES),
        name="first",
        in_specs=[smem, smem, vmem, vmem],
        out_shape=(
            jax.ShapeDtypeStruct((n_dom * n_sub, half, LANES), f32),
            pltpu.VMEM((31, sides, LANES), f32),
        ),
        out_specs=(pl.BlockSpec(memory_space=pltpu.HBM), vmem),
        scratch_shapes=[
            pltpu.VMEM((blocks * sides, LANES), f32),
            pltpu.SemaphoreType.DMA((n_dom * n_sub,)),
        ],
    )


def label_kernel(n_dom, n_sub, macros, planes, cells, slots, recv_rows):
    sides = 2 * macros
    capacity = recv_rows // n_dom

    def body(zone_ref, owner_ref, group_ref, pay_ref):
        d = lax.axis_index("dom")
        shape = (sides, LANES)
        row = iota(shape, 0)
        group = iota(shape, 1) & 3
        owner = owner_ref[...].astype(jnp.float32)
        si, sj = iota((slots, slots), 0), iota((slots, slots), 1)
        column = jnp.sum(jnp.where(si == sj, owner, 0.0), axis=1, keepdims=True)
        lower = jnp.where((column == owner) & (si < sj), 1.0, 0.0)
        position = jnp.sum(lower, axis=0, keepdims=True)
        flat_index = owner * recv_rows + (d * capacity).astype(jnp.float32) + position
        keyed = group_ref[...].astype(jnp.float32) + (d * recv_rows).astype(jnp.float32)

        def spread_lanes(values):
            count = values.shape[1]
            place = iota((count, LANES), 0)
            place = 32 * (place >> 3) + 4 * (place & 7) + 3
            hot = jnp.where(place == iota((count, LANES), 1), 1.0, 0.0)
            rows = jnp.broadcast_to(values, (sides, count))
            return jnp.dot(rows, hot, precision=lax.Precision.HIGHEST)

        index = jnp.where(row < macros, spread_lanes(flat_index), spread_lanes(keyed))
        zone = to_strip(zone_ref[...]).astype(jnp.float32)
        block = jnp.where(group == 2, lane_roll(zone, -1), lane_roll(zone, 1))
        block = jnp.where(group == 3, index, block)
        pay_ref[...] = block

    return pl.pallas_call(
        body,
        compiler_params=pltpu.CompilerParams(vmem_limit_bytes=VMEM_BYTES),
        name="label",
        out_shape=pltpu.VMEM((sides, LANES), jnp.float32),
    )


def inner_kernel(n_dom, n_sub, macros, planes, cells):
    rows = planes + 2 * HALO

    def body(kappa_ref, mu_ref, zone_ref, source_ref, low_ref, high_ref, edge_ref, pot_ref, coef_ref, sx_ref, w_ref):
        k = lax.axis_index("sub")
        sh = Plane((rows, cells))
        at = k * planes - HALO + iota((rows, cells), 0)
        inside, valid = at >= 1, (at >= 0) & (at < n_sub * planes)
        zones = zone_ref[...]
        for i, v in enumerate(table_lookup(zones, kappa_ref, 7) + table_lookup(zones, mu_ref, 8)):
            coef_ref[i] = v

        def macro_step(m, carry):
            def coef(i):
                return jnp.broadcast_to(coef_ref[i, pl.ds(m, 1), :], (rows, cells))

            mass = [coef(t) for t in range(7)]
            mu = [coef(7 + f) for f in range(8)]
            flat, rise, node_flat, node_rise = diagonals(mass, mu, sh)
            for t in range(7):
                diag = flat[t]
                if t in rise:
                    diag = diag + jnp.where(inside, rise[t], 0.0)
                w_ref[t] = EDGE_DAMPING / diag
            w_ref[7] = NODE_DAMPING / (node_flat + jnp.where(inside, node_rise, 0.0))
            node_open = valid & jnp.logical_not(sh.side)

            def loose(t, v):
                return jnp.where(sh.side, 0.0, v) if t in SHARED_TYPES else v

            def node_back(r):
                own = -(((r[0] + r[1]) + (r[2] + r[3])) + ((r[4] + r[5]) + r[6]))
                back = zb(r[2]) + sh.bx(r[0] + zb(r[4])) + sh.by(r[1] + zb(r[5]))
                return jnp.where(node_open, w_ref[7] * (own + back + sh.bxy(r[3] + zb(r[6]))), 0.0)

            def node_grad(c):
                cx, cy, cxy = sh.ax(c), sh.ay(c), sh.axy(c)
                ends = (cx, cy, za(c), cxy, za(cx), za(cy), za(cxy))
                return [jnp.where(valid, end - c, 0.0) for end in ends]

            e, r1 = [], []
            for t in range(7):
                sx_ref[t, 0:HALO, :] = low_ref[m, t]
                sx_ref[t, HALO : HALO + planes, :] = source_ref[m, t]
                sx_ref[t, HALO + planes : rows, :] = high_ref[m, t]
            for t in range(7):
                e.append(loose(t, w_ref[t] * sx_ref[t]))
                r1.append(loose(t, sx_ref[t] - mass[t] * e[t]))
            c1 = node_back(r1)
            grad = node_grad(c1)
            far = (
                sh.ax(e[1]),
                sh.ay(e[0]),
                sh.ax(e[2]),
                za(e[0]),
                sh.ay(e[2]),
                za(e[1]),
                sh.axy(e[2]),
                za(e[3]),
            )
            f = [
                jnp.where(valid, mu[i] * (e[a] + far[i] - e[g]), 0.0)
                for i, (a, _, g) in enumerate(FACE_EDGES)
            ]
            curled = [
                f[0] + f[2] + sh.by(f[1]) + zb(f[3]),
                f[1] + f[4] + sh.bx(f[0]) + zb(f[5]),
                f[3] + f[5] + f[7] + sh.bx(f[2]) + sh.by(f[4]) + sh.bxy(f[6]),
                f[6] + zb(f[7]) - f[0] - f[1],
                -f[2] - f[3],
                -f[4] - f[5],
                -f[6] - f[7],
            ]
            e2, left = [], []
            for t in range(7):
                res = r1[t] - curled[t] - mass[t] * grad[t]
                value = jnp.where(valid, loose(t, e[t] + grad[t] + w_ref[t] * res), 0.0)
                e2.append(value)
                left.append(loose(t, sx_ref[t] - mass[t] * value))
            c2 = node_back(left)
            grad = node_grad(c2)
            for t in range(7):
                edge_ref[m, t] = (e2[t] + grad[t])[HALO : HALO + planes]
            pot_ref[m] = (c1 + c2)[HALO : HALO + planes]
            return carry

        lax.fori_loop(0, macros, macro_step, 0)

    f32 = jnp.float32
    smem = pl.BlockSpec(memory_space=pltpu.SMEM)
    vmem = pl.BlockSpec(memory_space=pltpu.VMEM)
    return pl.pallas_call(
        body,
        compiler_params=pltpu.CompilerParams(vmem_limit_bytes=VMEM_BYTES),
        name="inner",
        in_specs=[smem, smem, vmem, vmem, vmem, vmem],
        out_shape=(
            pltpu.VMEM((macros, 7, planes, cells), f32),
            pltpu.VMEM((macros, planes, cells), f32),
        ),
        scratch_shapes=[
            pltpu.VMEM((15, macros, cells), f32),
            pltpu.VMEM((7, rows, cells), f32),
            pltpu.VMEM((8, rows, cells), f32),
        ],
    )


def group_sum(same, block):
    parts = []
    rest = block
    for _ in range(3):
        parts.append(rest.astype(jnp.bfloat16))
        rest = rest - parts[-1].astype(jnp.float32)
    wide = jnp.concatenate([same] * 3, axis=1)
    return jnp.dot(wide, jnp.concatenate(parts, axis=0), preferred_element_type=jnp.float32)


def prepare_kernel(n_dom, n_sub, macros, planes, cells, slots, recv_rows):
    sides = 2 * macros
    n = n_dom * sides
    total = n * planes

    def body(kappa_ref, mu_ref, *refs):
        same_ref, weight_ref, field_ref, recv_ref = refs[n_dom + 1 :]
        d = lax.axis_index("dom")
        for i in range(n_dom):
            recv_ref[d ^ i] = refs[i][...]
        shape = (n, LANES)
        group = iota(shape, 1) & 3
        index = jnp.concatenate([recv_ref[e] for e in range(n_dom)], axis=0)
        lane = iota(shape, 1)
        row = iota(shape, 0) % sides
        firsts = []
        for e in range(n_dom):
            one = recv_ref[e, 0:1, :]
            firsts.append(jnp.broadcast_to(one, (sides, LANES)))
        firsts = jnp.concatenate(firsts, axis=0)
        flat = []
        for p in range(planes):
            slot = (2 * (row % macros) + row // macros) * planes + p
            here = lane == 32 * (slot >> 3) + 4 * (slot & 7) + 3
            flat.append(jnp.sum(jnp.where(here, firsts, 0.0), axis=1, keepdims=True))
        flat = jnp.concatenate(flat, axis=0).astype(jnp.int32)
        owner = flat // recv_rows
        receive = flat - owner * recv_rows
        table = jnp.zeros((total, LANES), jnp.float32)
        for e in range(n_dom):
            one = recv_ref[e, macros : macros + 1, :]
            table = jnp.where(owner == e, jnp.broadcast_to(one, (total, LANES)), table)
        here = iota((total, LANES), 1) == 32 * (receive >> 3) + 4 * (receive & 7) + 3
        key = jnp.sum(jnp.where(here, table, 0.0), axis=1, keepdims=True)
        square = (total, total)
        diagonal = iota(square, 0) == iota(square, 1)
        key_row = jnp.sum(jnp.where(diagonal, key, 0.0), axis=0, keepdims=True)
        same = jnp.where(key == key_row, 1.0, 0.0).astype(jnp.bfloat16)

        zone = index.astype(jnp.int32)
        mass = table_lookup(zone, kappa_ref, 7)
        mu = table_lookup(zone, mu_ref, 8)
        upper = (iota(shape, 0) % sides) >= macros

        def near(v):
            return jnp.where(upper, lane_roll(v, -1), 0.0)

        def everywhere(v):
            out = jnp.where(group == 0, lane_roll(v, -1), v)
            out = jnp.where(group == 2, lane_roll(v, 1), out)
            return jnp.where(group == 3, lane_roll(v, 2), out)

        near_mu = [near(v) for v in mu]
        near_mass = [near(v) for v in mass]
        e1_low = mass[1] + mu[1] + mu[4] + near_mu[0]
        e2_diag = mass[2] + mu[3] + mu[5] + mu[7] + near_mu[2] + yb(mu[4]) + yb(near_mu[6])
        e5_diag = mass[5] + mu[4] + mu[5]
        node_low = near_mass[0] + yb(mass[1]) + yb(near_mass[3])
        for t in range(7):
            node_low = node_low + mass[t]
        node_diag = node_low + mass[2] + near_mass[4] + yb(mass[5]) + yb(near_mass[6])

        def loose_terms(low):
            diag = {
                0: mass[0] + mu[0] + mu[2] + yb(mu[1]),
                3: mass[3] + mu[0] + mu[1] + mu[6],
                4: mass[4] + mu[2] + mu[3],
                6: mass[6] + mu[6] + mu[7],
            }
            if not low:
                diag[0] = diag[0] + mu[3]
                diag[3] = diag[3] + mu[7]
            al = {t: mass[t] * (EDGE_DAMPING / diag[t]) for t in LOOSE_TYPES}
            be = {t: mass[t] * (1.0 - al[t]) for t in LOOSE_TYPES}
            al_n = {t: near(al[t]) for t in LOOSE_TYPES}
            be_n = {t: near(be[t]) for t in LOOSE_TYPES}
            p0 = al[3] * mu[1] + al_n[0] * near_mu[0]
            r0 = -al[0] * yb(mu[1]) - yb(al_n[3] * near_mu[0])
            p1 = al[4] * mu[3] + al[6] * mu[7] + al_n[0] * near_mu[2] + yb(al_n[3] * near_mu[6])
            r1 = -al[0] * mu[3] - al[3] * mu[7] - al_n[4] * near_mu[2] - yb(al_n[6] * near_mu[6])
            p3 = -(be[0] + be[3] + be[4] + be[6]) - be_n[0] - yb(be_n[3])
            if not low:
                p3 = p3 - be_n[4] - yb(be_n[6])
            return p0, r0, p1, p3, r1

        low_terms, high_terms = loose_terms(True), loose_terms(False)

        def lowest(low, high):
            return jnp.where(group == 0, everywhere(low), everywhere(high))

        blocks = []
        for low, high in (
            (e1_low, e1_low + mu[5]),
            (e2_diag, e2_diag),
            (e5_diag, e5_diag),
            (node_low, node_diag),
        ):
            high_all = everywhere(high)
            low_all = high_all if low is high else jnp.where(group == 0, everywhere(low), high_all)
            blocks.append(jnp.concatenate([low_all] + [high_all] * (planes - 1), axis=0))
        same_ref[...] = same
        summed = group_sum(same, jnp.concatenate(blocks, axis=1))
        for i in range(4):
            damp = EDGE_DAMPING if i < 3 else NODE_DAMPING
            weight_ref[i] = damp / summed[:, LANES * i : LANES * (i + 1)]
        out = [
            mass[1],
            mass[2],
            mass[5],
            mu[1] + near_mu[0],
            mu[3] + mu[7] + near_mu[2] + yb(near_mu[6]),
            mu[4],
            mu[5],
        ]
        out += list(high_terms)
        for i, v in enumerate(out):
            field_ref[i] = everywhere(v)
        for i in range(4):
            field_ref[12 + i] = lowest(low_terms[i], high_terms[i])

    f32 = jnp.float32
    smem = pl.BlockSpec(memory_space=pltpu.SMEM)
    vmem = pl.BlockSpec(memory_space=pltpu.VMEM)
    return pl.pallas_call(
        body,
        compiler_params=pltpu.CompilerParams(vmem_limit_bytes=VMEM_BYTES),
        name="prepare",
        in_specs=[smem, smem] + [vmem] * (n_dom + 1),
        out_shape=(
            pltpu.VMEM((total, total), jnp.bfloat16),
            pltpu.VMEM((4, total, LANES), f32),
            pltpu.VMEM((16, n, LANES), f32),
        ),
        scratch_shapes=[pltpu.VMEM((n_dom, sides, LANES), f32)],
    )


def solve_kernel(n_dom, n_sub, macros, planes, cells):
    sides = 2 * macros
    n = n_dom * sides

    def body(recv_ref, swap_ref, coef_ref, edge_in, pot_in, same_ref, weight_ref, field_ref, edge_ref, pot_ref, one_ref, two_ref, turn_ref):
        k = lax.axis_index("sub")
        d = lax.axis_index("dom")
        shape = (n, LANES)
        group = iota(shape, 1) & 3
        upper = (iota(shape, 0) % sides) >= macros

        odd = (k & 1) == 1

        def rows_of(layer, at):
            at, late = at % planes, at >= planes
            parts = []
            for e in range(n_dom):
                rows = (e * n_sub + layer, slice(at * sides, (at + 1) * sides), slice(None))
                mine, other = recv_ref[rows], swap_ref[rows]
                parts.append(jnp.where(odd, mine, other) if late else jnp.where(odd, other, mine))
            return jnp.concatenate(parts, axis=0)

        same = same_ref[...]
        edge_mass = [field_ref[i] for i in range(3)]

        def of(v, p):
            return v[p * n : (p + 1) * n]

        def weight(i, p):
            return weight_ref[i, p * n : (p + 1) * n, :]

        def by_layer(at):
            r = [rows_of(layer, at) for layer in range(4)]
            even = (group & 1) == 0
            halves = []
            for i in (0, 2):
                halves.append(jnp.where(even, r[i], lane_roll(r[i + 1], 1)))
                halves.append(jnp.where(even, lane_roll(r[i], -1), r[i + 1]))
            low = group < 2
            out = [jnp.where(low, halves[i], lane_roll(halves[i + 2], 2)) for i in (0, 1)]
            return out + [jnp.where(low, lane_roll(halves[i], -2), halves[i + 2]) for i in (0, 1)]

        def from_below(v):
            return jnp.where(group > 0, lane_roll(v, 1), 0.0)

        def from_above(v):
            return jnp.where(group < 3, lane_roll(v, -1), 0.0)

        def below(f, p):
            return f[p - 1] if p > 0 else from_below(f[planes - 1])

        def above(f, p):
            return f[p + 1] if p < planes - 1 else from_above(f[0])

        def summed(fields):
            block = jnp.concatenate([jnp.concatenate(f, axis=0) for f in fields], axis=1)
            out = group_sum(same, block)
            return [out[:, LANES * i : LANES * (i + 1)] for i in range(len(fields))]

        span = range(planes)

        def edge_terms(r):
            by0 = [yb(r[0][p]) for p in span]
            by2 = [yb(r[2][p]) for p in span]
            out = []
            for p in span:
                value = by0[p] - r[0][p] - r[1][p] - r[2][p]
                out.append(value + below(r[1], p) + below(by2, p))
            return out

        given = [by_layer(p) for p in span]
        more = [by_layer(planes + p) for p in span]
        src = [[given[p][i] for p in span] for i in range(3)]
        sums = summed(src)
        e1 = [[of(sums[i], p) * weight(i, p) for p in span] for i in range(3)]
        r1 = [[src[i][p] - edge_mass[i] * e1[i][p] for p in span] for i in range(3)]
        nodes = [given[p][3] + v for p, v in enumerate(edge_terms(r1))]
        nodes[0] = nodes[0] + jnp.where(upper, from_below(more[1][2]), 0.0)
        (sums,) = summed([nodes])
        c1 = [of(sums, p) * weight(3, p) for p in span]
        for p in span:
            one_ref[0, p], one_ref[1, p], one_ref[2, p] = e1[0][p], e1[1][p], c1[p]

        w4 = [field_ref[5] * (e1[0][p] + ya(e1[1][p]) - e1[2][p]) for p in span]
        w5 = [field_ref[6] * (e1[1][p] + above(e1[0], p) - e1[2][p]) for p in span]
        ahead = [ya(c1[p]) for p in span]
        base, res = [[], [], []], [[], [], []]
        for p in span:
            curled = (
                field_ref[3] * e1[0][p] + w4[p] + below(w5, p),
                field_ref[4] * e1[1][p] + w5[p] + yb(w4[p]),
                -w4[p] - w5[p],
            )
            grad = (ahead[p] - c1[p], above(c1, p) - c1[p], above(ahead, p) - c1[p])
            for i in range(3):
                value = r1[i][p] - curled[i] - edge_mass[i] * grad[i]
                if i < 2:
                    value = value + more[p][i]
                if i == 1 and p == planes - 1:
                    value = value + from_above(more[0][2])
                res[i].append(value)
                base[i].append(e1[i][p] + grad[i])
        sums = summed(res)
        e2 = [[base[i][p] + of(sums[i], p) * weight(i, p) for p in span] for i in range(3)]
        r2 = [[src[i][p] - edge_mass[i] * e2[i][p] for p in span] for i in range(3)]
        nodes = []
        for p, value in enumerate(edge_terms(r2)):
            p0, r0, p1, p3 = (field_ref[(12 if p == 0 else 7) + i] for i in range(4))
            value = value + more[p][3] + p0 * e1[0][p] + r0 * yb(e1[0][p]) + p1 * e1[1][p]
            value = value + field_ref[11] * below(e1[1], p) + p3 * c1[p]
            if p == 0:
                value = value + from_below(more[planes - 1][2])
            if p == 1:
                moved = row_roll(more[1][2], macros)
                value = value + jnp.where(upper, from_below(moved), 0.0)
            if p == planes - 1:
                value = value + from_above(more[2][2])
            nodes.append(value)
        (sums,) = summed([nodes])
        for p in span:
            for i in range(3):
                two_ref[i, p] = e2[i][p]
            two_ref[3, p] = of(sums, p) * weight(3, p)

        strip = (sides, LANES)
        sh = Strip(strip)
        has_below = jnp.where(k == 0, 0.0, 1.0)
        has_above = jnp.where(k == n_sub - 1, 0.0, 1.0)

        def flagged(p, v):
            flag = has_below if p < 0 else has_above if p >= planes else None
            return v if flag is None or v is None else v * flag

        mine = pl.ds(pl.multiple_of(d * sides, sides), sides)
        turned = {}

        def taken(ref, p, i):
            step, plane = p // planes, p % planes
            key = (ref is two_ref, i, plane)
            if key not in turned:
                turned[key] = pltpu.roll(ref[i, plane, mine, :], (LANES - k) & (LANES - 1), 1)
            value = jnp.where(sh.own, lane_roll(turned[key], -step), 0.0)
            return value * (has_below if step < 0 else has_above) if step else value

        my_mass = [coef_ref[t] for t in range(7)]
        my_mu = [coef_ref[7 + f] for f in range(8)]
        loose_r = {}
        step_e = {}
        c_one = {p: taken(one_ref, p, 2) for p in range(-1, planes + 2)}
        faces = {}
        for p in range(-1, planes + 1):
            ea, eb = taken(one_ref, p, 0), taken(one_ref, p, 1)
            faces[p] = (
                my_mu[0] * sh.ax(ea),
                my_mu[1] * ea,
                my_mu[2] * sh.ax(eb),
                my_mu[3] * eb,
                my_mu[6] * sh.axy(eb),
                my_mu[7] * eb,
            )
        for p in range(-1, planes + 1):
            f0, f1, f2, f3, f6, f7 = faces[p]
            types = LOOSE_TYPES if p >= 0 else (4, 6)
            grad = grad_at(c_one[p], c_one[p + 1], sh, types)
            curled = {4: -f2 - f3, 6: -f6 - f7}
            if p >= 0:
                below = faces[p - 1]
                curled[0] = f0 + f2 + yb(f1) + below[3]
                curled[3] = f6 + below[5] - f0 - f1
            step_e[p], loose_r[p] = [None] * 7, [None] * 7
            for t in types:
                weight_t = coef_ref[22 + t] if p == 0 else coef_ref[15 + t]
                value = grad[t] - weight_t * (curled[t] + my_mass[t] * grad[t])
                value = flagged(p, value)
                step_e[p][t] = value
                loose_r[p][t] = -my_mass[t] * value
        c_two = {}
        for p in range(planes + 1):
            node = back_at(loose_r[p], loose_r[p - 1], sh)
            node = (coef_ref[30] if p == 0 else coef_ref[29]) * node
            node = jnp.where(sh.own, taken(two_ref, p, 3), node)
            c_two[p] = flagged(p, node)

        def plain(v):
            return jnp.where(sh.upper, jnp.where(sh.col == 3, lane_roll(v, 3), lane_roll(v, -1)), v)

        for p in range(planes):
            grad = grad_at(c_two[p], c_two[p + 1], sh)
            for t in range(7):
                if t in SHARED_TYPES:
                    start = taken(two_ref, p, SHARED_TYPES.index(t))
                else:
                    start = step_e[p][t]
                turn_ref[t, :, p, :] = plain(start + grad[t])
            turn_ref[7, :, p, :] = plain(c_one[p] + c_two[p])

        x = iota((planes, LANES), 1) & (LAT - 1)

        def overlaid(v, low, high):
            columns = []
            for c in range(8):
                add = jnp.where(x >= LAT - 4, lane_roll(high, 28 - 4 * c), 0.0)
                add = jnp.where(x < 4, lane_roll(low, -4 * c), add)
                columns.append(v[:, LANES * c : LANES * (c + 1)] + add)
            return jnp.concatenate(columns, axis=1)

        def macro_step(m, carry):
            for t in range(7):
                low, high = turn_ref[t, m], turn_ref[t, macros + m]
                edge_ref[m, t] = overlaid(edge_in[m, t], low, high)
            pot_ref[m] = overlaid(pot_in[m], turn_ref[7, m], turn_ref[7, macros + m])
            return carry

        lax.fori_loop(0, macros, macro_step, 0)

    f32 = jnp.float32
    return pl.pallas_call(
        body,
        compiler_params=pltpu.CompilerParams(vmem_limit_bytes=VMEM_BYTES),
        name="solve",
        out_shape=(
            jax.ShapeDtypeStruct((macros, 7, planes, cells), f32),
            jax.ShapeDtypeStruct((macros, planes, cells), f32),
        ),
        scratch_shapes=[
            pltpu.VMEM((3, planes, n, LANES), f32),
            pltpu.VMEM((4, planes, n, LANES), f32),
            pltpu.VMEM((8, sides, planes, LANES), f32),
        ],
    )


def near_core(*values):
    return [pltpu.with_memory_space_constraint(v, pltpu.VMEM) for v in values]


def local_small(source, zone_ids, kappa_table, mu_table, owner_dev, owner_group):
    macros, _, planes, cells = source.shape
    n_dom, n_sub = lax.axis_size("dom"), lax.axis_size("sub")
    sizes = (n_dom, n_sub, macros, planes, cells)
    lists = (owner_dev.shape[1], owner_group.shape[1])
    up = [(i, i + 1) for i in range(n_sub - 1)]
    down = [(i + 1, i) for i in range(n_sub - 1)]
    tables = (kappa_table.T, mu_table.T)
    far = [pltpu.with_memory_space_constraint(v, pltpu.HBM) for v in (*tables, zone_ids, source)]
    pay, coef = first_kernel(*sizes)(*far)
    recv = lax.all_to_all(pay, ("dom", "sub"), 0, 0)
    swapped = lax.ppermute(recv, "sub", [(i, i ^ 1) for i in range(n_sub)])
    labels = label_kernel(*sizes, *lists)(zone_ids, owner_dev, owner_group)
    labels = [labels]
    for i in range(1, n_dom):
        route = [(e, e ^ i) for e in range(n_dom)]
        labels.append(lax.ppermute(labels[0], "dom", route))
    low = lax.ppermute(source[:, :, planes - HALO :], "sub", up)
    high = lax.ppermute(source[:, :, :HALO], "sub", down)
    edge, pot = inner_kernel(*sizes)(*tables, zone_ids, source, *near_core(low, high))
    fields = prepare_kernel(*sizes, *lists)(*tables, *near_core(*labels, pot))
    return solve_kernel(*sizes)(*near_core(recv, swapped, coef, edge, pot, *fields))


def fits_small(mesh, source, owner_dev, owner_group):
    macros = source.shape[0] // mesh.shape["dom"]
    planes = source.shape[2] // mesh.shape["sub"]
    return (
        macros == 4
        and planes == 4
        and source.shape[3] == LAT * LAT
        and mesh.shape["sub"] == 4
        and owner_dev.shape[1] == 2 * macros * planes
        and owner_group.shape[1] == 32
        and mesh.shape["dom"] in (1, 2, 4, 8)
    )


def solution(mesh):
    in_specs = (
        P("dom", None, "sub", None),
        P("dom", None),
        P(),
        P(),
        P("dom", None),
        P("dom", None),
    )
    out_specs = (P("dom", None, "sub", None), P("dom", "sub", None))

    def step(source, zone_ids, kappa_table, mu_table, owner_dev, owner_group):
        body = local_small if fits_small(mesh, source, owner_dev, owner_group) else local
        mapped = jax.shard_map(
            body, mesh=mesh, in_specs=in_specs, out_specs=out_specs, check_vma=False
        )
        return mapped(source, zone_ids, kappa_table, mu_table, owner_dev, owner_group)

    return step
```

```python
import jax
import jax.numpy as jnp
from jax import lax
from jax.experimental import pallas as pl
from jax.experimental.pallas import tpu as pltpu
from jax.sharding import PartitionSpec as P

LAT = 32
SWEEPS = 2


EDGE_OFFSETS = ((0, 0, 1), (0, 1, 0), (1, 0, 0), (0, 1, 1), (1, 0, 1), (1, 1, 0), (1, 1, 1))
FACE_EDGES = (
    (0, 1, 3),
    (1, 0, 3),
    (0, 2, 4),
    (2, 0, 4),
    (1, 2, 5),
    (2, 1, 5),
    (3, 2, 6),
    (2, 3, 6),
)
SHARED_TYPES = (1, 2, 5)
EDGE_DAMPING = 0.6
NODE_DAMPING = 0.8


def with_halo(block, sides, width):
    for axis, dim in sides:
        count = lax.axis_size(axis)
        forward = [(i, i + 1) for i in range(count - 1)]
        backward = [(target, source) for source, target in forward]
        low = lax.ppermute(
            lax.slice_in_dim(block, block.shape[dim] - width, None, axis=dim), axis, forward
        )
        high = lax.ppermute(lax.slice_in_dim(block, 0, width, axis=dim), axis, backward)
        block = jnp.concatenate([low, block, high], axis=dim)
    return block


def from_behind(block, axis, distance):
    devices = range(lax.axis_size(axis))
    route = [(i - distance, i) for i in devices if i - distance in devices]
    return lax.ppermute(block, axis, route)


def shift_ahead(values, rise_y, rise_x):
    offset = rise_y * LAT + rise_x
    if offset == 0:
        return values
    padding = jnp.zeros(values.shape[:-1] + (offset,), values.dtype)
    shifted = jnp.concatenate([values[..., offset:], padding], axis=-1)
    if rise_x:
        column = jnp.arange(values.shape[-1]) % LAT
        shifted = jnp.where(column < LAT - rise_x, shifted, jnp.zeros_like(shifted))
    return shifted


def shift_behind(values, rise_y, rise_x):
    offset = rise_y * LAT + rise_x
    if offset == 0:
        return values
    padding = jnp.zeros(values.shape[:-1] + (offset,), values.dtype)
    shifted = jnp.concatenate([padding, values[..., :-offset]], axis=-1)
    if rise_x:
        column = jnp.arange(values.shape[-1]) % LAT
        shifted = jnp.where(column >= rise_x, shifted, jnp.zeros_like(shifted))
    return shifted


def apply_operator(padded, halo_width, extra_planes, first_plane, mass_coef, curl_coef):
    planes = padded.shape[2] - 2 * halo_width
    face_count = planes + extra_planes + 1
    first_face = halo_width - extra_planes - 1
    face_planes = first_plane - extra_planes - 1 + jnp.arange(face_count)
    face_valid = (face_planes >= 0)[None, :, None]
    result = [
        mass_coef[edge_type][:, None, :]
        * padded[:, edge_type, halo_width - extra_planes : halo_width + planes]
        for edge_type in range(7)
    ]
    for face_index, (first_edge, second_edge, diagonal_edge) in enumerate(FACE_EDGES):
        rise_z, rise_y, rise_x = EDGE_OFFSETS[first_edge]
        far_values = shift_ahead(
            padded[:, second_edge, first_face + rise_z : first_face + rise_z + face_count],
            rise_y,
            rise_x,
        )
        circulation = (
            padded[:, first_edge, first_face : first_face + face_count]
            + far_values
            - padded[:, diagonal_edge, first_face : first_face + face_count]
        )
        weighted = jnp.where(face_valid, curl_coef[face_index][:, None, :] * circulation, 0.0)
        result[first_edge] = result[first_edge] + weighted[:, 1:]
        result[diagonal_edge] = result[diagonal_edge] - weighted[:, 1:]
        result[second_edge] = result[second_edge] + shift_behind(
            weighted[:, 1 - rise_z : 1 - rise_z + planes + extra_planes], rise_y, rise_x
        )
    return jnp.stack(result, axis=1)


def edge_diagonal(mass_coef, curl_coef, first_plane, planes):
    inside = (first_plane + jnp.arange(planes) >= 1)[None, :, None]
    flat_planes = jnp.zeros((1, planes, 1), mass_coef.dtype)
    diagonal = [mass_coef[edge_type][:, None, :] + flat_planes for edge_type in range(7)]
    for face_index, (first_edge, second_edge, diagonal_edge) in enumerate(FACE_EDGES):
        rise_z, rise_y, rise_x = EDGE_OFFSETS[first_edge]
        own_term = curl_coef[face_index][:, None, :]
        diagonal[first_edge] = diagonal[first_edge] + own_term
        diagonal[diagonal_edge] = diagonal[diagonal_edge] + own_term
        behind_term = shift_behind(curl_coef[face_index], rise_y, rise_x)[:, None, :] + flat_planes
        if rise_z:
            behind_term = jnp.where(inside, behind_term, 0.0)
        diagonal[second_edge] = diagonal[second_edge] + behind_term
    return jnp.stack(diagonal, axis=1)


def node_diagonal(mass_coef, first_plane, planes):
    inside = (first_plane + jnp.arange(planes) >= 1)[None, :, None]
    total = jnp.zeros((mass_coef.shape[1], planes, mass_coef.shape[2]), mass_coef.dtype)
    for edge_type in range(7):
        rise_z, rise_y, rise_x = EDGE_OFFSETS[edge_type]
        total = total + mass_coef[edge_type][:, None, :]
        behind_term = shift_behind(mass_coef[edge_type], rise_y, rise_x)[:, None, :] + jnp.zeros(
            (1, planes, 1), mass_coef.dtype
        )
        if rise_z:
            behind_term = jnp.where(inside, behind_term, 0.0)
        total = total + behind_term
    return total


def node_residual(lowered, planes):
    total = jnp.zeros((lowered.shape[0], planes, lowered.shape[3]), lowered.dtype)
    for edge_type in range(7):
        rise_z, rise_y, rise_x = EDGE_OFFSETS[edge_type]
        total = (
            total
            + shift_behind(lowered[:, edge_type, 1 - rise_z : 1 - rise_z + planes], rise_y, rise_x)
            - lowered[:, edge_type, 1:]
        )
    return total


def gradient(raised, planes):
    result = []
    for edge_type in range(7):
        rise_z, rise_y, rise_x = EDGE_OFFSETS[edge_type]
        result.append(
            shift_ahead(raised[:, rise_z : rise_z + planes], rise_y, rise_x) - raised[:, :planes]
        )
    return jnp.stack(result, axis=1)


def edge_sides(values):
    macro_count, type_count, plane_count, _ = values.shape
    lattice = values.reshape(macro_count, type_count, plane_count, LAT, LAT)
    chosen = jnp.stack([lattice[:, edge_type] for edge_type in SHARED_TYPES], axis=1)
    sides = jnp.stack([chosen[..., 0], chosen[..., LAT - 1]], axis=1)
    return jnp.transpose(sides, (0, 1, 3, 2, 4)).reshape(-1, 3 * LAT)


def insert_edges(values, blocks):
    macro_count, type_count, plane_count, _ = values.shape
    shaped = blocks.reshape(macro_count, 2, plane_count, 3, LAT)
    shaped = jnp.transpose(shaped, (0, 1, 3, 2, 4))
    lattice = values.reshape(macro_count, type_count, plane_count, LAT, LAT)
    for side_index, column in ((0, 0), (1, LAT - 1)):
        for slot_type, edge_type in enumerate(SHARED_TYPES):
            lattice = lattice.at[:, edge_type, :, :, column].set(shaped[:, side_index, slot_type])
    return lattice.reshape(values.shape)


def node_sides(values):
    macro_count, plane_count, _ = values.shape
    lattice = values.reshape(macro_count, plane_count, LAT, LAT)
    sides = jnp.stack([lattice[..., 0], lattice[..., LAT - 1]], axis=1)
    return sides.reshape(-1, LAT)


def insert_nodes(values, blocks):
    macro_count, plane_count, _ = values.shape
    shaped = blocks.reshape(macro_count, 2, plane_count, LAT)
    lattice = values.reshape(macro_count, plane_count, LAT, LAT)
    for side_index, column in ((0, 0), (1, LAT - 1)):
        lattice = lattice.at[:, :, :, column].set(shaped[:, side_index])
    return lattice.reshape(values.shape)


def local(source, zone_ids, kappa_table, mu_table, owner_dev, owner_group):
    macro_count, type_count, planes, cell_count = source.shape
    first_plane = lax.axis_index("sub") * planes
    onehot = (jnp.arange(kappa_table.shape[0])[:, None] == zone_ids.reshape(1, -1)).astype(
        jnp.float32
    )
    mass_coef = jnp.dot(kappa_table.T, onehot, precision=lax.Precision.HIGHEST).reshape(
        type_count, macro_count, cell_count
    )
    curl_coef = jnp.dot(mu_table.T, onehot, precision=lax.Precision.HIGHEST).reshape(
        mu_table.shape[1], macro_count, cell_count
    )
    peer_count = lax.axis_size("dom")
    recv_rows = owner_group.shape[1]
    capacity = recv_rows // peer_count
    slot_count = owner_dev.shape[1]
    owner_of = owner_dev[0]
    groups = owner_group[0]
    earlier = jnp.arange(slot_count)[None, :] < jnp.arange(slot_count)[:, None]
    position = jnp.sum((owner_of[:, None] == owner_of[None, :]) & earlier, axis=1)
    slot_place = owner_of * capacity + position
    spread = (jnp.arange(recv_rows)[:, None] == slot_place[None, :]).astype(jnp.float32)
    same_group = (groups[:, None] == groups[None, :]).astype(jnp.float32)

    def owner_sum(received):
        summed = jnp.dot(
            same_group, received.reshape(recv_rows, -1), precision=lax.Precision.HIGHEST
        )
        return lax.all_to_all(
            summed.reshape(peer_count, capacity, -1), "dom", split_axis=0, concat_axis=0, tiled=True
        )

    def assemble(blocks):
        outgoing = jnp.dot(spread, blocks, precision=lax.Precision.HIGHEST).reshape(
            peer_count, capacity, blocks.shape[1]
        )
        returned = owner_sum(
            lax.all_to_all(outgoing, "dom", split_axis=0, concat_axis=0, tiled=True)
        )
        return jnp.take(returned.reshape(recv_rows, -1), slot_place, axis=0)

    rim_width = 2

    def rimmed(values):
        return with_halo(values, (("sub", 2),), rim_width)

    edge_diag = edge_diagonal(mass_coef, curl_coef, first_plane, planes)
    node_diag = node_diagonal(mass_coef, first_plane, planes)
    edge_width = 3 * LAT
    first_blocks = [edge_sides(edge_diag), node_sides(node_diag)]
    diag_sums = assemble(jnp.concatenate(first_blocks, axis=1))
    full_edge_diag = insert_edges(edge_diag, diag_sums[:, :edge_width])
    full_node_diag = insert_nodes(node_diag, diag_sums[:, edge_width : edge_width + LAT])
    source_below = from_behind(source[:, :, planes - 1 :], "sub", 1)
    edge_field = jnp.zeros_like(source)
    potential = jnp.zeros((macro_count, planes, cell_count), jnp.float32)
    for sweep_index in range(SWEEPS):
        if sweep_index == 0:
            residual = source
            residual_sum = assemble(edge_sides(residual))
        else:
            residual = source - apply_operator(
                rimmed(edge_field), rim_width, 0, first_plane, mass_coef, curl_coef
            )
            residual_sum = assemble(edge_sides(residual))
        full_residual = insert_edges(residual, residual_sum)
        edge_field = edge_field + EDGE_DAMPING * full_residual / full_edge_diag
        padded = rimmed(edge_field)
        lowered = jnp.concatenate([source_below, source], axis=2) - apply_operator(
            padded, 2, 1, first_plane, mass_coef, curl_coef
        )
        node_values = node_residual(lowered, planes)
        node_sum = assemble(node_sides(node_values))
        correction = NODE_DAMPING * insert_nodes(node_values, node_sum) / full_node_diag
        plane_above = from_behind(correction[:, :1], "sub", -1)
        edge_field = edge_field + gradient(
            jnp.concatenate([correction, plane_above], axis=1), planes
        )
        potential = potential + correction
    return (edge_field, potential)


LANES = 128
HALO = 2
VMEM_BYTES = 24 * 1024 * 1024
LOOSE_TYPES = (0, 3, 4, 6)


def lane_roll(v, s):
    s = s % v.shape[-1]
    return pltpu.roll(v, s, v.ndim - 1) if s else v


def row_roll(v, s):
    s = s % v.shape[0]
    return pltpu.roll(v, s, 0) if s else v


def iota(shape, dim):
    return lax.broadcasted_iota(jnp.int32, shape, dim)


def zb(v):
    return row_roll(v, 1)


def za(v):
    return row_roll(v, -1)


class Plane:
    def __init__(self, shape):
        self.lane = iota(shape, 1)
        self.x = self.lane & (LAT - 1)
        self.cells = shape[1]
        self.side = (self.x == 0) | (self.x == LAT - 1)

    def ax(self, v):
        return jnp.where(self.x < LAT - 1, lane_roll(v, -1), 0.0)

    def ay(self, v):
        return jnp.where(self.lane < self.cells - LAT, lane_roll(v, -LAT), 0.0)

    def bx(self, v):
        return jnp.where(self.x > 0, lane_roll(v, 1), 0.0)

    def by(self, v):
        return jnp.where(self.lane >= LAT, lane_roll(v, LAT), 0.0)

    def bxy(self, v):
        return jnp.where((self.lane >= LAT) & (self.x > 0), lane_roll(v, LAT + 1), 0.0)

    def axy(self, v):
        inner = (self.lane < self.cells - LAT) & (self.x < LAT - 1)
        return jnp.where(inner, lane_roll(v, -LAT - 1), 0.0)


def yb(v):
    lane = iota(v.shape, 1)
    first = jnp.where(lane < 4, 0.0, lane_roll(v, 36))
    return jnp.where(lane < 32, first, lane_roll(v, 32))


def ya(v):
    lane = iota(v.shape, 1)
    last = jnp.where(lane >= 124, 0.0, lane_roll(v, -36))
    return jnp.where(lane >= 96, last, lane_roll(v, -32))


class Strip:
    def __init__(self, shape):
        half = shape[0] // 2
        self.col = iota(shape, 1) & 3
        self.upper = iota(shape, 0) >= half
        self.own = self.col == 0

    def ax(self, v):
        wrap = jnp.where(self.upper, lane_roll(v, 3), 0.0)
        step = jnp.where(self.upper & self.own, 0.0, lane_roll(v, -1))
        return jnp.where(self.col == 3, wrap, step)

    def bx(self, v):
        wrap = jnp.where(self.upper, lane_roll(v, -3), 0.0)
        step = jnp.where(self.upper & (self.col == 1), 0.0, lane_roll(v, 1))
        return jnp.where(self.own, wrap, step)

    def ay(self, v):
        return ya(v)

    def by(self, v):
        return yb(v)

    def bxy(self, v):
        return yb(self.bx(v))

    def axy(self, v):
        return ya(self.ax(v))


def to_strip(v):
    lane = iota((v.shape[0], LANES), 1)
    block = (lane & 31) >> 2
    low = jnp.zeros((v.shape[0], LANES), v.dtype)
    high = low
    for c in range(8):
        column = v[:, LANES * c : LANES * (c + 1)]
        low = jnp.where(block == c, lane_roll(column, 4 * c), low)
        high = jnp.where(block == c, lane_roll(column, 4 * c - 28), high)
    high = jnp.where((lane & 3) == 0, lane_roll(high, -3), lane_roll(high, 1))
    return jnp.concatenate([low, high], axis=0)


def plus(*terms):
    total = None
    for term in terms:
        if term is not None:
            total = term if total is None else total + term
    return total


def on(f, v):
    return None if v is None else f(v)


def minus(v):
    return on(lambda a: -a, v)


def times(c, v):
    return on(lambda a: c * a, v)


def table_lookup(zone, table_ref, width):
    out = [jnp.zeros(zone.shape, jnp.float32)] * width
    for z in range(table_ref.shape[1]):
        hit = zone == z
        out = [jnp.where(hit, table_ref[i, z], v) for i, v in enumerate(out)]
    return out


def diagonals(mass, mu, sh):
    flat = [
        mass[0] + mu[0] + mu[2] + sh.by(mu[1]),
        mass[1] + mu[1] + mu[4] + sh.bx(mu[0]),
        mass[2] + mu[3] + mu[5] + mu[7] + sh.bx(mu[2]) + sh.by(mu[4]) + sh.bxy(mu[6]),
        mass[3] + mu[0] + mu[1] + mu[6],
        mass[4] + mu[2] + mu[3],
        mass[5] + mu[4] + mu[5],
        mass[6] + mu[6] + mu[7],
    ]
    rise = {0: mu[3], 1: mu[5], 3: mu[7]}
    node_flat = sh.bx(mass[0]) + sh.by(mass[1]) + sh.bxy(mass[3])
    for t in range(7):
        node_flat = node_flat + mass[t]
    node_rise = mass[2] + sh.bx(mass[4]) + sh.by(mass[5]) + sh.bxy(mass[6])
    return flat, rise, node_flat, node_rise


def grad_at(c, c_up, sh, types=range(7)):
    moves = (sh.ax, sh.ay, lambda v: v, sh.axy, sh.ax, sh.ay, sh.axy)
    out = [None] * 7
    for t in types:
        out[t] = plus(on(moves[t], c_up if EDGE_OFFSETS[t][0] else c), minus(c))
    return out


def back_at(r, r_below, sh):
    return plus(
        minus(plus(*r)),
        r_below[2],
        on(sh.bx, plus(r[0], r_below[4])),
        on(sh.by, plus(r[1], r_below[5])),
        on(sh.bxy, plus(r[3], r_below[6])),
    )


NONE7 = [None] * 7


def first_kernel(n_dom, n_sub, macros, planes, cells, slots, recv_rows):
    sides = 2 * macros
    capacity = recv_rows // n_dom
    half = (planes + 1) * sides

    def body(kappa_ref, mu_ref, zone_ref, source_ref, owner_ref, group_ref, pay_ref, coef_ref, hold_ref, sems):
        k = lax.axis_index("sub")
        d = lax.axis_index("dom")
        shape = (sides, LANES)
        sh = Strip(shape)
        row = iota(shape, 0)
        group = iota(shape, 1) & 3
        zone = to_strip(zone_ref[...])
        mass = table_lookup(zone, kappa_ref, 7)
        mu = table_lookup(zone, mu_ref, 8)
        flat, rise, node_flat, node_rise = diagonals(mass, mu, sh)
        w = [EDGE_DAMPING / (flat[t] + rise[t] if t in rise else flat[t]) for t in range(7)]
        w_low = [EDGE_DAMPING / flat[t] if t in rise else w[t] for t in range(7)]
        lowest = k == 0
        w_zero = [jnp.where(lowest, w_low[t], w[t]) for t in range(7)]
        nw = NODE_DAMPING / (node_flat + node_rise)
        nw_zero = jnp.where(lowest, NODE_DAMPING / node_flat, nw)
        for i, v in enumerate(mass + mu + w + w_zero + [nw, nw_zero]):
            coef_ref[i] = v
        has_below = jnp.where(lowest, 0.0, 1.0)
        has_above = jnp.where(k == n_sub - 1, 0.0, 1.0)

        def loose(t, v):
            return jnp.where(sh.own, 0.0, v) if t in SHARED_TYPES else v

        def flagged(p, v):
            flag = has_below if p < 0 else has_above if p >= planes else None
            return v if flag is None or v is None else v * flag

        src = {p: [to_strip(source_ref[:, t, p, :]) for t in range(7)] for p in range(planes)}
        e1, r1 = {}, {}
        for p in range(planes):
            wp = w_zero if p == 0 else w
            e1[p] = [loose(t, wp[t] * src[p][t]) for t in range(7)]
            r1[p] = [loose(t, src[p][t] - mass[t] * e1[p][t]) for t in range(7)]
        n1, c1 = {}, {}
        for p in range(planes + 1):
            n1[p] = back_at(r1.get(p, NONE7), r1.get(p - 1, NONE7), sh)
            c1[p] = jnp.where(sh.own, 0.0, (nw_zero if p == 0 else nw) * n1[p])
            c1[p] = flagged(p, c1[p])
        faces = {}
        for p in range(-1, planes):
            e, e_up = e1.get(p, NONE7), e1.get(p + 1, NONE7)
            far = (
                on(sh.ax, e[1]),
                on(sh.ay, e[0]),
                on(sh.ax, e[2]),
                e_up[0],
                on(sh.ay, e[2]),
                e_up[1],
                on(sh.axy, e[2]),
                e_up[3],
            )
            faces[p] = [
                flagged(p, times(mu[f], plus(e[a], far[f], minus(e[g]))))
                for f, (a, _, g) in enumerate(FACE_EDGES)
            ]
        res, r2 = {}, {}
        none8 = [None] * 8
        for p in range(-1, planes + 1):
            f, f_below = faces.get(p, none8), faces.get(p - 1, none8)
            curled = [
                plus(f[0], f[2], on(sh.by, f[1]), f_below[3]),
                plus(f[1], f[4], on(sh.bx, f[0]), f_below[5]),
                plus(f[3], f[5], f[7], on(sh.bx, f[2]), on(sh.by, f[4]), on(sh.bxy, f[6])),
                plus(f[6], f_below[7], minus(f[0]), minus(f[1])),
                minus(plus(f[2], f[3])),
                minus(plus(f[4], f[5])),
                minus(plus(f[6], f[7])),
            ]
            grad = grad_at(c1.get(p), c1.get(p + 1), sh)
            wp = w_zero if p == 0 else w
            res[p], r2[p] = [], []
            for t in range(7):
                g = grad[t]
                value = plus(
                    r1.get(p, NONE7)[t], minus(curled[t]), minus(times(mass[t], g))
                )
                res[p].append(value)
                e2 = plus(e1.get(p, NONE7)[t], g, times(wp[t], value))
                s = src[p][t] if p in src else None
                left = flagged(p, plus(s, minus(times(mass[t], e2))))
                r2[p].append(on(lambda v: loose(t, v), left))
        n2 = {p: back_at(r2.get(p, NONE7), r2.get(p - 1, NONE7), sh) for p in range(-1, planes + 2)}

        def merge(g0, g1, g2, g3):
            out = jnp.where(group == 1, lane_roll(g1, 1), g0)
            out = jnp.where(group == 2, lane_roll(g2, 2), out)
            return jnp.where(group == 3, lane_roll(g3, 3), out)

        high = jnp.where(row < macros, row_roll(n2[planes + 1], macros), n1[planes])
        spare = [flagged(-1, res[-1][2]), high, n2[-1], n2[planes]]
        for p in range(planes):
            rows = slice(p * sides, (p + 1) * sides)
            hold_ref[0, rows, :] = merge(src[p][1], src[p][2], src[p][5], n1[p])
            hold_ref[1, rows, :] = merge(res[p][1], res[p][2], spare[p], n2[p])
        owner = owner_ref[...].astype(jnp.float32)
        si, sj = iota((slots, slots), 0), iota((slots, slots), 1)
        column = jnp.sum(jnp.where(si == sj, owner, 0.0), axis=1, keepdims=True)
        lower = jnp.where((column == owner) & (si < sj), 1.0, 0.0)
        position = jnp.sum(lower, axis=0, keepdims=True)
        flat_index = owner * recv_rows + (d * capacity).astype(jnp.float32) + position
        keyed = group_ref[...].astype(jnp.float32) + (d * recv_rows).astype(jnp.float32)

        def spread_lanes(values):
            count = values.shape[1]
            place = iota((count, LANES), 0)
            place = 32 * (place >> 3) + 4 * (place & 7) + 3
            hot = jnp.where(place == iota((count, LANES), 1), 1.0, 0.0)
            rows = jnp.broadcast_to(values, (sides, count))
            return jnp.dot(rows, hot, precision=lax.Precision.HIGHEST)

        index = jnp.where(row < macros, spread_lanes(flat_index), spread_lanes(keyed))
        zone_f = zone.astype(jnp.float32)
        label = jnp.where(group == 2, lane_roll(zone_f, -1), lane_roll(zone_f, 1))
        label = jnp.where(group == 3, index, label)
        for i in range(2):
            hold_ref[i, planes * sides :, :] = label
        copies = [
            pltpu.make_async_copy(hold_ref.at[dest % 2], pay_ref.at[dest], sems.at[dest])
            for dest in range(n_dom * n_sub)
        ]
        for copy in copies:
            copy.start()
        for copy in copies:
            copy.wait()

    f32 = jnp.float32
    smem = pl.BlockSpec(memory_space=pltpu.SMEM)
    vmem = pl.BlockSpec(memory_space=pltpu.VMEM)
    return pl.pallas_call(
        body,
        compiler_params=pltpu.CompilerParams(vmem_limit_bytes=VMEM_BYTES),
        name="first",
        in_specs=[smem, smem, vmem, vmem, vmem, vmem],
        out_shape=(
            jax.ShapeDtypeStruct((n_dom * n_sub, half, LANES), f32),
            pltpu.VMEM((31, sides, LANES), f32),
        ),
        out_specs=(pl.BlockSpec(memory_space=pltpu.HBM), vmem),
        scratch_shapes=[
            pltpu.VMEM((2, half, LANES), f32),
            pltpu.SemaphoreType.DMA((n_dom * n_sub,)),
        ],
    )


def inner_kernel(n_dom, n_sub, macros, planes, cells):
    rows = planes + 2 * HALO

    def body(kappa_ref, mu_ref, zone_ref, source_ref, low_ref, high_ref, edge_ref, pot_ref, coef_ref, sx_ref, w_ref):
        k = lax.axis_index("sub")
        sh = Plane((rows, cells))
        at = k * planes - HALO + iota((rows, cells), 0)
        inside, valid = at >= 1, (at >= 0) & (at < n_sub * planes)
        zones = zone_ref[...]
        for i, v in enumerate(table_lookup(zones, kappa_ref, 7) + table_lookup(zones, mu_ref, 8)):
            coef_ref[i] = v

        def macro_step(m, carry):
            def coef(i):
                return jnp.broadcast_to(coef_ref[i, pl.ds(m, 1), :], (rows, cells))

            mass = [coef(t) for t in range(7)]
            mu = [coef(7 + f) for f in range(8)]
            flat, rise, node_flat, node_rise = diagonals(mass, mu, sh)
            for t in range(7):
                diag = flat[t]
                if t in rise:
                    diag = diag + jnp.where(inside, rise[t], 0.0)
                w_ref[t] = EDGE_DAMPING / diag
            w_ref[7] = NODE_DAMPING / (node_flat + jnp.where(inside, node_rise, 0.0))
            node_open = valid & jnp.logical_not(sh.side)

            def loose(t, v):
                return jnp.where(sh.side, 0.0, v) if t in SHARED_TYPES else v

            def node_back(r):
                own = -(((r[0] + r[1]) + (r[2] + r[3])) + ((r[4] + r[5]) + r[6]))
                back = zb(r[2]) + sh.bx(r[0] + zb(r[4])) + sh.by(r[1] + zb(r[5]))
                return jnp.where(node_open, w_ref[7] * (own + back + sh.bxy(r[3] + zb(r[6]))), 0.0)

            def node_grad(c):
                cx, cy, cxy = sh.ax(c), sh.ay(c), sh.axy(c)
                ends = (cx, cy, za(c), cxy, za(cx), za(cy), za(cxy))
                return [jnp.where(valid, end - c, 0.0) for end in ends]

            e, r1 = [], []
            for t in range(7):
                sx_ref[t, 0:HALO, :] = low_ref[m, t]
                sx_ref[t, HALO : HALO + planes, :] = source_ref[m, t]
                sx_ref[t, HALO + planes : rows, :] = high_ref[m, t]
            for t in range(7):
                e.append(loose(t, w_ref[t] * sx_ref[t]))
                r1.append(loose(t, sx_ref[t] - mass[t] * e[t]))
            c1 = node_back(r1)
            grad = node_grad(c1)
            far = (
                sh.ax(e[1]),
                sh.ay(e[0]),
                sh.ax(e[2]),
                za(e[0]),
                sh.ay(e[2]),
                za(e[1]),
                sh.axy(e[2]),
                za(e[3]),
            )
            f = [
                jnp.where(valid, mu[i] * (e[a] + far[i] - e[g]), 0.0)
                for i, (a, _, g) in enumerate(FACE_EDGES)
            ]
            curled = [
                f[0] + f[2] + sh.by(f[1]) + zb(f[3]),
                f[1] + f[4] + sh.bx(f[0]) + zb(f[5]),
                f[3] + f[5] + f[7] + sh.bx(f[2]) + sh.by(f[4]) + sh.bxy(f[6]),
                f[6] + zb(f[7]) - f[0] - f[1],
                -f[2] - f[3],
                -f[4] - f[5],
                -f[6] - f[7],
            ]
            e2, left = [], []
            for t in range(7):
                res = r1[t] - curled[t] - mass[t] * grad[t]
                value = jnp.where(valid, loose(t, e[t] + grad[t] + w_ref[t] * res), 0.0)
                e2.append(value)
                left.append(loose(t, sx_ref[t] - mass[t] * value))
            c2 = node_back(left)
            grad = node_grad(c2)
            for t in range(7):
                edge_ref[m, t] = (e2[t] + grad[t])[HALO : HALO + planes]
            pot_ref[m] = (c1 + c2)[HALO : HALO + planes]
            return carry

        lax.fori_loop(0, macros, macro_step, 0)

    f32 = jnp.float32
    smem = pl.BlockSpec(memory_space=pltpu.SMEM)
    vmem = pl.BlockSpec(memory_space=pltpu.VMEM)
    return pl.pallas_call(
        body,
        compiler_params=pltpu.CompilerParams(vmem_limit_bytes=VMEM_BYTES),
        name="inner",
        in_specs=[smem, smem, vmem, vmem, vmem, vmem],
        out_shape=(
            pltpu.VMEM((macros, 7, planes, cells), f32),
            pltpu.VMEM((macros, planes, cells), f32),
        ),
        scratch_shapes=[
            pltpu.VMEM((15, macros, cells), f32),
            pltpu.VMEM((7, rows, cells), f32),
            pltpu.VMEM((8, rows, cells), f32),
        ],
    )


def group_sum(same, block):
    parts = []
    rest = block
    for _ in range(3):
        parts.append(rest.astype(jnp.bfloat16))
        rest = rest - parts[-1].astype(jnp.float32)
    wide = jnp.concatenate([same] * 3, axis=1)
    return jnp.dot(wide, jnp.concatenate(parts, axis=0), preferred_element_type=jnp.float32)


def prepare_kernel(n_dom, n_sub, macros, planes, cells, slots, recv_rows):
    sides = 2 * macros
    n = n_dom * sides
    total = n * planes

    def body(kappa_ref, mu_ref, wide_ref, same_ref, weight_ref, field_ref, recv_ref):
        for e in range(n_dom):
            recv_ref[e] = wide_ref[e * lax.axis_size("sub"), planes * sides :, :]
        shape = (n, LANES)
        group = iota(shape, 1) & 3
        index = jnp.concatenate([recv_ref[e] for e in range(n_dom)], axis=0)
        lane = iota(shape, 1)
        row = iota(shape, 0) % sides
        firsts = []
        for e in range(n_dom):
            one = recv_ref[e, 0:1, :]
            firsts.append(jnp.broadcast_to(one, (sides, LANES)))
        firsts = jnp.concatenate(firsts, axis=0)
        flat = []
        for p in range(planes):
            slot = (2 * (row % macros) + row // macros) * planes + p
            here = lane == 32 * (slot >> 3) + 4 * (slot & 7) + 3
            flat.append(jnp.sum(jnp.where(here, firsts, 0.0), axis=1, keepdims=True))
        flat = jnp.concatenate(flat, axis=0).astype(jnp.int32)
        owner = flat // recv_rows
        receive = flat - owner * recv_rows
        table = jnp.zeros((total, LANES), jnp.float32)
        for e in range(n_dom):
            one = recv_ref[e, macros : macros + 1, :]
            table = jnp.where(owner == e, jnp.broadcast_to(one, (total, LANES)), table)
        here = iota((total, LANES), 1) == 32 * (receive >> 3) + 4 * (receive & 7) + 3
        key = jnp.sum(jnp.where(here, table, 0.0), axis=1, keepdims=True)
        square = (total, total)
        diagonal = iota(square, 0) == iota(square, 1)
        key_row = jnp.sum(jnp.where(diagonal, key, 0.0), axis=0, keepdims=True)
        same = jnp.where(key == key_row, 1.0, 0.0).astype(jnp.bfloat16)

        zone = index.astype(jnp.int32)
        mass = table_lookup(zone, kappa_ref, 7)
        mu = table_lookup(zone, mu_ref, 8)
        upper = (iota(shape, 0) % sides) >= macros

        def near(v):
            return jnp.where(upper, lane_roll(v, -1), 0.0)

        def everywhere(v):
            out = jnp.where(group == 0, lane_roll(v, -1), v)
            out = jnp.where(group == 2, lane_roll(v, 1), out)
            return jnp.where(group == 3, lane_roll(v, 2), out)

        near_mu = [near(v) for v in mu]
        near_mass = [near(v) for v in mass]
        e1_low = mass[1] + mu[1] + mu[4] + near_mu[0]
        e2_diag = mass[2] + mu[3] + mu[5] + mu[7] + near_mu[2] + yb(mu[4]) + yb(near_mu[6])
        e5_diag = mass[5] + mu[4] + mu[5]
        node_low = near_mass[0] + yb(mass[1]) + yb(near_mass[3])
        for t in range(7):
            node_low = node_low + mass[t]
        node_diag = node_low + mass[2] + near_mass[4] + yb(mass[5]) + yb(near_mass[6])

        def loose_terms(low):
            diag = {
                0: mass[0] + mu[0] + mu[2] + yb(mu[1]),
                3: mass[3] + mu[0] + mu[1] + mu[6],
                4: mass[4] + mu[2] + mu[3],
                6: mass[6] + mu[6] + mu[7],
            }
            if not low:
                diag[0] = diag[0] + mu[3]
                diag[3] = diag[3] + mu[7]
            al = {t: mass[t] * (EDGE_DAMPING / diag[t]) for t in LOOSE_TYPES}
            be = {t: mass[t] * (1.0 - al[t]) for t in LOOSE_TYPES}
            al_n = {t: near(al[t]) for t in LOOSE_TYPES}
            be_n = {t: near(be[t]) for t in LOOSE_TYPES}
            p0 = al[3] * mu[1] + al_n[0] * near_mu[0]
            r0 = -al[0] * yb(mu[1]) - yb(al_n[3] * near_mu[0])
            p1 = al[4] * mu[3] + al[6] * mu[7] + al_n[0] * near_mu[2] + yb(al_n[3] * near_mu[6])
            r1 = -al[0] * mu[3] - al[3] * mu[7] - al_n[4] * near_mu[2] - yb(al_n[6] * near_mu[6])
            p3 = -(be[0] + be[3] + be[4] + be[6]) - be_n[0] - yb(be_n[3])
            if not low:
                p3 = p3 - be_n[4] - yb(be_n[6])
            return p0, r0, p1, p3, r1

        low_terms, high_terms = loose_terms(True), loose_terms(False)

        def lowest(low, high):
            return jnp.where(group == 0, everywhere(low), everywhere(high))

        blocks = []
        for low, high in (
            (e1_low, e1_low + mu[5]),
            (e2_diag, e2_diag),
            (e5_diag, e5_diag),
            (node_low, node_diag),
        ):
            high_all = everywhere(high)
            low_all = high_all if low is high else jnp.where(group == 0, everywhere(low), high_all)
            blocks.append(jnp.concatenate([low_all] + [high_all] * (planes - 1), axis=0))
        same_ref[...] = same
        summed = group_sum(same, jnp.concatenate(blocks, axis=1))
        for i in range(4):
            damp = EDGE_DAMPING if i < 3 else NODE_DAMPING
            weight_ref[i] = damp / summed[:, LANES * i : LANES * (i + 1)]
        out = [
            mass[1],
            mass[2],
            mass[5],
            mu[1] + near_mu[0],
            mu[3] + mu[7] + near_mu[2] + yb(near_mu[6]),
            mu[4],
            mu[5],
        ]
        out += list(high_terms)
        for i, v in enumerate(out):
            field_ref[i] = everywhere(v)
        for i in range(4):
            field_ref[12 + i] = lowest(low_terms[i], high_terms[i])

    f32 = jnp.float32
    smem = pl.BlockSpec(memory_space=pltpu.SMEM)
    vmem = pl.BlockSpec(memory_space=pltpu.VMEM)
    return pl.pallas_call(
        body,
        compiler_params=pltpu.CompilerParams(vmem_limit_bytes=VMEM_BYTES),
        name="prepare",
        in_specs=[smem, smem, vmem],
        out_shape=(
            pltpu.VMEM((total, total), jnp.bfloat16),
            pltpu.VMEM((4, total, LANES), f32),
            pltpu.VMEM((16, n, LANES), f32),
        ),
        scratch_shapes=[pltpu.VMEM((n_dom, sides, LANES), f32)],
    )


def solve_kernel(n_dom, n_sub, macros, planes, cells):
    sides = 2 * macros
    n = n_dom * sides

    def body(recv_ref, swap_ref, coef_ref, edge_in, pot_in, same_ref, weight_ref, field_ref, edge_ref, pot_ref, one_ref, two_ref, turn_ref):
        k = lax.axis_index("sub")
        d = lax.axis_index("dom")
        shape = (n, LANES)
        group = iota(shape, 1) & 3
        upper = (iota(shape, 0) % sides) >= macros

        odd = (k & 1) == 1

        def rows_of(layer, at):
            at, late = at % planes, at >= planes
            parts = []
            for e in range(n_dom):
                rows = (e * n_sub + layer, slice(at * sides, (at + 1) * sides), slice(None))
                mine, other = recv_ref[rows], swap_ref[rows]
                parts.append(jnp.where(odd, mine, other) if late else jnp.where(odd, other, mine))
            return jnp.concatenate(parts, axis=0)

        same = same_ref[...]
        edge_mass = [field_ref[i] for i in range(3)]

        def of(v, p):
            return v[p * n : (p + 1) * n]

        def weight(i, p):
            return weight_ref[i, p * n : (p + 1) * n, :]

        def by_layer(at):
            r = [rows_of(layer, at) for layer in range(4)]
            even = (group & 1) == 0
            halves = []
            for i in (0, 2):
                halves.append(jnp.where(even, r[i], lane_roll(r[i + 1], 1)))
                halves.append(jnp.where(even, lane_roll(r[i], -1), r[i + 1]))
            low = group < 2
            out = [jnp.where(low, halves[i], lane_roll(halves[i + 2], 2)) for i in (0, 1)]
            return out + [jnp.where(low, lane_roll(halves[i], -2), halves[i + 2]) for i in (0, 1)]

        def from_below(v):
            return jnp.where(group > 0, lane_roll(v, 1), 0.0)

        def from_above(v):
            return jnp.where(group < 3, lane_roll(v, -1), 0.0)

        def below(f, p):
            return f[p - 1] if p > 0 else from_below(f[planes - 1])

        def above(f, p):
            return f[p + 1] if p < planes - 1 else from_above(f[0])

        def summed(fields):
            block = jnp.concatenate([jnp.concatenate(f, axis=0) for f in fields], axis=1)
            out = group_sum(same, block)
            return [out[:, LANES * i : LANES * (i + 1)] for i in range(len(fields))]

        span = range(planes)

        def edge_terms(r):
            by0 = [yb(r[0][p]) for p in span]
            by2 = [yb(r[2][p]) for p in span]
            out = []
            for p in span:
                value = by0[p] - r[0][p] - r[1][p] - r[2][p]
                out.append(value + below(r[1], p) + below(by2, p))
            return out

        given = [by_layer(p) for p in span]
        more = [by_layer(planes + p) for p in span]
        src = [[given[p][i] for p in span] for i in range(3)]
        sums = summed(src)
        e1 = [[of(sums[i], p) * weight(i, p) for p in span] for i in range(3)]
        r1 = [[src[i][p] - edge_mass[i] * e1[i][p] for p in span] for i in range(3)]
        nodes = [given[p][3] + v for p, v in enumerate(edge_terms(r1))]
        nodes[0] = nodes[0] + jnp.where(upper, from_below(more[1][2]), 0.0)
        (sums,) = summed([nodes])
        c1 = [of(sums, p) * weight(3, p) for p in span]
        for p in span:
            one_ref[0, p], one_ref[1, p], one_ref[2, p] = e1[0][p], e1[1][p], c1[p]

        w4 = [field_ref[5] * (e1[0][p] + ya(e1[1][p]) - e1[2][p]) for p in span]
        w5 = [field_ref[6] * (e1[1][p] + above(e1[0], p) - e1[2][p]) for p in span]
        ahead = [ya(c1[p]) for p in span]
        base, res = [[], [], []], [[], [], []]
        for p in span:
            curled = (
                field_ref[3] * e1[0][p] + w4[p] + below(w5, p),
                field_ref[4] * e1[1][p] + w5[p] + yb(w4[p]),
                -w4[p] - w5[p],
            )
            grad = (ahead[p] - c1[p], above(c1, p) - c1[p], above(ahead, p) - c1[p])
            for i in range(3):
                value = r1[i][p] - curled[i] - edge_mass[i] * grad[i]
                if i < 2:
                    value = value + more[p][i]
                if i == 1 and p == planes - 1:
                    value = value + from_above(more[0][2])
                res[i].append(value)
                base[i].append(e1[i][p] + grad[i])
        sums = summed(res)
        e2 = [[base[i][p] + of(sums[i], p) * weight(i, p) for p in span] for i in range(3)]
        r2 = [[src[i][p] - edge_mass[i] * e2[i][p] for p in span] for i in range(3)]
        nodes = []
        for p, value in enumerate(edge_terms(r2)):
            p0, r0, p1, p3 = (field_ref[(12 if p == 0 else 7) + i] for i in range(4))
            value = value + more[p][3] + p0 * e1[0][p] + r0 * yb(e1[0][p]) + p1 * e1[1][p]
            value = value + field_ref[11] * below(e1[1], p) + p3 * c1[p]
            if p == 0:
                value = value + from_below(more[planes - 1][2])
            if p == 1:
                moved = row_roll(more[1][2], macros)
                value = value + jnp.where(upper, from_below(moved), 0.0)
            if p == planes - 1:
                value = value + from_above(more[2][2])
            nodes.append(value)
        (sums,) = summed([nodes])
        for p in span:
            for i in range(3):
                two_ref[i, p] = e2[i][p]
            two_ref[3, p] = of(sums, p) * weight(3, p)

        strip = (sides, LANES)
        sh = Strip(strip)
        has_below = jnp.where(k == 0, 0.0, 1.0)
        has_above = jnp.where(k == n_sub - 1, 0.0, 1.0)

        def flagged(p, v):
            flag = has_below if p < 0 else has_above if p >= planes else None
            return v if flag is None or v is None else v * flag

        mine = pl.ds(pl.multiple_of(d * sides, sides), sides)
        turned = {}

        def taken(ref, p, i):
            step, plane = p // planes, p % planes
            key = (ref is two_ref, i, plane)
            if key not in turned:
                turned[key] = pltpu.roll(ref[i, plane, mine, :], (LANES - k) & (LANES - 1), 1)
            value = jnp.where(sh.own, lane_roll(turned[key], -step), 0.0)
            return value * (has_below if step < 0 else has_above) if step else value

        my_mass = [coef_ref[t] for t in range(7)]
        my_mu = [coef_ref[7 + f] for f in range(8)]
        loose_r = {}
        step_e = {}
        c_one = {p: taken(one_ref, p, 2) for p in range(-1, planes + 2)}
        faces = {}
        for p in range(-1, planes + 1):
            ea, eb = taken(one_ref, p, 0), taken(one_ref, p, 1)
            faces[p] = (
                my_mu[0] * sh.ax(ea),
                my_mu[1] * ea,
                my_mu[2] * sh.ax(eb),
                my_mu[3] * eb,
                my_mu[6] * sh.axy(eb),
                my_mu[7] * eb,
            )
        for p in range(-1, planes + 1):
            f0, f1, f2, f3, f6, f7 = faces[p]
            types = LOOSE_TYPES if p >= 0 else (4, 6)
            grad = grad_at(c_one[p], c_one[p + 1], sh, types)
            curled = {4: -f2 - f3, 6: -f6 - f7}
            if p >= 0:
                below = faces[p - 1]
                curled[0] = f0 + f2 + yb(f1) + below[3]
                curled[3] = f6 + below[5] - f0 - f1
            step_e[p], loose_r[p] = [None] * 7, [None] * 7
            for t in types:
                weight_t = coef_ref[22 + t] if p == 0 else coef_ref[15 + t]
                value = grad[t] - weight_t * (curled[t] + my_mass[t] * grad[t])
                value = flagged(p, value)
                step_e[p][t] = value
                loose_r[p][t] = -my_mass[t] * value
        c_two = {}
        for p in range(planes + 1):
            node = back_at(loose_r[p], loose_r[p - 1], sh)
            node = (coef_ref[30] if p == 0 else coef_ref[29]) * node
            node = jnp.where(sh.own, taken(two_ref, p, 3), node)
            c_two[p] = flagged(p, node)

        def plain(v):
            return jnp.where(sh.upper, jnp.where(sh.col == 3, lane_roll(v, 3), lane_roll(v, -1)), v)

        for p in range(planes):
            grad = grad_at(c_two[p], c_two[p + 1], sh)
            for t in range(7):
                if t in SHARED_TYPES:
                    start = taken(two_ref, p, SHARED_TYPES.index(t))
                else:
                    start = step_e[p][t]
                turn_ref[t, :, p, :] = plain(start + grad[t])
            turn_ref[7, :, p, :] = plain(c_one[p] + c_two[p])

        x = iota((planes, LANES), 1) & (LAT - 1)

        def overlaid(v, low, high):
            columns = []
            for c in range(8):
                add = jnp.where(x >= LAT - 4, lane_roll(high, 28 - 4 * c), 0.0)
                add = jnp.where(x < 4, lane_roll(low, -4 * c), add)
                columns.append(v[:, LANES * c : LANES * (c + 1)] + add)
            return jnp.concatenate(columns, axis=1)

        def macro_step(m, carry):
            for t in range(7):
                low, high = turn_ref[t, m], turn_ref[t, macros + m]
                edge_ref[m, t] = overlaid(edge_in[m, t], low, high)
            pot_ref[m] = overlaid(pot_in[m], turn_ref[7, m], turn_ref[7, macros + m])
            return carry

        lax.fori_loop(0, macros, macro_step, 0)

    f32 = jnp.float32
    return pl.pallas_call(
        body,
        compiler_params=pltpu.CompilerParams(vmem_limit_bytes=VMEM_BYTES),
        name="solve",
        out_shape=(
            jax.ShapeDtypeStruct((macros, 7, planes, cells), f32),
            jax.ShapeDtypeStruct((macros, planes, cells), f32),
        ),
        scratch_shapes=[
            pltpu.VMEM((3, planes, n, LANES), f32),
            pltpu.VMEM((4, planes, n, LANES), f32),
            pltpu.VMEM((8, sides, planes, LANES), f32),
        ],
    )


def near_core(*values):
    return [pltpu.with_memory_space_constraint(v, pltpu.VMEM) for v in values]


def local_small(source, zone_ids, kappa_table, mu_table, owner_dev, owner_group):
    macros, _, planes, cells = source.shape
    n_dom, n_sub = lax.axis_size("dom"), lax.axis_size("sub")
    sizes = (n_dom, n_sub, macros, planes, cells)
    lists = (owner_dev.shape[1], owner_group.shape[1])
    up = [(i, i + 1) for i in range(n_sub - 1)]
    down = [(i + 1, i) for i in range(n_sub - 1)]
    tables = (kappa_table.T, mu_table.T)
    far = [pltpu.with_memory_space_constraint(v, pltpu.HBM) for v in (*tables, zone_ids, source, owner_dev, owner_group)]
    pay, coef = first_kernel(*sizes, *lists)(*far)
    recv = lax.all_to_all(pay, ("dom", "sub"), 0, 0)
    swapped = lax.ppermute(recv, "sub", [(i, i ^ 1) for i in range(n_sub)])
    low = lax.ppermute(source[:, :, planes - HALO :], "sub", up)
    high = lax.ppermute(source[:, :, :HALO], "sub", down)
    edge, pot = inner_kernel(*sizes)(*tables, zone_ids, source, *near_core(low, high))
    fields = prepare_kernel(*sizes, *lists)(*tables, *near_core(recv))
    return solve_kernel(*sizes)(*near_core(recv, swapped, coef, edge, pot, *fields))


def fits_small(mesh, source, owner_dev, owner_group):
    macros = source.shape[0] // mesh.shape["dom"]
    planes = source.shape[2] // mesh.shape["sub"]
    return (
        macros == 4
        and planes == 4
        and source.shape[3] == LAT * LAT
        and mesh.shape["sub"] == 4
        and owner_dev.shape[1] == 2 * macros * planes
        and owner_group.shape[1] == 32
        and mesh.shape["dom"] in (1, 2, 4, 8)
    )


def solution(mesh):
    in_specs = (
        P("dom", None, "sub", None),
        P("dom", None),
        P(),
        P(),
        P("dom", None),
        P("dom", None),
    )
    out_specs = (P("dom", None, "sub", None), P("dom", "sub", None))

    def step(source, zone_ids, kappa_table, mu_table, owner_dev, owner_group):
        body = local_small if fits_small(mesh, source, owner_dev, owner_group) else local
        mapped = jax.shard_map(
            body, mesh=mesh, in_specs=in_specs, out_specs=out_specs, check_vma=False
        )
        return mapped(source, zone_ids, kappa_table, mu_table, owner_dev, owner_group)

    return step
```
